128 devices in a mesh: tok: 8 (over z, core), hid: 16 (over x, y).
Axes of the slice: x: 4, y: 4, z: 4, core: 2. Of those that a mesh axis runs over, the one named last changes fastest.
Arguments:
- tokens: bfloat16 [1024, 4096], P('tok', 'hid'), may hold values from -6 to 6
- out_grad: bfloat16 [1024, 4096], P('tok', 'hid'), may hold values from -6 to 6
- routing_ids: int32 [1024, 2], P('tok'), may hold values from 0 to 7, all different within a row; in each aligned block of 128 rows (0 to 127, 128 to 255, ...) at most 48 rows name the same one
- route_weights: bfloat16 [1024, 2], P('tok'), may hold values from 0.049804688 to 1
- gate_matrix: bfloat16 [8, 4096, 8192], P('tok', None, 'hid'), may hold values from -0.125 to 0.125
- up_matrix: bfloat16 [8, 4096, 8192], P('tok', None, 'hid'), may hold values from -0.09375 to 0.09375
- down_matrix: bfloat16 [8, 8192, 4096], P('tok', 'hid'), may hold values from -0.0625 to 0.0625
Outputs:
- input_grad: bfloat16 [1024, 4096], P('tok', 'hid')
- route_grad: bfloat16 [1024, 2], P('tok')
- gate_matrix_grad: bfloat16 [8, 4096, 8192], P('tok', None, 'hid')
- up_matrix_grad: bfloat16 [8, 4096, 8192], P('tok', None, 'hid')
- down_matrix_grad: bfloat16 [8, 8192, 4096], P('tok', 'hid')
The draws below stay inside these ranges and needn't reach their ends.
Inputs may be any that keep to these rules, and one draw needn't show every extreme that they name: `routing_ids`: each token names two different experts. Among the 128 tokens of one index of tok no expert is named more than 48 times, a bound that some expert reaches in each such block.
All inputs are finite; a program needn't handle non-finite values.
Results may differ from the reference program's by a relative error of at most 0.0076.
Values may be sent and summed in bfloat16 or wider, within the bound.
A program may use at most 128 MiB of HBM per device.

```python
import math
import jax
import jax.numpy as jnp
import numpy as np
from jax import lax

D = 4096
FF = 8192
TOK_DEV = 128
EXPERTS = 8
TOKENS = 1024
CAP = 48
N_TOK = 8


def strengthened(drawn, rng, source, target, shards_of, factor):
    def block_of(axis_at):
        return (jnp.arange(drawn.shape[axis_at]) // (drawn.shape[axis_at] // shards_of)).reshape((-1,) + (1,) * (drawn.ndim - 1 - axis_at))

    one_side = jax.random.permutation(rng, shards_of)[block_of(target)]
    second = (block_of(target) + shards_of // 2) % shards_of
    return jnp.where((block_of(source) == one_side) | (block_of(source) == second), factor * drawn, drawn)


def block_levels(key, shape, shards, low, top_value):
    def one(axis_at, shards_of):
        draws = jax.random.uniform(jax.random.fold_in(jax.random.fold_in(key, 6), axis_at), (shards_of,), jnp.float32, low / len(shards), top_value / len(shards))
        return jnp.repeat(jnp.exp(draws), shape[axis_at] // shards_of).reshape((-1,) + (1,) * (len(shape) - axis_at - 1))

    level = one(*shards[0])
    for cut in shards[1:]:
        level = level * one(*cut)
    return level


def deal_out(rng, own, number, rows, count, top, most, skew):
    ranking = jax.random.permutation(rng, count)
    crowded, usual = portions_of(count, rows * top, most, skew, True), portions_of(count, rows * top, most, skew, False)
    places = jnp.arange(count)

    def named(tallies, offset_by):
        used = int((tallies > 0).sum())
        fixed = max(1, used // 4)
        shifted = fixed + (places - fixed + offset_by * (used - fixed)) % max(1, count - fixed)
        return jnp.zeros((count,), jnp.int32).at[ranking[jnp.where(places < fixed, places, shifted)]].set(jnp.asarray(tallies, jnp.int32))

    tallies = jnp.where(number % 4 == 0, named(crowded, number // 4), named(usual, number - number // 4 - 1))
    mixed = jax.random.permutation(jax.random.fold_in(own, 3), count)
    source_of, sink = mixed[0:count // 2 * 2:2], mixed[1:count // 2 * 2:2]
    margin = jnp.minimum(tallies[source_of] - 1, most - tallies[sink]) // 2
    margin = jnp.where((source_of == ranking[0]) | (sink == ranking[0]) | (tallies[sink] == 0), 0, jnp.maximum(margin, 0))
    shifted = jax.random.randint(jax.random.fold_in(own, 4), (count // 2,), 0, 1 << 20) % (margin + 1)
    tallies = tallies.at[source_of].add(-shifted).at[sink].add(shifted)
    members = jnp.searchsorted(jnp.cumsum(tallies), jnp.arange(rows * top), side="right").astype(jnp.int32)
    listing = members.reshape(top, rows).T
    listing = listing[jax.random.permutation(jax.random.fold_in(own, 1), rows)]
    offset_by = jax.random.randint(jax.random.fold_in(own, 2), (rows, 1), 0, top)
    return jnp.take_along_axis(listing, (jnp.arange(top)[None, :] + offset_by) % top, axis=1)


def portions_of(amount, total, limit, lean, full):
    portions = [(1 << 20) // math.isqrt(grade ** lean) + 1 for grade in range(1, amount + 1)]
    largest = limit if full else min(limit, max(-(-total // amount), total * portions[0] // sum(portions)))
    least = 1 if total - largest >= amount - 1 else 0
    given, rest = [largest] + [least] * (amount - 1), total - largest - least * (amount - 1)
    while rest > 0:
        movable = [i for i in range(1, amount) if given[i] < largest] or [i for i in range(1, amount) if given[i] < limit]
        whole, remaining = sum([portions[i] for i in movable]), rest
        for i in movable:
            addition = min(limit - given[i], max(1, remaining * portions[i] // whole), rest)
            given[i] = given[i] + addition
            rest = rest - addition
    return np.array(given)


def gaussian(own_key, dims, deviation, bound, shards=(), held_as=jnp.bfloat16):
    result = deviation * jax.random.normal(own_key, dims, jnp.float32)
    if shards:
        result = result * block_levels(own_key, dims, shards, -0.22, 0.18)
    return jnp.clip(result, -bound, bound).astype(held_as)


def bell_draw_with(own_key, extent, width, limit, split, heavy, kind=jnp.bfloat16):
    values = width * jax.random.normal(own_key, extent, jnp.float32)
    if split:
        values = values * block_levels(own_key, extent, split, -0.22, 0.18)
    return jnp.clip(strengthened(values, jax.random.fold_in(own_key, 3), *heavy), -limit, limit).astype(kind)


def setup_inputs(seed: int = 0) -> dict:
    keys = jax.random.split(jax.random.key(seed), 8)
    tokens = gaussian(keys[0], (TOKENS, D), 1.0, 6.0, ((0, 8), (1, 16)))
    out_grad = gaussian(keys[1], (TOKENS, D), 1.0, 6.0, ((0, 8), (1, 16)))
    routing_ids_keys = jax.random.split(jax.random.fold_in(keys[2], 1), TOKENS // TOK_DEV)
    routing_ids_turns = jax.random.permutation(jax.random.fold_in(keys[2], 3), TOKENS // TOK_DEV)
    routing_ids = jax.vmap(lambda own, number: deal_out(jax.random.fold_in(keys[2], 2), own, number, TOK_DEV, EXPERTS, 2, CAP, 2))(routing_ids_keys, routing_ids_turns).reshape((TOKENS, 2))
    route_weights = jnp.clip(jnp.exp(math.log(1.0) - 2.9996462 * jax.random.uniform(keys[3], (TOKENS, 2), jnp.float32) ** block_levels(keys[3], (TOKENS, 2), ((0, 8),), -0.2, 0.2)), 0.049804688, 1.0).astype(jnp.bfloat16)
    gate_matrix = bell_draw_with(keys[4], (EXPERTS, D, FF), D ** -0.5, 0.125, ((0, 8), (2, 16)), (2, 1, 16, 2.0))
    up_matrix = gaussian(keys[5], (EXPERTS, D, FF), D ** -0.5, 0.09375, ((0, 8), (2, 16)))
    down_matrix = gaussian(keys[6], (EXPERTS, FF, D), FF ** -0.5, 0.0625, ((0, 8), (1, 16)))
    return {"tokens": tokens, "out_grad": out_grad, "routing_ids": routing_ids, "route_weights": route_weights, "gate_matrix": gate_matrix, "up_matrix": up_matrix, "down_matrix": down_matrix}


def contract(left, right, left_dim, right_dim):
    return lax.dot_general(left, right, (((left_dim,), (right_dim,)), ((), ())), preferred_element_type=jnp.float32)


def expert_pass(items):
    rows_in, rows_grad, rows_weight, gate_w, up_w, down_w = items
    gate = contract(rows_in, gate_w, 1, 0)
    upper = contract(rows_in, up_w, 1, 0)
    sig = jax.nn.sigmoid(gate)
    act = gate * sig
    weight_col = rows_weight.astype(jnp.float32)[:, None]
    hidden = (act * upper).astype(jnp.bfloat16)
    scaled = (act * upper * weight_col).astype(jnp.bfloat16)
    back = contract(rows_grad, down_w, 1, 1)
    route_part = jnp.sum(hidden.astype(jnp.float32) * back, axis=1)
    back_scaled = back * weight_col
    up_delta = (back_scaled * act).astype(jnp.bfloat16)
    gate_delta = (back_scaled * upper * sig * (1.0 + gate * (1.0 - sig))).astype(jnp.bfloat16)
    gate_out = contract(rows_in, gate_delta, 0, 0).astype(jnp.bfloat16)
    up_out = contract(rows_in, up_delta, 0, 0).astype(jnp.bfloat16)
    down_out = contract(scaled, rows_grad, 0, 0).astype(jnp.bfloat16)
    row_grads = (contract(gate_delta, gate_w, 1, 1) + contract(up_delta, up_w, 1, 1)).astype(jnp.bfloat16)
    return gate_out, up_out, down_out, row_grads, route_part


def reference(tokens, out_grad, routing_ids, route_weights, gate_matrix, up_matrix, down_matrix):
    blocks = N_TOK
    expert_count = EXPERTS
    flat = routing_ids.reshape(blocks, -1).astype(jnp.int32)
    choices = flat.shape[1]
    onehot = (flat[:, :, None] == jnp.arange(expert_count, dtype=jnp.int32)[None, None, :]).astype(jnp.int32)
    position = jnp.sum((jnp.cumsum(onehot, axis=1) - onehot) * onehot, axis=2)
    block_ids = jnp.arange(blocks, dtype=jnp.int32)[:, None]
    table_row = (flat * (blocks * CAP) + block_ids * CAP + position).reshape(-1).astype(jnp.int32)
    total = blocks * choices
    table_size = expert_count * blocks * CAP
    source = jnp.full((table_size,), total, jnp.int32).at[table_row].set(jnp.arange(total, dtype=jnp.int32))
    valid = source < total
    clipped = jnp.minimum(source, total - 1)
    token_row = clipped // 2
    rows_in = jnp.where(valid[:, None], tokens[token_row], jnp.zeros((), jnp.bfloat16))
    rows_grad = jnp.where(valid[:, None], out_grad[token_row], jnp.zeros((), jnp.bfloat16))
    rows_weight = jnp.where(valid, route_weights.reshape(-1)[clipped], jnp.zeros((), jnp.bfloat16))
    per = blocks * CAP
    gate_out, up_out, down_out, row_grads, route_part = lax.map(
        expert_pass,
        (rows_in.reshape(expert_count, per, -1), rows_grad.reshape(expert_count, per, -1),
         rows_weight.reshape(expert_count, per), gate_matrix, up_matrix, down_matrix))
    row_grads = row_grads.reshape(table_size, -1)
    picked = row_grads[table_row].astype(jnp.float32)
    input_grad = jnp.sum(picked.reshape(total // 2, 2, -1), axis=1).astype(jnp.bfloat16)
    route_grad = route_part.reshape(-1)[table_row].astype(jnp.bfloat16).reshape(total // 2, 2)
    return input_grad, route_grad, gate_out, up_out, down_out
```

```python
import jax
import jax.numpy as jnp
from jax import lax
from jax.experimental import pallas as pl
from jax.experimental.pallas import tpu as pltpu
from jax.sharding import PartitionSpec as P

BF = jnp.bfloat16
F32 = jnp.float32
I32 = jnp.int32
NT = 8
NH = 16
SIGN = (1, -1)


def dot(a, b):
    return lax.dot_general(a, b, (((1,), (0,)), ((), ())), preferred_element_type=F32)


def dot_nt(a, b):
    return lax.dot_general(a, b, (((1,), (1,)), ((), ())), preferred_element_type=F32)


def m4(v):
    return lax.rem(v + 8, 4)


def pick(index, values):
    out = values[-1]
    for k in range(len(values) - 2, -1, -1):
        out = jnp.where(index == k, values[k], out)
    return out


def loop(lo, hi, body):
    def step(i, carry):
        body(i)
        return carry

    lax.fori_loop(lo, hi, step, 0)


def exchange(
    ids_ref, rw_ref, tok_ref, og_ref, wg_hbm, wu_hbm, wd_hbm,
    ig_ref, rg_ref, xt_out, g_out, d_out, hpt_out,
    wg, wu, wd, sel, selt, pack, psend, precv, xg, xt, acc_g, acc_u, acc_r,
    dd, hp, hpt, qs, qr, qt, qb,
    eb, rl1s, rl1r, fn1s, fn1r, rl2s, rl2r, fn2s, fn2r, shr, rb,
    w_sem, o_sem, zs, zr, gs, gr, r1s, r1r, f1s, f1r, r2s, r2r, f2s, f2r,
    qss, qsr, bs, br, cs, cr,
):
    t = lax.axis_index("tok")
    hid = lax.axis_index("hid")
    cx = lax.div(hid, 4)
    cy = lax.rem(hid, 4)
    cap = sel.shape[1]
    rows = NT * cap
    fb = xg.shape[-1]
    hu = wg.shape[-1]

    def to_hid(src, dst, ssem, rsem, target):
        return pltpu.make_async_remote_copy(
            src_ref=src, dst_ref=dst, send_sem=ssem, recv_sem=rsem,
            device_id={"hid": target}, device_id_type=pl.DeviceIdType.MESH,
        )

    def to_tok(src, dst, ssem, rsem, target):
        return pltpu.make_async_remote_copy(
            src_ref=src, dst_ref=dst, send_sem=ssem, recv_sem=rsem,
            device_id={"tok": target}, device_id_type=pl.DeviceIdType.MESH,
        )

    bar = pltpu.get_barrier_semaphore()
    loop(1, NT, lambda k: pl.semaphore_signal(
        bar, inc=1, device_id={"tok": lax.rem(t + k, NT)}, device_id_type=pl.DeviceIdType.MESH))
    loop(1, NH, lambda k: pl.semaphore_signal(
        bar, inc=1, device_id={"hid": lax.rem(hid + k, NH)}, device_id_type=pl.DeviceIdType.MESH))

    w_copies = [
        pltpu.make_async_copy(wg_hbm, wg, w_sem.at[0]),
        pltpu.make_async_copy(wu_hbm, wu, w_sem.at[1]),
        pltpu.make_async_copy(wd_hbm, wd, w_sem.at[2]),
    ]
    for c in w_copies:
        c.start()

    n_tok = tok_ref.shape[0]
    ids = ids_ref[...]
    rw = rw_ref[...].astype(F32)
    expert = lax.broadcasted_iota(I32, (NT, n_tok), 0)
    first = ids[0:1, :] == expert
    second = ids[1:2, :] == expert
    named = jnp.where(first, 1.0, 0.0) + jnp.where(second, 1.0, 0.0)
    weight = jnp.where(first, rw[0:1, :], 0.0) + jnp.where(second, rw[1:2, :], 0.0)
    earlier = (
        lax.broadcasted_iota(I32, (n_tok, n_tok), 0) < lax.broadcasted_iota(I32, (n_tok, n_tok), 1)
    )
    place = dot(named.astype(BF), jnp.where(earlier, 1.0, 0.0).astype(BF))
    code = jnp.where(named > 0.5, place, -1.0).astype(I32)
    slot = lax.broadcasted_iota(I32, (cap, n_tok), 0)
    lane = lax.broadcasted_iota(I32, (cap, n_tok), 1)
    diag = slot == lane
    for e in range(NT):
        one = jnp.where(slot == code[e : e + 1, :], 1.0, 0.0)
        sel[e] = one
        col = jnp.sum(one * weight[e : e + 1, :], axis=1, keepdims=True)
        row = jnp.sum(jnp.where(diag, col, 0.0), axis=0, keepdims=True)
        psend[e] = jnp.broadcast_to(row, (8, n_tok))
    picks = sel[...].reshape(rows, n_tok)
    picks_bf = picks.astype(BF)
    pack[0] = dot(picks_bf, tok_ref[...]).astype(BF).reshape(NT, cap, fb)
    pack[1] = dot(picks_bf, og_ref[...]).astype(BF).reshape(NT, cap, fb)
    xg[0, hid, t] = pack[0, t]
    xg[1, hid, t] = pack[1, t]
    precv[t] = psend[t]

    pl.semaphore_wait(bar, NT - 1 + NH - 1)

    def z_send(a, k):
        to = lax.rem(t + k, NT)
        return to_tok(pack.at[a, to], xg.at[a, hid, t], zs.at[a, k], zr.at[a, k], to)

    def p_send(k):
        to = lax.rem(t + k, NT)
        return to_tok(psend.at[to], precv.at[t], zs.at[2, k], zr.at[2, k], to)

    def z_recv(a, k):
        frm = lax.rem(t + NT - k, NT)
        return to_tok(pack.at[a, frm], xg.at[a, hid, frm], zs.at[a, k], zr.at[a, k], frm)

    def p_recv(k):
        frm = lax.rem(t + NT - k, NT)
        return to_tok(psend.at[frm], precv.at[frm], zs.at[2, k], zr.at[2, k], frm)

    loop(1, NT, lambda k: z_send(0, k).start())
    loop(1, NT, lambda k: z_send(1, k).start())
    loop(1, NT, lambda k: p_send(k).start())

    prim = (cx, cy)
    seco = (cy, cx)

    def blk(a, p, s):
        return 4 * p + s if a == 0 else 4 * s + p

    half = NT // 2

    def gather_copy(a, block, h, sem, target):
        ref = xg.at[a, block] if h is None else xg.at[a, block, pl.ds(h * half, half)]
        return to_hid(ref, ref, gs.at[a, sem], gr.at[a, sem], target)

    def p_own(a, d, recv=False):
        p, s = prim[a], seco[a]
        b = blk(a, m4(p - SIGN[d]) if recv else p, s)
        return gather_copy(a, b, None, d, blk(a, m4(p + SIGN[d]), s))

    def p_fwd(a, d, recv=False):
        p, s = prim[a], seco[a]
        b = blk(a, m4(p - 2 * SIGN[d]) if recv else m4(p - SIGN[d]), s)
        return gather_copy(a, b, d, 2 + d, blk(a, m4(p + SIGN[d]), s))

    def s_own(a, o, d, recv=False):
        p, s = prim[a], seco[a]
        b = blk(a, m4(p + o), m4(s - SIGN[d]) if recv else s)
        return gather_copy(a, b, None, 4 + 2 * o + d, blk(a, p, m4(s + SIGN[d])))

    def s_fwd(a, o, d, recv=False):
        p, s = prim[a], seco[a]
        b = blk(a, m4(p + o), m4(s - 2 * SIGN[d]) if recv else m4(s - SIGN[d]))
        return gather_copy(a, b, d, 12 + 2 * o + d, blk(a, p, m4(s + SIGN[d])))

    for a in range(2):
        loop(1, NT, lambda k: z_recv(a, k).wait_recv())
        for d in range(2):
            p_own(a, d).start()
            s_own(a, 0, d).start()
    loop(1, NT, lambda k: p_recv(k).wait_recv())

    acc_g[...] = jnp.zeros_like(acc_g)
    acc_u[...] = jnp.zeros_like(acc_u)
    acc_r[...] = jnp.zeros_like(acc_r)
    selt[...] = picks.T
    for c in w_copies:
        c.wait()

    o_of = (0, 3, 1, 0, 0, 2, 3, 3, 1, 1, 2, 2, 0, 3, 1, 2)
    q_of = (0, 0, 0, 3, 1, 0, 3, 1, 3, 1, 3, 1, 2, 2, 2, 2)

    def gather_step(j):
        @pl.when(j == 1)
        def _():
            for a in range(2):
                for d in range(2):
                    p_own(a, d, True).wait_recv()
                    p_fwd(a, d).start()
                    for d2 in range(2):
                        s_own(a, (4 - SIGN[d]) % 4, d2).start()
                for d in range(2):
                    s_own(a, 0, d, True).wait_recv()
                    s_fwd(a, 0, d).start()

        @pl.when(j == 5)
        def _():
            for a in range(2):
                for d in range(2):
                    p_fwd(a, d, True).wait_recv()
                for d in range(2):
                    s_own(a, 2, d).start()

        @pl.when(j == 6)
        def _():
            for a in range(2):
                for o in (3, 1):
                    for d in range(2):
                        s_own(a, o, d, True).wait_recv()
                        s_fwd(a, o, d).start()

        @pl.when(j == 10)
        def _():
            for a in range(2):
                for d in range(2):
                    s_own(a, 2, d, True).wait_recv()
                    s_fwd(a, 2, d).start()

        for n, o in ((12, 0), (13, 3), (14, 1), (15, 2)):
            @pl.when(j == n)
            def _():
                for a in range(2):
                    for d in range(2):
                        s_fwd(a, o, d, True).wait_recv()

        o = pick(j, o_of)
        q = pick(j, q_of)
        bx = blk(0, m4(cx + o), m4(cy + q))
        bg = blk(1, m4(cy + o), m4(cx + q))
        x = xg[0, bx].reshape(rows, fb)
        acc_g[...] += dot(x, wg[bx])
        acc_u[...] += dot(x, wu[bx])
        acc_r[...] += dot_nt(xg[1, bg].reshape(rows, fb), wd[:, pl.ds(pl.multiple_of(bg * fb, fb), fb)])
        xt[bx] = x.T

    loop(0, NH, gather_step)

    out_x = pltpu.make_async_copy(xt, xt_out, o_sem.at[0])
    out_g = pltpu.make_async_copy(xg.at[1], g_out, o_sem.at[1])
    out_x.start()
    out_g.start()

    def deltas(b):
        at = pl.ds(pl.multiple_of(b * cap, cap), cap)
        g = acc_g[at, :]
        u = acc_u[at, :]
        r = acc_r[at, :]
        p = jnp.sum(jnp.where(diag, precv[b, 0:1, :], 0.0), axis=1, keepdims=True)
        s = 1.0 / (1.0 + jnp.exp(-g))
        act = g * s
        au = act * u
        hp[at, :] = (au * p).astype(BF)
        q = jnp.sum(au.astype(BF).astype(F32) * r, axis=1, keepdims=True)
        qs[pl.ds(b, 1), :] = jnp.sum(jnp.where(diag, q, 0.0), axis=0, keepdims=True)
        rp = r * p
        dd[at, 0:hu] = (rp * u * s * (1.0 + g * (1.0 - s))).astype(BF)
        dd[at, hu : 2 * hu] = (rp * act).astype(BF)

    loop(0, NT, deltas)

    hrows = rows // 2

    def dprim(a):
        return cx + a * (cy - cx)

    def dseco(a):
        return cy + a * (cx - cy)

    def dblk(a, p, s):
        return (4 * p + s) + a * (3 * s - 3 * p)

    def eblock(a, h):
        at = pl.ds(pl.multiple_of(a * hrows, hrows), hrows)
        return dot_nt(dd[at, 0:hu], wg[h]) + dot_nt(dd[at, hu : 2 * hu], wu[h])

    def rl1(a, d, i):
        return to_hid(rl1s.at[a, d, i], rl1r.at[a, d, i], r1s.at[a, d, i], r1r.at[a, d, i],
                      dblk(a, m4(dprim(a) + 1 - 2 * d), dseco(a)))

    def fn1(a, d, q):
        return to_hid(fn1s.at[a, d, q], fn1r.at[a, d, q], f1s.at[a, d, q], f1r.at[a, d, q],
                      dblk(a, m4(dprim(a) + 1 - 2 * d), dseco(a)))

    def rl2(a, d):
        return to_hid(rl2s.at[a, d], rl2r.at[a, d], r2s.at[a, d], r2r.at[a, d],
                      dblk(a, dprim(a), m4(dseco(a) + 1 - 2 * d)))

    def fn2(a, d):
        return to_hid(fn2s.at[a, d], fn2r.at[a, d], f2s.at[a, d], f2r.at[a, d],
                      dblk(a, dprim(a), m4(dseco(a) + 1 - 2 * d)))

    def relay_step(n):
        a = lax.rem(n, 2)
        d = lax.rem(lax.div(n, 2), 2)
        i = lax.div(n, 4)
        q = 2 - i + d * (1 - 2 * i)
        e = eblock(a, dblk(a, m4(dprim(a) + 2), m4(dseco(a) + q)))
        rl1s[a, d, i] = e.astype(BF)
        rl1(a, d, i).start()

    loop(0, 8, relay_step)

    def q_send(k):
        to = lax.rem(hid + k, NH)
        return to_hid(qs, qr.at[hid], qss.at[k], qsr.at[k], to)

    def q_recv(k):
        frm = lax.rem(hid + NH - k, NH)
        return to_hid(qs, qr.at[frm], qss.at[k], qsr.at[k], frm)

    qr[hid] = qs[...]
    loop(1, NH, lambda k: q_send(k).start())

    q_order = (2, 3, 1, 0)

    def first_step(n):
        a = lax.rem(n, 2)
        d = lax.rem(lax.div(n, 2), 2)
        q = pick(lax.div(n, 4), q_order)
        in_first = jnp.where(d == 0, jnp.where((q == 2) | (q == 1), 1, 0),
                             jnp.where((q == 3) | (q == 0), 1, 0))
        i = jnp.where(d == 0, 2 - q, lax.div(3 - q, 3))
        e = eblock(a, dblk(a, m4(dprim(a) + 1 - 2 * d), m4(dseco(a) + q)))
        eb[...] = e.reshape(2, hrows // 2, fb)

        @pl.when(in_first == 1)
        def _():
            rl1(a, d, i).wait_recv()
            eb[...] += rl1r[a, d, i].astype(F32).reshape(2, hrows // 2, fb)

        fn1s[a, d, q] = eb[...].astype(BF).reshape(hrows, fb)
        fn1(a, d, q).start()

    loop(0, 16, first_step)

    hpt[...] = hp[...].T
    out_h = pltpu.make_async_copy(hpt, hpt_out, o_sem.at[2])
    out_d = pltpu.make_async_copy(dd, d_out, o_sem.at[3])
    out_h.start()
    out_d.start()

    loop(1, NH, lambda k: q_recv(k).wait_recv())
    total = qr[0]
    for h in range(1, NH):
        total = total + qr[h]
    qt[...] = total
    qb[t] = total

    def c_send(k):
        to = lax.rem(t + k, NT)
        return to_tok(qt, qb.at[t], cs.at[k], cr.at[k], to)

    def c_recv(k):
        frm = lax.rem(t + NT - k, NT)
        return to_tok(qt, qb.at[frm], cs.at[k], cr.at[k], frm)

    loop(1, NT, lambda k: c_send(k).start())

    def b_send(b):
        k = lax.rem(b - t + NT, NT)
        return to_tok(shr.at[b], rb.at[t], bs.at[k], br.at[k], b)

    def b_recv(k):
        frm = lax.rem(t + NT - k, NT)
        return to_tok(shr.at[frm], rb.at[frm], bs.at[k], br.at[k], frm)

    def second_step(n):
        a = lax.rem(n, 2)
        q = pick(lax.div(n, 2), q_order)
        e = eblock(a, dblk(a, dprim(a), m4(dseco(a) + q)))
        eb[...] = e.reshape(2, hrows // 2, fb)
        for d in range(2):
            fn1(a, d, q).wait_recv()
        eb[...] += (fn1r[a, 0, q].astype(F32) + fn1r[a, 1, q].astype(F32)).reshape(
            2, hrows // 2, fb)

        @pl.when(q == 2)
        def _():
            for d in range(2):
                rl2s[a, d] = eb[d].astype(BF)
                rl2(a, d).start()

        for d, at in ((0, 1), (1, 3)):
            @pl.when(q == at)
            def _():
                rl2(a, d).wait_recv()
                eb[d] += rl2r[a, d].astype(F32)
                fn2s[a, d] = eb[...].astype(BF)
                fn2(a, d).start()

        @pl.when(q == 0)
        def _():
            for d in range(2):
                fn2(a, d).wait_recv()
            s = eb[...] + fn2r[a, 0].astype(F32) + fn2r[a, 1].astype(F32)
            shr[pl.ds(a * half, half)] = s.astype(BF).reshape(half, cap, fb)
            for i in range(half):
                b = a * half + i

                @pl.when(b != t)
                def _():
                    b_send(b).start()

                @pl.when(b == t)
                def _():
                    rb[t] = shr[t]

    loop(0, 8, second_step)

    loop(1, NT, lambda k: c_recv(k).wait_recv())
    block = lax.broadcasted_iota(I32, (8, n_tok), 0)
    zero = jnp.zeros((1, n_tok), F32)
    route = [zero, zero]
    for e in range(NT):
        row = jnp.sum(jnp.where(block == t, qb[e], 0.0), axis=0, keepdims=True)
        col = jnp.sum(jnp.where(diag, row, 0.0), axis=1, keepdims=True)
        val = jnp.sum(sel[e] * col, axis=0, keepdims=True)
        for k in range(2):
            route[k] = route[k] + jnp.where(ids[k : k + 1, :] == e, val, 0.0)
    rg_ref[...] = jnp.concatenate(route, axis=0).astype(BF)

    loop(1, NT, lambda k: b_recv(k).wait_recv())
    ig_ref[...] = dot(selt[...].astype(BF), rb[...].reshape(rows, fb)).astype(BF)

    def drain_tok(k):
        for a in range(2):
            z_send(a, k).wait_send()
        p_send(k).wait_send()
        c_send(k).wait_send()
        b_send(lax.rem(t + k, NT)).wait_send()

    loop(1, NT, drain_tok)
    loop(1, NH, lambda k: q_send(k).wait_send())
    for a in range(2):
        for d in range(2):
            p_own(a, d).wait_send()
            p_fwd(a, d).wait_send()
            for o in range(4):
                s_own(a, o, d).wait_send()
                s_fwd(a, o, d).wait_send()
            for i in range(2):
                rl1(a, d, i).wait_send()
            for q in range(4):
                fn1(a, d, q).wait_send()
            rl2(a, d).wait_send()
            fn2(a, d).wait_send()
    out_x.wait()
    out_g.wait()
    out_h.wait()
    out_d.wait()


def weight_grads(xt_ref, d_ref, hpt_ref, g_ref, gate_ref, up_ref, down_ref):
    hu = gate_ref.shape[1]
    xt = xt_ref[0]
    gate_ref[...] = dot(xt, d_ref[:, 0:hu]).astype(BF)
    up_ref[...] = dot(xt, d_ref[:, hu : 2 * hu]).astype(BF)
    down_ref[...] = dot(hpt_ref[...], g_ref[0]).astype(BF)


def per_device(tokens, out_grad, routing_ids, route_weights, gate_matrix, up_matrix, down_matrix):
    n_tok, fb = tokens.shape
    cap = 3 * n_tok // NT
    rows = NT * cap
    hu = gate_matrix.shape[2]
    width = gate_matrix.shape[1]
    hr = rows // 2
    vmem = pltpu.VMEM
    dma = pltpu.SemaphoreType.DMA
    any_spec = pl.BlockSpec(memory_space=pl.ANY)
    vm_spec = pl.BlockSpec(memory_space=pltpu.VMEM)
    ig, rg, xt, g, dd, hpt = pl.pallas_call(
        exchange,
        name="exchange",
        out_shape=(
            jax.ShapeDtypeStruct((n_tok, fb), BF),
            jax.ShapeDtypeStruct((2, n_tok), BF),
            jax.ShapeDtypeStruct((NH, fb, rows), BF),
            jax.ShapeDtypeStruct((NH, NT, cap, fb), BF),
            jax.ShapeDtypeStruct((rows, 2 * hu), BF),
            jax.ShapeDtypeStruct((hu, rows), BF),
        ),
        in_specs=[vm_spec] * 4 + [any_spec] * 3,
        out_specs=(vm_spec, vm_spec, any_spec, any_spec, any_spec, any_spec),
        scratch_shapes=[
            vmem((NH, fb, hu), BF), vmem((NH, fb, hu), BF), vmem((hu, width), BF),
            vmem((NT, cap, n_tok), F32), vmem((n_tok, rows), F32),
            vmem((2, NT, cap, fb), BF), vmem((NT, 8, n_tok), F32), vmem((NT, 8, n_tok), F32),
            vmem((2, NH, NT, cap, fb), BF), vmem((NH, fb, rows), BF),
            vmem((rows, hu), F32), vmem((rows, hu), F32), vmem((rows, hu), F32),
            vmem((rows, 2 * hu), BF), vmem((rows, hu), BF), vmem((hu, rows), BF),
            vmem((8, n_tok), F32), vmem((NH, 8, n_tok), F32), vmem((8, n_tok), F32),
            vmem((NT, 8, n_tok), F32),
            vmem((2, hr // 2, fb), F32),
            vmem((2, 2, 2, hr, fb), BF), vmem((2, 2, 2, hr, fb), BF),
            vmem((2, 2, 4, hr, fb), BF), vmem((2, 2, 4, hr, fb), BF),
            vmem((2, 2, hr // 2, fb), BF), vmem((2, 2, hr // 2, fb), BF),
            vmem((2, 2, 2, hr // 2, fb), BF), vmem((2, 2, 2, hr // 2, fb), BF),
            vmem((NT, cap, fb), BF), vmem((NT, cap, fb), BF),
            dma((3,)), dma((4,)),
            dma((3, NT)), dma((3, NT)),
            dma((2, 20)), dma((2, 20)),
            dma((2, 2, 2)), dma((2, 2, 2)),
            dma((2, 2, 4)), dma((2, 2, 4)),
            dma((2, 2)), dma((2, 2)),
            dma((2, 2)), dma((2, 2)),
            dma((NH,)), dma((NH,)),
            dma((NT,)), dma((NT,)),
            dma((NT,)), dma((NT,)),
        ],
        compiler_params=pltpu.CompilerParams(
            collective_id=0, has_side_effects=True, vmem_limit_bytes=52 * 1024 * 1024
        ),
    )(
        routing_ids.T, route_weights.T, tokens, out_grad,
        gate_matrix.reshape(NH, fb, hu), up_matrix.reshape(NH, fb, hu), down_matrix[0],
    )
    gate_out, up_out, down_out = pl.pallas_call(
        weight_grads,
        name="weight_grads",
        grid=(NH,),
        out_shape=(
            jax.ShapeDtypeStruct((width, hu), BF),
            jax.ShapeDtypeStruct((width, hu), BF),
            jax.ShapeDtypeStruct((hu, width), BF),
        ),
        in_specs=[
            pl.BlockSpec((1, fb, rows), lambda i: (i, 0, 0)),
            pl.BlockSpec((rows, 2 * hu), lambda i: (0, 0)),
            pl.BlockSpec((hu, rows), lambda i: (0, 0)),
            pl.BlockSpec((1, rows, fb), lambda i: (i, 0, 0)),
        ],
        out_specs=(
            pl.BlockSpec((fb, hu), lambda i: (i, 0)),
            pl.BlockSpec((fb, hu), lambda i: (i, 0)),
            pl.BlockSpec((hu, fb), lambda i: (0, i)),
        ),
        compiler_params=pltpu.CompilerParams(vmem_limit_bytes=24 * 1024 * 1024),
    )(xt, dd, hpt, g.reshape(NH, rows, fb))
    return (ig, rg.T, gate_out[None], up_out[None], down_out[None])


def solution(mesh):
    in_specs = (
        P("tok", "hid"),
        P("tok", "hid"),
        P("tok", None),
        P("tok", None),
        P("tok", None, "hid"),
        P("tok", None, "hid"),
        P("tok", "hid", None),
    )
    out_specs = (
        P("tok", "hid"),
        P("tok", None),
        P("tok", None, "hid"),
        P("tok", None, "hid"),
        P("tok", "hid", None),
    )
    return jax.shard_map(
        per_device, mesh=mesh, in_specs=in_specs, out_specs=out_specs, check_vma=False
    )
```

```python
import jax
import jax.numpy as jnp
from jax import lax
from jax.experimental import pallas as pl
from jax.experimental.pallas import tpu as pltpu
from jax.sharding import PartitionSpec as P

BF = jnp.bfloat16
F32 = jnp.float32
I32 = jnp.int32
NT = 8
NH = 16
SIGN = (1, -1)


def dot(a, b):
    return lax.dot_general(a, b, (((1,), (0,)), ((), ())), preferred_element_type=F32)


def dot_nt(a, b):
    return lax.dot_general(a, b, (((1,), (1,)), ((), ())), preferred_element_type=F32)


def m4(v):
    return lax.rem(v + 8, 4)


def pick(index, values):
    out = values[-1]
    for k in range(len(values) - 2, -1, -1):
        out = jnp.where(index == k, values[k], out)
    return out


def loop(lo, hi, body):
    def step(i, carry):
        body(i)
        return carry

    lax.fori_loop(lo, hi, step, 0)


def exchange(
    ids_hbm, rw_hbm, tok_hbm, og_hbm, wg_hbm, wu_hbm, wd_hbm,
    ig_ref, rg_ref, gate_ref, up_ref, down_ref,
    ids_ref, rw_ref, tok_ref, og_ref, wg, wu, wd, sel, selt, pack, psend, precv, xg, xt, acc_g, acc_u, acc_r,
    dd, hp, hpt, qs, qr, qt, qb,
    eb, rl1s, rl1r, fn1s, fn1r, rl2s, rl2r, fn2s, fn2r, shr, rb,
    w_sem, zs, zr, gs, gr, r1s, r1r, f1s, f1r, r2s, r2r, f2s, f2r,
    qss, qsr, bs, br, cs, cr,
):
    t = lax.axis_index("tok")
    hid = lax.axis_index("hid")
    cx = lax.div(hid, 4)
    cy = lax.rem(hid, 4)
    cap = sel.shape[1]
    rows = NT * cap
    fb = xg.shape[-1]
    hu = wg.shape[-1]

    def to_hid(src, dst, ssem, rsem, target):
        return pltpu.make_async_remote_copy(
            src_ref=src, dst_ref=dst, send_sem=ssem, recv_sem=rsem,
            device_id={"hid": target}, device_id_type=pl.DeviceIdType.MESH,
        )

    def to_tok(src, dst, ssem, rsem, target):
        return pltpu.make_async_remote_copy(
            src_ref=src, dst_ref=dst, send_sem=ssem, recv_sem=rsem,
            device_id={"tok": target}, device_id_type=pl.DeviceIdType.MESH,
        )

    small = [
        pltpu.make_async_copy(src, dst, w_sem.at[3 + k])
        for k, (src, dst) in enumerate(
            ((ids_hbm, ids_ref), (rw_hbm, rw_ref), (tok_hbm, tok_ref), (og_hbm, og_ref))
        )
    ]
    for c in small:
        c.start()

    bar = pltpu.get_barrier_semaphore()
    loop(1, NT, lambda k: pl.semaphore_signal(
        bar, inc=1, device_id={"tok": lax.rem(t + k, NT)}, device_id_type=pl.DeviceIdType.MESH))
    loop(1, NH, lambda k: pl.semaphore_signal(
        bar, inc=1, device_id={"hid": lax.rem(hid + k, NH)}, device_id_type=pl.DeviceIdType.MESH))

    w_copies = [
        pltpu.make_async_copy(wg_hbm, wg, w_sem.at[0]),
        pltpu.make_async_copy(wu_hbm, wu, w_sem.at[1]),
        pltpu.make_async_copy(wd_hbm, wd, w_sem.at[2]),
    ]
    for c in w_copies:
        c.start()

    for c in small:
        c.wait()

    n_tok = tok_ref.shape[0]
    ids = ids_ref[...]
    rw = rw_ref[...].astype(F32)
    expert = lax.broadcasted_iota(I32, (NT, n_tok), 0)
    first = ids[0:1, :] == expert
    second = ids[1:2, :] == expert
    named = jnp.where(first, 1.0, 0.0) + jnp.where(second, 1.0, 0.0)
    weight = jnp.where(first, rw[0:1, :], 0.0) + jnp.where(second, rw[1:2, :], 0.0)
    earlier = (
        lax.broadcasted_iota(I32, (n_tok, n_tok), 0) < lax.broadcasted_iota(I32, (n_tok, n_tok), 1)
    )
    place = dot(named.astype(BF), jnp.where(earlier, 1.0, 0.0).astype(BF))
    code = jnp.where(named > 0.5, place, -1.0).astype(I32)
    slot = lax.broadcasted_iota(I32, (cap, n_tok), 0)
    lane = lax.broadcasted_iota(I32, (cap, n_tok), 1)
    diag = slot == lane
    for e in range(NT):
        one = jnp.where(slot == code[e : e + 1, :], 1.0, 0.0)
        sel[e] = one
        col = jnp.sum(one * weight[e : e + 1, :], axis=1, keepdims=True)
        row = jnp.sum(jnp.where(diag, col, 0.0), axis=0, keepdims=True)
        psend[e] = jnp.broadcast_to(row, (8, n_tok))
    picks = sel[...].reshape(rows, n_tok)
    picks_bf = picks.astype(BF)
    pack[0] = dot(picks_bf, tok_ref[...]).astype(BF).reshape(NT, cap, fb)
    pack[1] = dot(picks_bf, og_ref[...]).astype(BF).reshape(NT, cap, fb)
    xg[0, hid, t] = pack[0, t]
    xg[1, hid, t] = pack[1, t]
    precv[t] = psend[t]

    pl.semaphore_wait(bar, NT - 1 + NH - 1)

    def z_send(a, k):
        to = lax.rem(t + k, NT)
        return to_tok(pack.at[a, to], xg.at[a, hid, t], zs.at[a, k], zr.at[a, k], to)

    def p_send(k):
        to = lax.rem(t + k, NT)
        return to_tok(psend.at[to], precv.at[t], zs.at[2, k], zr.at[2, k], to)

    def z_recv(a, k):
        frm = lax.rem(t + NT - k, NT)
        return to_tok(pack.at[a, frm], xg.at[a, hid, frm], zs.at[a, k], zr.at[a, k], frm)

    def p_recv(k):
        frm = lax.rem(t + NT - k, NT)
        return to_tok(psend.at[frm], precv.at[frm], zs.at[2, k], zr.at[2, k], frm)

    loop(1, NT, lambda k: z_send(0, k).start())
    loop(1, NT, lambda k: z_send(1, k).start())
    loop(1, NT, lambda k: p_send(k).start())

    prim = (cx, cy)
    seco = (cy, cx)

    def blk(a, p, s):
        return 4 * p + s if a == 0 else 4 * s + p

    half = NT // 2

    def gather_copy(a, block, h, sem, target):
        ref = xg.at[a, block] if h is None else xg.at[a, block, pl.ds(h * half, half)]
        return to_hid(ref, ref, gs.at[a, sem], gr.at[a, sem], target)

    def p_own(a, d, recv=False):
        p, s = prim[a], seco[a]
        b = blk(a, m4(p - SIGN[d]) if recv else p, s)
        return gather_copy(a, b, None, d, blk(a, m4(p + SIGN[d]), s))

    def p_fwd(a, d, recv=False):
        p, s = prim[a], seco[a]
        b = blk(a, m4(p - 2 * SIGN[d]) if recv else m4(p - SIGN[d]), s)
        return gather_copy(a, b, d, 2 + d, blk(a, m4(p + SIGN[d]), s))

    def s_own(a, o, d, recv=False):
        p, s = prim[a], seco[a]
        b = blk(a, m4(p + o), m4(s - SIGN[d]) if recv else s)
        return gather_copy(a, b, None, 4 + 2 * o + d, blk(a, p, m4(s + SIGN[d])))

    def s_fwd(a, o, d, recv=False):
        p, s = prim[a], seco[a]
        b = blk(a, m4(p + o), m4(s - 2 * SIGN[d]) if recv else m4(s - SIGN[d]))
        return gather_copy(a, b, d, 12 + 2 * o + d, blk(a, p, m4(s + SIGN[d])))

    for a in range(2):
        loop(1, NT, lambda k: z_recv(a, k).wait_recv())
        for d in range(2):
            p_own(a, d).start()
            s_own(a, 0, d).start()
    loop(1, NT, lambda k: p_recv(k).wait_recv())

    acc_g[...] = jnp.zeros_like(acc_g)
    acc_u[...] = jnp.zeros_like(acc_u)
    acc_r[...] = jnp.zeros_like(acc_r)
    selt[...] = picks.T
    for c in w_copies:
        c.wait()

    o_of = (0, 3, 1, 0, 0, 2, 3, 3, 1, 1, 2, 2, 0, 3, 1, 2)
    q_of = (0, 0, 0, 3, 1, 0, 3, 1, 3, 1, 3, 1, 2, 2, 2, 2)

    def gather_step(j):
        @pl.when(j == 1)
        def _():
            for a in range(2):
                for d in range(2):
                    p_own(a, d, True).wait_recv()
                    p_fwd(a, d).start()
                    for d2 in range(2):
                        s_own(a, (4 - SIGN[d]) % 4, d2).start()
                for d in range(2):
                    s_own(a, 0, d, True).wait_recv()
                    s_fwd(a, 0, d).start()

        @pl.when(j == 5)
        def _():
            for a in range(2):
                for d in range(2):
                    p_fwd(a, d, True).wait_recv()
                for d in range(2):
                    s_own(a, 2, d).start()

        @pl.when(j == 6)
        def _():
            for a in range(2):
                for o in (3, 1):
                    for d in range(2):
                        s_own(a, o, d, True).wait_recv()
                        s_fwd(a, o, d).start()

        @pl.when(j == 10)
        def _():
            for a in range(2):
                for d in range(2):
                    s_own(a, 2, d, True).wait_recv()
                    s_fwd(a, 2, d).start()

        for n, o in ((12, 0), (13, 3), (14, 1), (15, 2)):
            @pl.when(j == n)
            def _():
                for a in range(2):
                    for d in range(2):
                        s_fwd(a, o, d, True).wait_recv()

        o = pick(j, o_of)
        q = pick(j, q_of)
        bx = blk(0, m4(cx + o), m4(cy + q))
        bg = blk(1, m4(cy + o), m4(cx + q))
        x = xg[0, bx].reshape(rows, fb)
        acc_g[...] += dot(x, wg[bx])
        acc_u[...] += dot(x, wu[bx])
        acc_r[...] += dot_nt(xg[1, bg].reshape(rows, fb), wd[:, pl.ds(pl.multiple_of(bg * fb, fb), fb)])
        xt[bx] = x.T

    loop(0, NH, gather_step)

    def deltas(b):
        at = pl.ds(pl.multiple_of(b * cap, cap), cap)
        g = acc_g[at, :]
        u = acc_u[at, :]
        r = acc_r[at, :]
        p = jnp.sum(jnp.where(diag, precv[b, 0:1, :], 0.0), axis=1, keepdims=True)
        s = 1.0 / (1.0 + jnp.exp(-g))
        act = g * s
        au = act * u
        hp[at, :] = (au * p).astype(BF)
        q = jnp.sum(au.astype(BF).astype(F32) * r, axis=1, keepdims=True)
        qs[pl.ds(b, 1), :] = jnp.sum(jnp.where(diag, q, 0.0), axis=0, keepdims=True)
        rp = r * p
        dd[at, 0:hu] = (rp * u * s * (1.0 + g * (1.0 - s))).astype(BF)
        dd[at, hu : 2 * hu] = (rp * act).astype(BF)

    loop(0, NT, deltas)

    hrows = rows // 2

    def dprim(a):
        return cx + a * (cy - cx)

    def dseco(a):
        return cy + a * (cx - cy)

    def dblk(a, p, s):
        return (4 * p + s) + a * (3 * s - 3 * p)

    def eblock(a, h):
        at = pl.ds(pl.multiple_of(a * hrows, hrows), hrows)
        return dot_nt(dd[at, 0:hu], wg[h]) + dot_nt(dd[at, hu : 2 * hu], wu[h])

    def rl1(a, d, i):
        return to_hid(rl1s.at[a, d, i], rl1r.at[a, d, i], r1s.at[a, d, i], r1r.at[a, d, i],
                      dblk(a, m4(dprim(a) + 1 - 2 * d), dseco(a)))

    def fn1(a, d, q):
        return to_hid(fn1s.at[a, d, q], fn1r.at[a, d, q], f1s.at[a, d, q], f1r.at[a, d, q],
                      dblk(a, m4(dprim(a) + 1 - 2 * d), dseco(a)))

    def rl2(a, d):
        return to_hid(rl2s.at[a, d], rl2r.at[a, d], r2s.at[a, d], r2r.at[a, d],
                      dblk(a, dprim(a), m4(dseco(a) + 1 - 2 * d)))

    def fn2(a, d):
        return to_hid(fn2s.at[a, d], fn2r.at[a, d], f2s.at[a, d], f2r.at[a, d],
                      dblk(a, dprim(a), m4(dseco(a) + 1 - 2 * d)))

    def relay_step(n):
        a = lax.rem(n, 2)
        d = lax.rem(lax.div(n, 2), 2)
        i = lax.div(n, 4)
        q = 2 - i + d * (1 - 2 * i)
        e = eblock(a, dblk(a, m4(dprim(a) + 2), m4(dseco(a) + q)))
        rl1s[a, d, i] = e.astype(BF)
        rl1(a, d, i).start()

    loop(0, 8, relay_step)
    hpt[...] = hp[...].T

    def weight_step(c):
        at = pl.ds(pl.multiple_of(2 * c * fb, 2 * fb), 2 * fb)
        x = xt[pl.ds(2 * c, 2)].reshape(2 * fb, rows)
        gate_ref[at, :] = dot(x, dd[:, 0:hu]).astype(BF)
        up_ref[at, :] = dot(x, dd[:, hu : 2 * hu]).astype(BF)
        for i in range(2):
            h = 2 * c + i
            down_ref[:, pl.ds(pl.multiple_of(h * fb, fb), fb)] = dot(
                hpt[...], xg[1, h].reshape(rows, fb)).astype(BF)


    def q_send(k):
        to = lax.rem(hid + k, NH)
        return to_hid(qs, qr.at[hid], qss.at[k], qsr.at[k], to)

    def q_recv(k):
        frm = lax.rem(hid + NH - k, NH)
        return to_hid(qs, qr.at[frm], qss.at[k], qsr.at[k], frm)

    qr[hid] = qs[...]
    loop(1, NH, lambda k: q_send(k).start())

    q_order = (2, 3, 1, 0)

    def first_step(n):
        a = lax.rem(n, 2)
        d = lax.rem(lax.div(n, 2), 2)
        q = pick(lax.div(n, 4), q_order)
        in_first = jnp.where(d == 0, jnp.where((q == 2) | (q == 1), 1, 0),
                             jnp.where((q == 3) | (q == 0), 1, 0))
        i = jnp.where(d == 0, 2 - q, lax.div(3 - q, 3))
        e = eblock(a, dblk(a, m4(dprim(a) + 1 - 2 * d), m4(dseco(a) + q)))
        eb[...] = e.reshape(2, hrows // 2, fb)

        @pl.when(in_first == 1)
        def _():
            rl1(a, d, i).wait_recv()
            eb[...] += rl1r[a, d, i].astype(F32).reshape(2, hrows // 2, fb)

        fn1s[a, d, q] = eb[...].astype(BF).reshape(hrows, fb)
        fn1(a, d, q).start()

    loop(0, 16, first_step)
    loop(0, 4, weight_step)

    loop(1, NH, lambda k: q_recv(k).wait_recv())
    total = qr[0]
    for h in range(1, NH):
        total = total + qr[h]
    qt[...] = total
    qb[t] = total

    def c_send(k):
        to = lax.rem(t + k, NT)
        return to_tok(qt, qb.at[t], cs.at[k], cr.at[k], to)

    def c_recv(k):
        frm = lax.rem(t + NT - k, NT)
        return to_tok(qt, qb.at[frm], cs.at[k], cr.at[k], frm)

    loop(1, NT, lambda k: c_send(k).start())

    def b_send(b):
        k = lax.rem(b - t + NT, NT)
        return to_tok(shr.at[b], rb.at[t], bs.at[k], br.at[k], b)

    def b_recv(k):
        frm = lax.rem(t + NT - k, NT)
        return to_tok(shr.at[frm], rb.at[frm], bs.at[k], br.at[k], frm)

    def second_step(n):
        a = lax.rem(n, 2)
        q = pick(lax.div(n, 2), q_order)
        e = eblock(a, dblk(a, dprim(a), m4(dseco(a) + q)))
        eb[...] = e.reshape(2, hrows // 2, fb)
        for d in range(2):
            fn1(a, d, q).wait_recv()
        eb[...] += (fn1r[a, 0, q].astype(F32) + fn1r[a, 1, q].astype(F32)).reshape(
            2, hrows // 2, fb)

        @pl.when(q == 2)
        def _():
            for d in range(2):
                rl2s[a, d] = eb[d].astype(BF)
                rl2(a, d).start()

        for d, at in ((0, 1), (1, 3)):
            @pl.when(q == at)
            def _():
                rl2(a, d).wait_recv()
                eb[d] += rl2r[a, d].astype(F32)
                fn2s[a, d] = eb[...].astype(BF)
                fn2(a, d).start()

        @pl.when(q == 0)
        def _():
            for d in range(2):
                fn2(a, d).wait_recv()
            s = eb[...] + fn2r[a, 0].astype(F32) + fn2r[a, 1].astype(F32)
            shr[pl.ds(a * half, half)] = s.astype(BF).reshape(half, cap, fb)
            for i in range(half):
                b = a * half + i

                @pl.when(b != t)
                def _():
                    b_send(b).start()

                @pl.when(b == t)
                def _():
                    rb[t] = shr[t]

    def second_pair(k):
        weight_step(4 + k)
        second_step(2 * k)
        second_step(2 * k + 1)

    loop(0, 4, second_pair)

    loop(1, NT, lambda k: c_recv(k).wait_recv())
    block = lax.broadcasted_iota(I32, (8, n_tok), 0)
    zero = jnp.zeros((1, n_tok), F32)
    route = [zero, zero]
    for e in range(NT):
        row = jnp.sum(jnp.where(block == t, qb[e], 0.0), axis=0, keepdims=True)
        col = jnp.sum(jnp.where(diag, row, 0.0), axis=1, keepdims=True)
        val = jnp.sum(sel[e] * col, axis=0, keepdims=True)
        for k in range(2):
            route[k] = route[k] + jnp.where(ids[k : k + 1, :] == e, val, 0.0)
    rg_ref[...] = jnp.concatenate(route, axis=0).astype(BF)

    loop(1, NT, lambda k: b_recv(k).wait_recv())
    ig_ref[...] = dot(selt[...].astype(BF), rb[...].reshape(rows, fb)).astype(BF)

    def drain_tok(k):
        for a in range(2):
            z_send(a, k).wait_send()
        p_send(k).wait_send()
        c_send(k).wait_send()
        b_send(lax.rem(t + k, NT)).wait_send()

    loop(1, NT, drain_tok)
    loop(1, NH, lambda k: q_send(k).wait_send())
    for a in range(2):
        for d in range(2):
            p_own(a, d).wait_send()
            p_fwd(a, d).wait_send()
            for o in range(4):
                s_own(a, o, d).wait_send()
                s_fwd(a, o, d).wait_send()
            for i in range(2):
                rl1(a, d, i).wait_send()
            for q in range(4):
                fn1(a, d, q).wait_send()
            rl2(a, d).wait_send()
            fn2(a, d).wait_send()


def copy_out(*refs):
    n = (len(refs) - 1) // 2
    sem = refs[2 * n]
    copies = [pltpu.make_async_copy(refs[k], refs[n + k], sem.at[k]) for k in range(n)]
    for c in copies:
        c.start()
    for c in copies:
        c.wait()


def per_device(tokens, out_grad, routing_ids, route_weights, gate_matrix, up_matrix, down_matrix):
    n_tok, fb = tokens.shape
    cap = 3 * n_tok // NT
    rows = NT * cap
    hu = gate_matrix.shape[2]
    width = gate_matrix.shape[1]
    hr = rows // 2
    vmem = pltpu.VMEM
    dma = pltpu.SemaphoreType.DMA
    hbm_spec = pl.BlockSpec(memory_space=pltpu.HBM)
    vm_spec = pl.BlockSpec(memory_space=pltpu.VMEM)
    shapes = (
        jax.ShapeDtypeStruct((n_tok, fb), BF),
        jax.ShapeDtypeStruct((2, n_tok), BF),
        jax.ShapeDtypeStruct((width, hu), BF),
        jax.ShapeDtypeStruct((width, hu), BF),
        jax.ShapeDtypeStruct((hu, width), BF),
    )
    held = pl.pallas_call(
        exchange,
        name="exchange",
        out_shape=tuple(vmem(s.shape, s.dtype) for s in shapes),
        in_specs=[hbm_spec] * 7,
        out_specs=(vm_spec,) * 5,
        scratch_shapes=[
            vmem((2, n_tok), I32), vmem((2, n_tok), BF), vmem((n_tok, fb), BF), vmem((n_tok, fb), BF),
            vmem((NH, fb, hu), BF), vmem((NH, fb, hu), BF), vmem((hu, width), BF),
            vmem((NT, cap, n_tok), F32), vmem((n_tok, rows), F32),
            vmem((2, NT, cap, fb), BF), vmem((NT, 8, n_tok), F32), vmem((NT, 8, n_tok), F32),
            vmem((2, NH, NT, cap, fb), BF), vmem((NH, fb, rows), BF),
            vmem((rows, hu), F32), vmem((rows, hu), F32), vmem((rows, hu), F32),
            vmem((rows, 2 * hu), BF), vmem((rows, hu), BF), vmem((hu, rows), BF),
            vmem((8, n_tok), F32), vmem((NH, 8, n_tok), F32), vmem((8, n_tok), F32),
            vmem((NT, 8, n_tok), F32),
            vmem((2, hr // 2, fb), F32),
            vmem((2, 2, 2, hr, fb), BF), vmem((2, 2, 2, hr, fb), BF),
            vmem((2, 2, 4, hr, fb), BF), vmem((2, 2, 4, hr, fb), BF),
            vmem((2, 2, hr // 2, fb), BF), vmem((2, 2, hr // 2, fb), BF),
            vmem((2, 2, 2, hr // 2, fb), BF), vmem((2, 2, 2, hr // 2, fb), BF),
            vmem((NT, cap, fb), BF), vmem((NT, cap, fb), BF),
            dma((7,)),
            dma((3, NT)), dma((3, NT)),
            dma((2, 20)), dma((2, 20)),
            dma((2, 2, 2)), dma((2, 2, 2)),
            dma((2, 2, 4)), dma((2, 2, 4)),
            dma((2, 2)), dma((2, 2)),
            dma((2, 2)), dma((2, 2)),
            dma((NH,)), dma((NH,)),
            dma((NT,)), dma((NT,)),
            dma((NT,)), dma((NT,)),
        ],
        compiler_params=pltpu.CompilerParams(
            collective_id=0, has_side_effects=True, vmem_limit_bytes=38 * 1024 * 1024
        ),
    )(*[
        pltpu.with_memory_space_constraint(a, pltpu.HBM)
        for a in (
            routing_ids.T, route_weights.T, tokens, out_grad,
            gate_matrix.reshape(NH, fb, hu), up_matrix.reshape(NH, fb, hu), down_matrix[0],
        )
    ])
    ig, rg, gate_out, up_out, down_out = pl.pallas_call(
        copy_out,
        name="copy_out",
        out_shape=shapes,
        in_specs=[vm_spec] * 5,
        out_specs=(hbm_spec,) * 5,
        scratch_shapes=[dma((5,))],
        compiler_params=pltpu.CompilerParams(vmem_limit_bytes=1024 * 1024),
    )(*[pltpu.with_memory_space_constraint(a, pltpu.VMEM) for a in held])
    return (ig, rg.T, gate_out[None], up_out[None], down_out[None])


def solution(mesh):
    in_specs = (
        P("tok", "hid"),
        P("tok", "hid"),
        P("tok", None),
        P("tok", None),
        P("tok", None, "hid"),
        P("tok", None, "hid"),
        P("tok", "hid", None),
    )
    out_specs = (
        P("tok", "hid"),
        P("tok", None),
        P("tok", None, "hid"),
        P("tok", None, "hid"),
        P("tok", "hid", None),
    )
    return jax.shard_map(
        per_device, mesh=mesh, in_specs=in_specs, out_specs=out_specs, check_vma=False
    )
```

```python
import jax
import jax.numpy as jnp
from jax import lax
from jax.experimental import pallas as pl
from jax.experimental.pallas import tpu as pltpu
from jax.sharding import PartitionSpec as P

BF = jnp.bfloat16
F32 = jnp.float32
I32 = jnp.int32
NT = 8
NH = 16
SIGN = (1, -1)
PARTNERS = ((0, 1), (2, 0), (2, 1), (1, 0), (1, 1), (3, 0), (3, 1))


def dot(a, b):
    return lax.dot_general(a, b, (((1,), (0,)), ((), ())), preferred_element_type=F32)


def dot_nt(a, b):
    return lax.dot_general(a, b, (((1,), (1,)), ((), ())), preferred_element_type=F32)


def m4(v):
    return lax.rem(v + 8, 4)


def pick(index, values):
    out = values[-1]
    for k in range(len(values) - 2, -1, -1):
        out = jnp.where(index == k, values[k], out)
    return out


def loop(lo, hi, body):
    def step(i, carry):
        body(i)
        return carry

    lax.fori_loop(lo, hi, step, 0)


def exchange(
    ids_hbm, rw_hbm, tok_hbm, og_hbm, wg_hbm, wu_hbm, wd_hbm,
    ig_ref, rg_ref, gate_ref, up_ref, down_ref,
    ids_ref, rw_ref, tok_ref, og_ref, wg, wu, wd, sel, selt, pack, psend, precv, xg, xt, acc_g, acc_u, acc_r,
    dd, hp, hpt, qs, q1, q2, qt, qb,
    e32, rl1s, rl1r, fn1s, fn1r, rl2s, rl2r, fn2s, fn2r, shr, rb,
    w_sem, zs, zr, gs, gr, r1s, r1r, f1s, f1r, r2s, r2r, f2s, f2r,
    qss, qsr, bs, br, cs, cr,
):
    t = lax.axis_index("tok")
    hid = lax.axis_index("hid")
    z = lax.div(t, 2)
    core = lax.rem(t, 2)
    cx = lax.div(hid, 4)
    cy = lax.rem(hid, 4)
    cap = sel.shape[1]
    rows = NT * cap
    fb = xg.shape[-1]
    hu = wg.shape[-1]

    def to_hid(src, dst, ssem, rsem, target):
        return pltpu.make_async_remote_copy(
            src_ref=src, dst_ref=dst, send_sem=ssem, recv_sem=rsem,
            device_id={"hid": target}, device_id_type=pl.DeviceIdType.MESH,
        )

    def to_tok(src, dst, ssem, rsem, target):
        return pltpu.make_async_remote_copy(
            src_ref=src, dst_ref=dst, send_sem=ssem, recv_sem=rsem,
            device_id={"tok": target}, device_id_type=pl.DeviceIdType.MESH,
        )

    small = [
        pltpu.make_async_copy(src, dst, w_sem.at[3 + k])
        for k, (src, dst) in enumerate(
            ((ids_hbm, ids_ref), (rw_hbm, rw_ref), (tok_hbm, tok_ref), (og_hbm, og_ref))
        )
    ]
    for c in small:
        c.start()

    bar = pltpu.get_barrier_semaphore()
    for dz, dc in PARTNERS:
        pl.semaphore_signal(
            bar, inc=1, device_id={"tok": 2 * m4(z + dz) + lax.rem(core + dc, 2)},
            device_id_type=pl.DeviceIdType.MESH)
    for k in range(1, 4):
        for target in (4 * m4(cx + k) + cy, 4 * cx + m4(cy + k)):
            pl.semaphore_signal(
                bar, inc=1, device_id={"hid": target}, device_id_type=pl.DeviceIdType.MESH)

    w_copies = [
        pltpu.make_async_copy(wg_hbm, wg, w_sem.at[0]),
        pltpu.make_async_copy(wu_hbm, wu, w_sem.at[1]),
        pltpu.make_async_copy(wd_hbm, wd, w_sem.at[2]),
    ]
    for c in w_copies:
        c.start()

    for c in small:
        c.wait()

    n_tok = tok_ref.shape[0]
    ids = ids_ref[...]
    rw = rw_ref[...].astype(F32)
    expert = lax.broadcasted_iota(I32, (NT, n_tok), 0)
    first = ids[0:1, :] == expert
    second = ids[1:2, :] == expert
    named = jnp.where(first, 1.0, 0.0) + jnp.where(second, 1.0, 0.0)
    weight = jnp.where(first, rw[0:1, :], 0.0) + jnp.where(second, rw[1:2, :], 0.0)
    earlier = (
        lax.broadcasted_iota(I32, (n_tok, n_tok), 0) < lax.broadcasted_iota(I32, (n_tok, n_tok), 1)
    )
    place = dot(named.astype(BF), jnp.where(earlier, 1.0, 0.0).astype(BF))
    code = jnp.where(named > 0.5, place, -1.0).astype(I32)
    slot = lax.broadcasted_iota(I32, (cap, n_tok), 0)
    lane = lax.broadcasted_iota(I32, (cap, n_tok), 1)
    diag = slot == lane
    for e in range(NT):
        one = jnp.where(slot == code[e : e + 1, :], 1.0, 0.0)
        sel[e] = one
        col = jnp.sum(one * weight[e : e + 1, :], axis=1, keepdims=True)
        row = jnp.sum(jnp.where(diag, col, 0.0), axis=0, keepdims=True)
        psend[e] = jnp.broadcast_to(row, (8, n_tok))
    picks = sel[...].reshape(rows, n_tok)
    picks_bf = picks.astype(BF)
    pack[0] = dot(picks_bf, tok_ref[...]).astype(BF).reshape(NT, cap, fb)
    pack[1] = dot(picks_bf, og_ref[...]).astype(BF).reshape(NT, cap, fb)
    xg[0, hid, core] = pack[0, t]
    xg[1, hid, core] = pack[1, t]
    precv[core] = psend[t]

    pl.semaphore_wait(bar, len(PARTNERS) + 6)

    def partner(m, back):
        dz, dc = PARTNERS[m]
        return 2 * m4(z - dz if back else z + dz) + lax.rem(core + dc, 2)

    def z_send(a, m):
        to = partner(m, False)
        place = 2 * ((4 - PARTNERS[m][0]) % 4) + core
        if a == 2:
            return to_tok(psend.at[to], precv.at[place], zs.at[2, m], zr.at[2, m], to)
        return to_tok(pack.at[a, to], xg.at[a, hid, place], zs.at[a, m], zr.at[a, m], to)

    def z_recv(a, m):
        frm = partner(m, True)
        place = 2 * ((4 - PARTNERS[m][0]) % 4) + lax.rem(core + PARTNERS[m][1], 2)
        if a == 2:
            return to_tok(psend.at[frm], precv.at[place], zs.at[2, m], zr.at[2, m], frm)
        return to_tok(pack.at[a, frm], xg.at[a, hid, place], zs.at[a, m], zr.at[a, m], frm)

    z_send(0, 0).start()
    z_send(1, 0).start()
    for a in range(3):
        for m in range(7):
            if a == 2 or m > 0:
                z_send(a, m).start()

    prim = (cx, cy)
    seco = (cy, cx)

    def blk(a, p, s):
        return 4 * p + s if a == 0 else 4 * s + p

    half = NT // 2
    span = {(0, None): (0, 2), (0, 0): (0, 1), (0, 1): (1, 1),
            (1, None): (2, 6), (1, 0): (2, 3), (1, 1): (5, 3)}

    def gather_copy(a, w, block, h, sem, target):
        first, count = span[w, h]
        ref = xg.at[a, block, pl.ds(first, count)]
        return to_hid(ref, ref, gs.at[w, a, sem], gr.at[w, a, sem], target)

    def p_own(a, w, d, recv=False):
        p, s = prim[a], seco[a]
        b = blk(a, m4(p - SIGN[d]) if recv else p, s)
        return gather_copy(a, w, b, None, d, blk(a, m4(p + SIGN[d]), s))

    def p_fwd(a, w, d, recv=False):
        p, s = prim[a], seco[a]
        b = blk(a, m4(p - 2 * SIGN[d]) if recv else m4(p - SIGN[d]), s)
        return gather_copy(a, w, b, d, 2 + d, blk(a, m4(p + SIGN[d]), s))

    def s_own(a, w, o, d, recv=False):
        p, s = prim[a], seco[a]
        b = blk(a, m4(p + o), m4(s - SIGN[d]) if recv else s)
        return gather_copy(a, w, b, None, 4 + 2 * o + d, blk(a, p, m4(s + SIGN[d])))

    def s_fwd(a, w, o, d, recv=False):
        p, s = prim[a], seco[a]
        b = blk(a, m4(p + o), m4(s - 2 * SIGN[d]) if recv else m4(s - SIGN[d]))
        return gather_copy(a, w, b, d, 12 + 2 * o + d, blk(a, p, m4(s + SIGN[d])))

    def gather_begin(w, a):
        for d in range(2):
            p_own(a, w, d).start()
            s_own(a, w, 0, d).start()

    def gather_1(w, a):
        for d in range(2):
            p_own(a, w, d, True).wait_recv()
            p_fwd(a, w, d).start()
            for d2 in range(2):
                s_own(a, w, (4 - SIGN[d]) % 4, d2).start()
        for d in range(2):
            s_own(a, w, 0, d, True).wait_recv()
            s_fwd(a, w, 0, d).start()

    def gather_5(w, a):
        for d in range(2):
            p_fwd(a, w, d, True).wait_recv()
        for d in range(2):
            s_own(a, w, 2, d).start()

    def gather_pass(w, a, o):
        for d in range(2):
            s_own(a, w, o, d, True).wait_recv()
            s_fwd(a, w, o, d).start()

    for a in range(2):
        z_recv(a, 0).wait_recv()
        gather_begin(0, a)
    acc_g[...] = jnp.zeros_like(acc_g)
    acc_u[...] = jnp.zeros_like(acc_u)
    acc_r[...] = jnp.zeros_like(acc_r)
    selt[...] = picks.T
    for a in range(2):
        gather_1(0, a)
    for a in range(2):
        gather_5(0, a)
    for a in range(2):
        for m in range(1, 7):
            z_recv(a, m).wait_recv()
        gather_begin(1, a)
    for a in range(2):
        for o in (3, 1):
            gather_pass(0, a, o)
    for a in range(2):
        gather_pass(0, a, 2)
    for m in range(7):
        z_recv(2, m).wait_recv()
    for c in w_copies:
        c.wait()

    o_of = (0, 3, 1, 0, 0, 2, 3, 3, 1, 1, 2, 2, 0, 3, 1, 2)
    q_of = (0, 0, 0, 3, 1, 0, 3, 1, 3, 1, 3, 1, 2, 2, 2, 2)

    def gather_step(j):
        @pl.when(j == 1)
        def _():
            for a in range(2):
                gather_1(1, a)

        @pl.when(j == 5)
        def _():
            for a in range(2):
                gather_5(1, a)

        @pl.when(j == 6)
        def _():
            for a in range(2):
                for o in (3, 1):
                    gather_pass(1, a, o)

        @pl.when(j == 10)
        def _():
            for a in range(2):
                gather_pass(1, a, 2)

        for n, o in ((12, 0), (13, 3), (14, 1), (15, 2)):
            @pl.when(j == n)
            def _():
                for a in range(2):
                    for w in range(2):
                        for d in range(2):
                            s_fwd(a, w, o, d, True).wait_recv()

        o = pick(j, o_of)
        q = pick(j, q_of)
        bx = blk(0, m4(cx + o), m4(cy + q))
        bg = blk(1, m4(cy + o), m4(cx + q))
        x = xg[0, bx].reshape(rows, fb)
        acc_g[...] += dot(x, wg[bx])
        acc_u[...] += dot(x, wu[bx])
        acc_r[...] += dot_nt(xg[1, bg].reshape(rows, fb), wd[:, pl.ds(pl.multiple_of(bg * fb, fb), fb)])
        xt[bx] = x.T

    loop(0, NH, gather_step)

    def deltas(b):
        at = pl.ds(pl.multiple_of(b * cap, cap), cap)
        g = acc_g[at, :]
        u = acc_u[at, :]
        r = acc_r[at, :]
        p = jnp.sum(jnp.where(diag, precv[b, 0:1, :], 0.0), axis=1, keepdims=True)
        s = 1.0 / (1.0 + jnp.exp(-g))
        act = g * s
        au = act * u
        hp[at, :] = (au * p).astype(BF)
        q = jnp.sum(au.astype(BF).astype(F32) * r, axis=1, keepdims=True)
        qs[pl.ds(b, 1), :] = jnp.sum(jnp.where(diag, q, 0.0), axis=0, keepdims=True)
        rp = r * p
        dd[at, 0:hu] = (rp * u * s * (1.0 + g * (1.0 - s))).astype(BF)
        dd[at, hu : 2 * hu] = (rp * act).astype(BF)

    loop(0, NT, deltas)

    hrows = rows // 2

    def along(a, d):
        p, s = prim[a], seco[a]
        return blk(a, m4(p + SIGN[d]), s)

    def across(a, d):
        p, s = prim[a], seco[a]
        return blk(a, p, m4(s + SIGN[d]))

    def rl1(a, d, i):
        return to_hid(rl1s.at[a, d, i], rl1r.at[a, d, i], r1s.at[a, d, i], r1r.at[a, d, i], along(a, d))

    def fn1(a, d, q):
        return to_hid(fn1s.at[a, d, q], fn1r.at[a, d, q], f1s.at[a, d, q], f1r.at[a, d, q], along(a, d))

    def rl2(a, d):
        return to_hid(rl2s.at[a, d], rl2r.at[a, d], r2s.at[a, d], r2r.at[a, d], across(a, d))

    def fn2(a, d):
        return to_hid(fn2s.at[a, d], fn2r.at[a, d], f2s.at[a, d], f2r.at[a, d], across(a, d))

    def q_x(k, recv=False):
        frm = m4(cx - k) if recv else cx
        return to_hid(qs, q1.at[frm], qss.at[0, k], qsr.at[0, k], 4 * m4(cx + k) + cy)

    def q_y(k, recv=False):
        frm = m4(cy - k) if recv else cy
        return to_hid(qt, q2.at[frm], qss.at[1, k], qsr.at[1, k], 4 * cx + m4(cy + k))

    x_of = (2, 2, 3, 2, 1, 2, 0, 1, 3, 3, 1, 1, 3, 0, 0, 0)
    y_of = (2, 3, 2, 1, 2, 0, 2, 3, 3, 1, 1, 0, 0, 1, 3, 0)

    def e_step(n):
        h = 4 * m4(cx + pick(n, x_of)) + m4(cy + pick(n, y_of))
        e = dot_nt(dd[:, 0:hu], wg[h]) + dot_nt(dd[:, hu : 2 * hu], wu[h])
        e32[h] = e.reshape(2, hrows, fb)
        for k, (d, i) in ((0, (0, 0)), (1, (1, 0)), (3, (0, 1)), (5, (1, 1))):
            for a in range(2):
                @pl.when(n == (k + a if k else 0))
                def _():
                    rl1s[a, d, i] = e32[h, a].astype(BF)
                    rl1(a, d, i).start()

    loop(0, NH, e_step)

    q1[cx] = qs[...]
    for k in range(1, 4):
        q_x(k).start()

    relayed = {2: (0, 0), 1: (0, 1), 3: (1, 0), 0: (1, 1)}

    def first_step(q):
        way, i = relayed[q]
        for d in (1 - way, way):
            for a in range(2):
                e = e32[blk(a, m4(prim[a] + SIGN[d]), m4(seco[a] + q)), a]
                if d == way:
                    rl1(a, d, i).wait_recv()
                    e = e + rl1r[a, d, i].astype(F32)
                fn1s[a, d, q] = e.astype(BF)
                fn1(a, d, q).start()

    def total_of(a, q):
        for d in range(2):
            fn1(a, d, q).wait_recv()
        return (e32[blk(a, prim[a], m4(seco[a] + q)), a]
                + fn1r[a, 0, q].astype(F32) + fn1r[a, 1, q].astype(F32))

    hpt[...] = hp[...].T

    def weight_step(c):
        at = pl.ds(pl.multiple_of(2 * c * fb, 2 * fb), 2 * fb)
        x = xt[pl.ds(2 * c, 2)].reshape(2 * fb, rows)
        gate_ref[at, :] = dot(x, dd[:, 0:hu]).astype(BF)
        up_ref[at, :] = dot(x, dd[:, hu : 2 * hu]).astype(BF)
        for i in range(2):
            h = 2 * c + i
            down_ref[:, pl.ds(pl.multiple_of(h * fb, fb), fb)] = dot(
                hpt[...], xg[1, h].reshape(rows, fb)).astype(BF)

    first_step(2)
    first_step(3)
    for k in range(1, 4):
        q_x(k, True).wait_recv()
    qt[...] = q1[0] + q1[1] + q1[2] + q1[3]
    q2[cy] = qt[...]
    for k in range(1, 4):
        q_y(k).start()
    loop(0, 2, weight_step)
    first_step(1)
    loop(2, 3, weight_step)
    quarter = hrows // 2
    for a in range(2):
        s = total_of(a, 2)
        for d in range(2):
            rl2s[a, d] = s[d * quarter : (d + 1) * quarter].astype(BF)
            rl2(a, d).start()
    first_step(0)
    loop(3, 6, weight_step)
    for k in range(1, 4):
        q_y(k, True).wait_recv()
    qw = q2[0] + q2[1] + q2[2] + q2[3]
    qsum = qb.at[NT]
    qsum[...] = qw
    qb[t] = qw

    def c_send(m):
        to = partner(m, False)
        return to_tok(qb.at[NT], qb.at[t], cs.at[m], cr.at[m], to)

    def c_recv(m):
        frm = partner(m, True)
        return to_tok(qb.at[NT], qb.at[frm], cs.at[m], cr.at[m], frm)

    for m in range(7):
        c_send(m).start()

    for d, q in ((1, 3), (0, 1)):
        for a in range(2):
            s = total_of(a, q)
            rl2(a, d).wait_recv()
            r = rl2r[a, d].astype(F32)
            at = slice(d * quarter, (d + 1) * quarter)
            other = slice((1 - d) * quarter, (2 - d) * quarter)
            fn2s[a, d, d] = (s[at] + r).astype(BF)
            fn2s[a, d, 1 - d] = s[other].astype(BF)
            fn2(a, d).start()
    loop(6, 8, weight_step)

    def b_send(m):
        to = partner(m, False)
        dz, dc = PARTNERS[m]
        return to_tok(shr.at[2 * dz + lax.rem(core + dc, 2)], rb.at[t], bs.at[m], br.at[m], to)

    def b_recv(m):
        frm = partner(m, True)
        return to_tok(shr.at[0], rb.at[frm], bs.at[m], br.at[m], frm)

    for a in (1, 0):
        s = total_of(a, 0)
        for d in range(2):
            fn2(a, d).wait_recv()
            s = s + fn2r[a, d].astype(F32).reshape(hrows, fb)
        shr[a * half : (a + 1) * half] = s.astype(BF).reshape(half, cap, fb)
        for m, (dz, dc) in enumerate(PARTNERS):
            if dz // 2 == a:
                b_send(m).start()
    rb[t] = shr[core]

    for m in range(7):
        c_recv(m).wait_recv()
    block = lax.broadcasted_iota(I32, (8, n_tok), 0)
    zero = jnp.zeros((1, n_tok), F32)
    route = [zero, zero]
    for e in range(NT):
        row = jnp.sum(jnp.where(block == 2 * m4(z - e // 2) + core, qb[e], 0.0), axis=0, keepdims=True)
        col = jnp.sum(jnp.where(diag, row, 0.0), axis=1, keepdims=True)
        val = jnp.sum(sel[e] * col, axis=0, keepdims=True)
        for k in range(2):
            route[k] = route[k] + jnp.where(ids[k : k + 1, :] == e, val, 0.0)
    rg_ref[...] = jnp.concatenate(route, axis=0).astype(BF)

    for m in range(7):
        b_recv(m).wait_recv()
    ig_ref[...] = dot(selt[...].astype(BF), rb[...].reshape(rows, fb)).astype(BF)

    for m in range(7):
        for a in range(3):
            z_send(a, m).wait_send()
        c_send(m).wait_send()
        b_send(m).wait_send()
    for k in range(1, 4):
        q_x(k).wait_send()
        q_y(k).wait_send()
    for a in range(2):
        for d in range(2):
            for w in range(2):
                p_own(a, w, d).wait_send()
                p_fwd(a, w, d).wait_send()
                for o in range(4):
                    s_own(a, w, o, d).wait_send()
                    s_fwd(a, w, o, d).wait_send()
            for i in range(2):
                rl1(a, d, i).wait_send()
            for q in range(4):
                fn1(a, d, q).wait_send()
            rl2(a, d).wait_send()
            fn2(a, d).wait_send()


def copy_out(*refs):
    n = (len(refs) - 1) // 2
    sem = refs[2 * n]
    copies = [pltpu.make_async_copy(refs[k], refs[n + k], sem.at[k]) for k in range(n)]
    for c in copies:
        c.start()
    for c in copies:
        c.wait()


def per_device(tokens, out_grad, routing_ids, route_weights, gate_matrix, up_matrix, down_matrix):
    n_tok, fb = tokens.shape
    cap = 3 * n_tok // NT
    rows = NT * cap
    hu = gate_matrix.shape[2]
    width = gate_matrix.shape[1]
    hr = rows // 2
    vmem = pltpu.VMEM
    dma = pltpu.SemaphoreType.DMA
    hbm_spec = pl.BlockSpec(memory_space=pltpu.HBM)
    vm_spec = pl.BlockSpec(memory_space=pltpu.VMEM)
    shapes = (
        jax.ShapeDtypeStruct((n_tok, fb), BF),
        jax.ShapeDtypeStruct((2, n_tok), BF),
        jax.ShapeDtypeStruct((width, hu), BF),
        jax.ShapeDtypeStruct((width, hu), BF),
        jax.ShapeDtypeStruct((hu, width), BF),
    )
    held = pl.pallas_call(
        exchange,
        name="exchange",
        out_shape=tuple(vmem(s.shape, s.dtype) for s in shapes),
        in_specs=[hbm_spec] * 7,
        out_specs=(vm_spec,) * 5,
        scratch_shapes=[
            vmem((2, n_tok), I32), vmem((2, n_tok), BF), vmem((n_tok, fb), BF), vmem((n_tok, fb), BF),
            vmem((NH, fb, hu), BF), vmem((NH, fb, hu), BF), vmem((hu, width), BF),
            vmem((NT, cap, n_tok), F32), vmem((n_tok, rows), F32),
            vmem((2, NT, cap, fb), BF), vmem((NT, 8, n_tok), F32), vmem((NT, 8, n_tok), F32),
            vmem((2, NH, NT, cap, fb), BF), vmem((NH, fb, rows), BF),
            vmem((rows, hu), F32), vmem((rows, hu), F32), vmem((rows, hu), F32),
            vmem((rows, 2 * hu), BF), vmem((rows, hu), BF), vmem((hu, rows), BF),
            vmem((8, n_tok), F32), vmem((4, 8, n_tok), F32), vmem((4, 8, n_tok), F32),
            vmem((8, n_tok), F32), vmem((NT + 1, 8, n_tok), F32),
            vmem((NH, 2, hr, fb), F32),
            vmem((2, 2, 2, hr, fb), BF), vmem((2, 2, 2, hr, fb), BF),
            vmem((2, 2, 4, hr, fb), BF), vmem((2, 2, 4, hr, fb), BF),
            vmem((2, 2, hr // 2, fb), BF), vmem((2, 2, hr // 2, fb), BF),
            vmem((2, 2, 2, hr // 2, fb), BF), vmem((2, 2, 2, hr // 2, fb), BF),
            vmem((NT, cap, fb), BF), vmem((NT, cap, fb), BF),
            dma((7,)),
            dma((3, NT)), dma((3, NT)),
            dma((2, 2, 20)), dma((2, 2, 20)),
            dma((2, 2, 2)), dma((2, 2, 2)),
            dma((2, 2, 4)), dma((2, 2, 4)),
            dma((2, 2)), dma((2, 2)),
            dma((2, 2)), dma((2, 2)),
            dma((2, 4)), dma((2, 4)),
            dma((NT,)), dma((NT,)),
            dma((NT,)), dma((NT,)),
        ],
        compiler_params=pltpu.CompilerParams(
            collective_id=0, has_side_effects=True, vmem_limit_bytes=46 * 1024 * 1024
        ),
    )(*[
        pltpu.with_memory_space_constraint(a, pltpu.HBM)
        for a in (
            routing_ids.T, route_weights.T, tokens, out_grad,
            gate_matrix.reshape(NH, fb, hu), up_matrix.reshape(NH, fb, hu), down_matrix[0],
        )
    ])
    ig, rg, gate_out, up_out, down_out = pl.pallas_call(
        copy_out,
        name="copy_out",
        out_shape=shapes,
        in_specs=[vm_spec] * 5,
        out_specs=(hbm_spec,) * 5,
        scratch_shapes=[dma((5,))],
        compiler_params=pltpu.CompilerParams(vmem_limit_bytes=1024 * 1024),
    )(*[pltpu.with_memory_space_constraint(a, pltpu.VMEM) for a in held])
    return (ig, rg.T, gate_out[None], up_out[None], down_out[None])


def solution(mesh):
    in_specs = (
        P("tok", "hid"),
        P("tok", "hid"),
        P("tok", None),
        P("tok", None),
        P("tok", None, "hid"),
        P("tok", None, "hid"),
        P("tok", "hid", None),
    )
    out_specs = (
        P("tok", "hid"),
        P("tok", None),
        P("tok", None, "hid"),
        P("tok", None, "hid"),
        P("tok", "hid", None),
    )
    return jax.shard_map(
        per_device, mesh=mesh, in_specs=in_specs, out_specs=out_specs, check_vma=False
    )
```

```python
import jax
import jax.numpy as jnp
from jax import lax
from jax.experimental import pallas as pl
from jax.experimental.pallas import tpu as pltpu
from jax.sharding import PartitionSpec as P

BF = jnp.bfloat16
F32 = jnp.float32
I32 = jnp.int32
NT = 8
NH = 16
SIGN = (1, -1)
PARTNERS = ((0, 1), (1, 0), (1, 1), (3, 0), (3, 1), (2, 0), (2, 1))
PLACE = (0, 1, 3, 2)
RELAYS = (
    ((0, 0, 0), (1, 0, 0)), ((0, 1, 0),), ((1, 1, 0),), ((0, 0, 1),), ((1, 0, 1),), ((0, 1, 1),), ((1, 1, 1),),
)


def dot(a, b):
    return lax.dot_general(a, b, (((1,), (0,)), ((), ())), preferred_element_type=F32)


def dot_nt(a, b):
    return lax.dot_general(a, b, (((1,), (1,)), ((), ())), preferred_element_type=F32)


def m4(v):
    return lax.rem(v + 8, 4)


def pick(index, values):
    out = values[-1]
    for k in range(len(values) - 2, -1, -1):
        out = jnp.where(index == k, values[k], out)
    return out


def loop(lo, hi, body):
    def step(i, carry):
        body(i)
        return carry

    lax.fori_loop(lo, hi, step, 0)


def exchange(
    ids_hbm, rw_hbm, tok_hbm, og_hbm, wg_hbm, wu_hbm, wd_hbm,
    ig_ref, rg_ref, gate_ref, up_ref, down_ref,
    ids_ref, rw_ref, tok_ref, og_ref, wg, wu, wd, sel, selt, pack, psend, precv, xg, xt, acc_g, acc_u, acc_r,
    dd, hp, hpt, qs, q1, q2, qt, qb,
    e32, rl1s, rl1r, fn1s, fn1r, rl2s, rl2r, fn2s, fn2r, shr, rb,
    w_sem, zs, zr, gs, gr, gf, r1s, r1r, f1r, r2r, f2r, qss, qsr, bs, br,
):
    t = lax.axis_index("tok")
    hid = lax.axis_index("hid")
    z = lax.div(t, 2)
    core = lax.rem(t, 2)
    cx = lax.div(hid, 4)
    cy = lax.rem(hid, 4)
    cap = sel.shape[1]
    rows = NT * cap
    fb = xg.shape[-1]
    hu = wg.shape[-1]

    def to_hid(src, dst, ssem, rsem, target):
        return pltpu.make_async_remote_copy(
            src_ref=src, dst_ref=dst, send_sem=ssem, recv_sem=rsem,
            device_id={"hid": target}, device_id_type=pl.DeviceIdType.MESH,
        )

    def to_tok(src, dst, ssem, rsem, target):
        return pltpu.make_async_remote_copy(
            src_ref=src, dst_ref=dst, send_sem=ssem, recv_sem=rsem,
            device_id={"tok": target}, device_id_type=pl.DeviceIdType.MESH,
        )

    small = [
        pltpu.make_async_copy(src, dst, w_sem.at[3 + k])
        for k, (src, dst) in enumerate(
            ((ids_hbm, ids_ref), (rw_hbm, rw_ref), (tok_hbm, tok_ref), (og_hbm, og_ref))
        )
    ]
    for c in small:
        c.start()

    bar = pltpu.get_barrier_semaphore()
    for dz, dc in PARTNERS:
        pl.semaphore_signal(
            bar, inc=1, device_id={"tok": 2 * m4(z + dz) + lax.rem(core + dc, 2)},
            device_id_type=pl.DeviceIdType.MESH)
    for k in range(1, 4):
        for target in (4 * m4(cx + k) + cy, 4 * cx + m4(cy + k)):
            pl.semaphore_signal(
                bar, inc=1, device_id={"hid": target}, device_id_type=pl.DeviceIdType.MESH)

    w_copies = [
        pltpu.make_async_copy(wg_hbm, wg, w_sem.at[0]),
        pltpu.make_async_copy(wu_hbm, wu, w_sem.at[1]),
        pltpu.make_async_copy(wd_hbm, wd, w_sem.at[2]),
    ]
    for c in w_copies:
        c.start()

    for c in small:
        c.wait()

    n_tok = tok_ref.shape[0]
    ids = ids_ref[...]
    rw = rw_ref[...].astype(F32)
    expert = lax.broadcasted_iota(I32, (NT, n_tok), 0)
    first = ids[0:1, :] == expert
    second = ids[1:2, :] == expert
    named = jnp.where(first, 1.0, 0.0) + jnp.where(second, 1.0, 0.0)
    weight = jnp.where(first, rw[0:1, :], 0.0) + jnp.where(second, rw[1:2, :], 0.0)
    earlier = (
        lax.broadcasted_iota(I32, (n_tok, n_tok), 0) < lax.broadcasted_iota(I32, (n_tok, n_tok), 1)
    )
    place = dot(named.astype(BF), jnp.where(earlier, 1.0, 0.0).astype(BF))
    code = jnp.where(named > 0.5, place, -1.0).astype(I32)
    slot = lax.broadcasted_iota(I32, (cap, n_tok), 0)
    lane = lax.broadcasted_iota(I32, (cap, n_tok), 1)
    diag = slot == lane
    for e in range(NT):
        one = jnp.where(slot == code[e : e + 1, :], 1.0, 0.0)
        sel[e] = one
        col = jnp.sum(one * weight[e : e + 1, :], axis=1, keepdims=True)
        row = jnp.sum(jnp.where(diag, col, 0.0), axis=0, keepdims=True)
        psend[e] = jnp.broadcast_to(row, (8, n_tok))
    picks = sel[...].reshape(rows, n_tok)
    picks_bf = picks.astype(BF)
    pack[0] = dot(picks_bf, tok_ref[...]).astype(BF).reshape(NT, cap, fb)
    pack[1] = dot(picks_bf, og_ref[...]).astype(BF).reshape(NT, cap, fb)
    xg[0, hid, core] = pack[0, t]
    xg[1, hid, core] = pack[1, t]
    precv[core] = psend[t]

    pl.semaphore_wait(bar, len(PARTNERS) + 6)

    def partner(m, back):
        dz, dc = PARTNERS[m]
        return 2 * m4(z - dz if back else z + dz) + lax.rem(core + dc, 2)

    def z_send(a, m):
        to = partner(m, False)
        place = 2 * PLACE[-PARTNERS[m][0] % 4] + core
        if a == 2:
            return to_tok(psend.at[to], precv.at[place], zs.at[1], zr.at[2, 0], to)
        return to_tok(pack.at[a, to], xg.at[a, hid, place], zs.at[0], zr.at[a, (m + 3) // 4], to)

    def z_recv(a, group):
        first, count = ((0, 1), (2, 4), (6, 2))[group]
        ref = xg.at[a, hid, pl.ds(1 - core if group == 0 else first, count)]
        return to_tok(ref, ref, zs.at[0], zr.at[a, group], partner(0, True))

    def p_recv():
        ref = precv.at[pl.ds(0, 7)]
        return to_tok(ref, ref, zs.at[1], zr.at[2, 0], partner(0, True))

    for group in ((0,), (1, 2, 3, 4), (5, 6)):
        for a in range(2):
            for m in group:
                z_send(a, m).start()
    for m in range(7):
        z_send(2, m).start()

    prim = (cx, cy)
    seco = (cy, cx)

    def blk(a, p, s):
        return 4 * p + s if a == 0 else 4 * s + p

    half = NT // 2
    span = {}
    for w, (first, count) in enumerate(((0, 2), (2, 4), (6, 2))):
        span[w, None] = (first, count)
        span[w, 0] = (first, count // 2)
        span[w, 1] = (first + count // 2, count // 2)

    def gather_copy(a, w, block, h, sem, target):
        first, count = span[w, h]
        ref = xg.at[a, block, pl.ds(first, count)]
        rsem = gr.at[w, a, sem] if sem < 11 else gf.at[a, sem - 11]
        return to_hid(ref, ref, gs.at[0], rsem, target)

    def p_own(a, w, d, recv=False):
        p, s = prim[a], seco[a]
        b = blk(a, m4(p - SIGN[d]) if recv else p, s)
        return gather_copy(a, w, b, None, d, blk(a, m4(p + SIGN[d]), s))

    def p_fwd(a, w, d, recv=False):
        p, s = prim[a], seco[a]
        b = blk(a, m4(p - 2 * SIGN[d]) if recv else m4(p - SIGN[d]), s)
        return gather_copy(a, w, b, d, 2, blk(a, m4(p + SIGN[d]), s))

    def s_own(a, w, o, d, recv=False):
        p, s = prim[a], seco[a]
        b = blk(a, m4(p + o), m4(s - SIGN[d]) if recv else s)
        return gather_copy(a, w, b, None, 3 + 2 * o + d, blk(a, p, m4(s + SIGN[d])))

    def s_fwd(a, w, o, d, recv=False):
        p, s = prim[a], seco[a]
        b = blk(a, m4(p + o), m4(s - 2 * SIGN[d]) if recv else m4(s - SIGN[d]))
        return gather_copy(a, w, b, d, 11 + o, blk(a, p, m4(s + SIGN[d])))

    def gather_begin(w, a):
        for d in range(2):
            p_own(a, w, d).start()
            s_own(a, w, 0, d).start()

    def gather_1(w, a):
        for d in range(2):
            p_own(a, w, d, True).wait_recv()
            p_fwd(a, w, d).start()
            for d2 in range(2):
                s_own(a, w, (4 - SIGN[d]) % 4, d2).start()
        for d in range(2):
            s_own(a, w, 0, d, True).wait_recv()
            s_fwd(a, w, 0, d).start()

    def gather_5(w, a):
        p, s = prim[a], seco[a]
        gather_copy(a, w, blk(a, m4(p + 2), s), None, 2, blk(a, m4(p + 1), s)).wait_recv()
        for d in range(2):
            s_own(a, w, 2, d).start()

    def gather_end(a, o):
        p, s = prim[a], seco[a]
        ref = xg.at[a, blk(a, m4(p + o), m4(s + 2))]
        to_hid(ref, ref, gs.at[0], gf.at[a, o], blk(a, p, m4(s + 1))).wait_recv()

    def gather_pass(w, a, o):
        for d in range(2):
            s_own(a, w, o, d, True).wait_recv()
            s_fwd(a, w, o, d).start()

    for a in range(2):
        z_recv(a, 0).wait_recv()
        gather_begin(0, a)
    acc_g[...] = jnp.zeros_like(acc_g)
    acc_u[...] = jnp.zeros_like(acc_u)
    acc_r[...] = jnp.zeros_like(acc_r)
    selt[...] = picks.T
    for a in range(2):
        gather_1(0, a)
    for a in range(2):
        z_recv(a, 1).wait_recv()
        gather_begin(1, a)
    for a in range(2):
        gather_5(0, a)
    for a in range(2):
        for o in (3, 1):
            gather_pass(0, a, o)
    for a in range(2):
        z_recv(a, 2).wait_recv()
        gather_begin(2, a)
    for a in range(2):
        gather_pass(0, a, 2)
    p_recv().wait_recv()
    for c in w_copies:
        c.wait()

    o_of = (0, 3, 1, 0, 0, 2, 3, 3, 1, 1, 2, 2, 0, 3, 1, 2)
    q_of = (0, 0, 0, 3, 1, 0, 3, 1, 3, 1, 3, 1, 2, 2, 2, 2)

    def gather_step(j):
        @pl.when(j == 1)
        def _():
            for w in (1, 2):
                for a in range(2):
                    gather_1(w, a)

        @pl.when(j == 5)
        def _():
            for w in (1, 2):
                for a in range(2):
                    gather_5(w, a)

        @pl.when(j == 6)
        def _():
            for w in (1, 2):
                for a in range(2):
                    for o in (3, 1):
                        gather_pass(w, a, o)

        @pl.when(j == 10)
        def _():
            for w in (1, 2):
                for a in range(2):
                    gather_pass(w, a, 2)

        for n, o in ((12, 0), (13, 3), (14, 1), (15, 2)):
            @pl.when(j == n)
            def _():
                for a in range(2):
                    gather_end(a, o)

        o = pick(j, o_of)
        q = pick(j, q_of)
        bx = blk(0, m4(cx + o), m4(cy + q))
        bg = blk(1, m4(cy + o), m4(cx + q))
        x = xg[0, bx].reshape(rows, fb)
        acc_g[...] += dot(x, wg[bx])
        acc_u[...] += dot(x, wu[bx])
        acc_r[...] += dot_nt(xg[1, bg].reshape(rows, fb), wd[:, pl.ds(pl.multiple_of(bg * fb, fb), fb)])
        xt[bx] = x.T
        for w in (wg, wu):
            for k in range(hu // fb):
                w[bx, :, k * fb : (k + 1) * fb] = w[bx, :, k * fb : (k + 1) * fb].T

    loop(0, NH, gather_step)

    def deltas(b):
        at = pl.ds(pl.multiple_of(b * cap, cap), cap)
        g = acc_g[at, :]
        u = acc_u[at, :]
        r = acc_r[at, :]
        p = jnp.sum(jnp.where(diag, precv[b, 0:1, :], 0.0), axis=1, keepdims=True)
        s = 1.0 / (1.0 + jnp.exp(-g))
        act = g * s
        au = act * u
        hp[at, :] = (au * p).astype(BF)
        q = jnp.sum(au.astype(BF).astype(F32) * r, axis=1, keepdims=True)
        qs[pl.ds(b, 1), :] = jnp.sum(jnp.where(diag, q, 0.0), axis=0, keepdims=True)
        rp = r * p
        dd[at, 0:hu] = (rp * u * s * (1.0 + g * (1.0 - s))).astype(BF)
        dd[at, hu : 2 * hu] = (rp * act).astype(BF)

    loop(0, NT, deltas)

    hrows = rows // 2

    def along(a, d):
        p, s = prim[a], seco[a]
        return blk(a, m4(p + SIGN[d]), s)

    def across(a, d):
        p, s = prim[a], seco[a]
        return blk(a, p, m4(s + SIGN[d]))

    def rl1(a, d, i):
        return to_hid(rl1s.at[a, d, i], rl1r.at[a, d, i], r1s.at[0], r1r.at[a, d, i], along(a, d))

    def fn1(a, d, q):
        return to_hid(fn1s.at[a, d, q], fn1r.at[a, q, d], r1s.at[1], f1r.at[a, q], along(a, d))

    def rl2(a, d):
        return to_hid(rl2s.at[a, d], rl2r.at[a, d], r1s.at[2], r2r.at[a, d], across(a, d))

    def fn2(a, d):
        return to_hid(fn2s.at[a, d], fn2r.at[a, d], r1s.at[3], f2r.at[a], across(a, d))

    def q_x(k):
        return to_hid(qs, q1.at[cx], qss.at[0], qsr.at[0], 4 * m4(cx + k) + cy)

    def q_y(k):
        return to_hid(qt, q2.at[cy], qss.at[1], qsr.at[1], 4 * cx + m4(cy + k))

    x_of = (2, 2, 3, 2, 1, 2, 0, 1, 3, 3, 1, 1, 3, 0, 0, 0)
    y_of = (2, 3, 2, 1, 2, 0, 2, 3, 3, 1, 1, 0, 0, 1, 3, 0)

    def e_step(n):
        where = []
        for k in range(2):
            h = 4 * m4(cx + pick(2 * n + k, x_of)) + m4(cy + pick(2 * n + k, y_of))
            turned = jnp.concatenate(
                [w[h, :, i * fb : (i + 1) * fb] for w in (wg, wu) for i in range(hu // fb)], axis=0)
            where.append(h)
            e32[h] = dot(dd[...], turned).reshape(2, hrows, fb)
        for k, todo in enumerate(RELAYS):
            @pl.when(n == k // 2)
            def _():
                for a, d, i in todo:
                    rl1s[a, d, i] = e32[where[k % 2], a].astype(BF)
                    rl1(a, d, i).start()

    q1[cx] = qs[...]
    for k in range(1, 4):
        q_x(k).start()
    loop(0, NH // 2, e_step)

    relayed = {2: (0, 0), 1: (0, 1), 3: (1, 0), 0: (1, 1)}

    def first_step(q):
        way, i = relayed[q]
        for d in (1 - way, way):
            for a in range(2):
                e = e32[blk(a, m4(prim[a] + SIGN[d]), m4(seco[a] + q)), a]
                if d == way:
                    rl1(a, d, i).wait_recv()
                    e = e + rl1r[a, d, i].astype(F32)
                fn1s[a, d, q] = e.astype(BF)
                fn1(a, d, q).start()

    def total_of(a, q):
        to_hid(fn1r.at[a, q], fn1r.at[a, q], r1s.at[1], f1r.at[a, q], along(a, 0)).wait_recv()
        return (e32[blk(a, prim[a], m4(seco[a] + q)), a]
                + fn1r[a, q, 0].astype(F32) + fn1r[a, q, 1].astype(F32))

    hpt[...] = hp[...].T

    def weight_step(c):
        at = pl.ds(pl.multiple_of(2 * c * fb, 2 * fb), 2 * fb)
        x = xt[pl.ds(2 * c, 2)].reshape(2 * fb, rows)
        gate_ref[at, :] = dot(x, dd[:, 0:hu]).astype(BF)
        up_ref[at, :] = dot(x, dd[:, hu : 2 * hu]).astype(BF)
        for i in range(2):
            h = 2 * c + i
            down_ref[:, pl.ds(pl.multiple_of(h * fb, fb), fb)] = dot(
                hpt[...], xg[1, h].reshape(rows, fb)).astype(BF)

    first_step(2)
    first_step(3)
    to_hid(q1.at[pl.ds(0, 3)], q1.at[pl.ds(0, 3)], qss.at[0], qsr.at[0], along(0, 0)).wait_recv()
    qt[...] = q1[0] + q1[1] + q1[2] + q1[3]
    q2[cy] = qt[...]
    for k in range(1, 4):
        q_y(k).start()
    loop(0, 2, weight_step)
    first_step(1)
    loop(2, 3, weight_step)
    quarter = hrows // 2
    for a in range(2):
        s = total_of(a, 2)
        for d in range(2):
            rl2s[a, d] = s[d * quarter : (d + 1) * quarter].astype(BF)
            rl2(a, d).start()
    first_step(0)
    loop(3, 6, weight_step)
    to_hid(q2.at[pl.ds(0, 3)], q2.at[pl.ds(0, 3)], qss.at[1], qsr.at[1], across(0, 0)).wait_recv()
    qw = q2[0] + q2[1] + q2[2] + q2[3]
    qsum = qb.at[NT]
    qsum[...] = qw
    qb[t] = qw

    def c_send(m):
        to = partner(m, False)
        return to_tok(qb.at[NT], qb.at[t], bs.at[1], br.at[1], to)

    for m in range(7):
        c_send(m).start()

    for d, q in ((1, 3), (0, 1)):
        for a in range(2):
            s = total_of(a, q)
            rl2(a, d).wait_recv()
            r = rl2r[a, d].astype(F32)
            at = slice(d * quarter, (d + 1) * quarter)
            other = slice((1 - d) * quarter, (2 - d) * quarter)
            fn2s[a, d, d] = (s[at] + r).astype(BF)
            fn2s[a, d, 1 - d] = s[other].astype(BF)
            fn2(a, d).start()
    loop(6, 8, weight_step)

    def b_send(m):
        to = partner(m, False)
        dz, dc = PARTNERS[m]
        return to_tok(shr.at[2 * PLACE[dz] + lax.rem(core + dc, 2)], rb.at[t], bs.at[0], br.at[0], to)

    for a in (1, 0):
        s = total_of(a, 0)
        to_hid(fn2r.at[a], fn2r.at[a], r1s.at[3], f2r.at[a], across(a, 0)).wait_recv()
        for d in range(2):
            s = s + fn2r[a, d].astype(F32).reshape(hrows, fb)
        shr[a * half : (a + 1) * half] = s.astype(BF).reshape(half, cap, fb)
        for m, (dz, dc) in enumerate(PARTNERS):
            if PLACE[dz] // 2 == a:
                b_send(m).start()
    rb[t] = shr[core]

    def back_wait(ref, k):
        ref = ref.at[pl.ds(0, len(PARTNERS))]
        return to_tok(ref, ref, bs.at[k], br.at[k], partner(0, True))

    back_wait(qb, 1).wait_recv()
    block = lax.broadcasted_iota(I32, (8, n_tok), 0)
    zero = jnp.zeros((1, n_tok), F32)
    route = [zero, zero]
    for e in range(NT):
        row = jnp.sum(jnp.where(block == 2 * pick(m4(z - e // 2), PLACE) + core, qb[e], 0.0), axis=0, keepdims=True)
        col = jnp.sum(jnp.where(diag, row, 0.0), axis=1, keepdims=True)
        val = jnp.sum(sel[e] * col, axis=0, keepdims=True)
        for k in range(2):
            route[k] = route[k] + jnp.where(ids[k : k + 1, :] == e, val, 0.0)
    rg_ref[...] = jnp.concatenate(route, axis=0).astype(BF)

    back_wait(rb, 0).wait_recv()
    ig_ref[...] = dot(selt[...].astype(BF), rb[...].reshape(rows, fb)).astype(BF)

    n_z = len(PARTNERS)
    near = partner(0, False)
    beside = along(0, 0)
    ends = [
        to_tok(pack.at[:, pl.ds(0, n_z)], pack.at[:, pl.ds(0, n_z)], zs.at[0], zr.at[0, 0], near),
        to_tok(psend.at[pl.ds(0, n_z)], psend.at[pl.ds(0, n_z)], zs.at[1], zr.at[0, 0], near),
        to_hid(xg.at[:, pl.ds(0, NH - 1)], xg.at[:, pl.ds(0, NH - 1)], gs.at[0], gf.at[0, 0], beside),
        to_hid(rl1s, rl1r, r1s.at[0], gf.at[0, 0], beside),
        to_hid(fn1s, fn1s, r1s.at[1], gf.at[0, 0], beside),
        to_hid(rl2s, rl2r, r1s.at[2], gf.at[0, 0], beside),
        to_hid(fn2s, fn2r, r1s.at[3], gf.at[0, 0], beside),
        to_hid(q1.at[pl.ds(0, 3)], q1.at[pl.ds(0, 3)], qss.at[0], gf.at[0, 0], beside),
        to_hid(q2.at[pl.ds(0, 3)], q2.at[pl.ds(0, 3)], qss.at[1], gf.at[0, 0], beside),
        back_wait(shr, 0),
        back_wait(qb, 1),
    ]
    for c in ends:
        c.wait_send()


def copy_out(*refs):
    n = (len(refs) - 1) // 2
    sem = refs[2 * n]
    copies = [pltpu.make_async_copy(refs[k], refs[n + k], sem.at[k]) for k in range(n)]
    for c in copies:
        c.start()
    for c in copies:
        c.wait()


def per_device(tokens, out_grad, routing_ids, route_weights, gate_matrix, up_matrix, down_matrix):
    n_tok, fb = tokens.shape
    cap = 3 * n_tok // NT
    rows = NT * cap
    hu = gate_matrix.shape[2]
    width = gate_matrix.shape[1]
    hr = rows // 2
    vmem = pltpu.VMEM
    dma = pltpu.SemaphoreType.DMA
    hbm_spec = pl.BlockSpec(memory_space=pltpu.HBM)
    vm_spec = pl.BlockSpec(memory_space=pltpu.VMEM)
    shapes = (
        jax.ShapeDtypeStruct((n_tok, fb), BF),
        jax.ShapeDtypeStruct((2, n_tok), BF),
        jax.ShapeDtypeStruct((width, hu), BF),
        jax.ShapeDtypeStruct((width, hu), BF),
        jax.ShapeDtypeStruct((hu, width), BF),
    )
    held = pl.pallas_call(
        exchange,
        name="exchange",
        out_shape=tuple(vmem(s.shape, s.dtype) for s in shapes),
        in_specs=[hbm_spec] * 7,
        out_specs=(vm_spec,) * 5,
        scratch_shapes=[
            vmem((2, n_tok), I32), vmem((2, n_tok), BF), vmem((n_tok, fb), BF), vmem((n_tok, fb), BF),
            vmem((NH, fb, hu), BF), vmem((NH, fb, hu), BF), vmem((hu, width), BF),
            vmem((NT, cap, n_tok), F32), vmem((n_tok, rows), F32),
            vmem((2, NT, cap, fb), BF), vmem((NT, 8, n_tok), F32), vmem((NT, 8, n_tok), F32),
            vmem((2, NH, NT, cap, fb), BF), vmem((NH, fb, rows), BF),
            vmem((rows, hu), F32), vmem((rows, hu), F32), vmem((rows, hu), F32),
            vmem((rows, 2 * hu), BF), vmem((rows, hu), BF), vmem((hu, rows), BF),
            vmem((8, n_tok), F32), vmem((4, 8, n_tok), F32), vmem((4, 8, n_tok), F32),
            vmem((8, n_tok), F32), vmem((NT + 1, 8, n_tok), F32),
            vmem((NH, 2, hr, fb), F32),
            vmem((2, 2, 2, hr, fb), BF), vmem((2, 2, 2, hr, fb), BF),
            vmem((2, 2, 4, hr, fb), BF), vmem((2, 4, 2, hr, fb), BF),
            vmem((2, 2, hr // 2, fb), BF), vmem((2, 2, hr // 2, fb), BF),
            vmem((2, 2, 2, hr // 2, fb), BF), vmem((2, 2, 2, hr // 2, fb), BF),
            vmem((NT, cap, fb), BF), vmem((NT, cap, fb), BF),
            dma((7,)),
            dma((2,)), dma((3, 3)),
            dma((1,)), dma((3, 2, 11)), dma((2, 4)),
            dma((4,)), dma((2, 2, 2)), dma((2, 4)), dma((2, 2)), dma((2,)),
            dma((2,)), dma((2,)), dma((2,)), dma((2,)),
        ],
        compiler_params=pltpu.CompilerParams(
            collective_id=0, has_side_effects=True, vmem_limit_bytes=46 * 1024 * 1024
        ),
    )(*[
        pltpu.with_memory_space_constraint(a, pltpu.HBM)
        for a in (
            routing_ids.T, route_weights.T, tokens, out_grad,
            gate_matrix.reshape(NH, fb, hu), up_matrix.reshape(NH, fb, hu), down_matrix[0],
        )
    ])
    ig, rg, gate_out, up_out, down_out = pl.pallas_call(
        copy_out,
        name="copy_out",
        out_shape=shapes,
        in_specs=[vm_spec] * 5,
        out_specs=(hbm_spec,) * 5,
        scratch_shapes=[dma((5,))],
        compiler_params=pltpu.CompilerParams(vmem_limit_bytes=1024 * 1024),
    )(*[pltpu.with_memory_space_constraint(a, pltpu.VMEM) for a in held])
    return (ig, rg.T, gate_out[None], up_out[None], down_out[None])


def solution(mesh):
    in_specs = (
        P("tok", "hid"),
        P("tok", "hid"),
        P("tok", None),
        P("tok", None),
        P("tok", None, "hid"),
        P("tok", None, "hid"),
        P("tok", "hid", None),
    )
    out_specs = (
        P("tok", "hid"),
        P("tok", None),
        P("tok", None, "hid"),
        P("tok", None, "hid"),
        P("tok", "hid", None),
    )
    return jax.shard_map(
        per_device, mesh=mesh, in_specs=in_specs, out_specs=out_specs, check_vma=False
    )
```

```python
import jax
import jax.numpy as jnp
from jax import lax
from jax.experimental import pallas as pl
from jax.experimental.pallas import tpu as pltpu
from jax.sharding import PartitionSpec as P

BF = jnp.bfloat16
F32 = jnp.float32
I32 = jnp.int32
NT = 8
NH = 16
SIGN = (1, -1)
PARTNERS = ((0, 1), (1, 0), (1, 1), (3, 0), (3, 1), (2, 0), (2, 1))
PLACE = (0, 1, 3, 2)
STREAMS = ((0, 0, 2, 0), (0, 2, 4, 0), (0, 6, 2, 1), (1, 6, 2, 1), (2, 0, 128, 1))
X_OWN, X_NEXT, X_FAR, G_FAR, RAW = range(5)
RELAYS = (
    ((0, 0, 0), (1, 0, 0)), ((0, 1, 0),), ((1, 1, 0),), ((0, 0, 1),), ((1, 0, 1),), ((0, 1, 1),), ((1, 1, 1),),
)


def dot(a, b):
    return lax.dot_general(a, b, (((1,), (0,)), ((), ())), preferred_element_type=F32)


def dot_nt(a, b):
    return lax.dot_general(a, b, (((1,), (1,)), ((), ())), preferred_element_type=F32)


def m4(v):
    return lax.rem(v + 8, 4)


def pick(index, values):
    out = values[-1]
    for k in range(len(values) - 2, -1, -1):
        out = jnp.where(index == k, values[k], out)
    return out


def loop(lo, hi, body):
    def step(i, carry):
        body(i)
        return carry

    lax.fori_loop(lo, hi, step, 0)


def exchange(
    ids_hbm, rw_hbm, tok_hbm, og_hbm, wg_hbm, wu_hbm, wd_hbm,
    ig_ref, rg_ref, gate_ref, up_ref, down_ref,
    ids_ref, rw_ref, tok_ref, raw, wg, wu, wd, sel, picks, selt, pack, pk, psend, precv, xg, xt, acc_g, acc_u, acc_r,
    dd, hp, hpt, qs, q1, q2, qt, qb,
    e32, rl1s, rl1r, fn1s, fn1r, rl2s, rl2r, fn2s, fn2r, shr, rb,
    w_sem, zs, zr, zg, gs, gr, gf, r1s, r1r, f1r, r2r, f2r, qss, qsr, bs, br,
):
    t = lax.axis_index("tok")
    hid = lax.axis_index("hid")
    z = lax.div(t, 2)
    core = lax.rem(t, 2)
    cx = lax.div(hid, 4)
    cy = lax.rem(hid, 4)
    cap = sel.shape[1]
    rows = NT * cap
    fb = xg.shape[-1]
    hu = wg.shape[-1]

    def to_hid(src, dst, ssem, rsem, target):
        return pltpu.make_async_remote_copy(
            src_ref=src, dst_ref=dst, send_sem=ssem, recv_sem=rsem,
            device_id={"hid": target}, device_id_type=pl.DeviceIdType.MESH,
        )

    def to_tok(src, dst, ssem, rsem, target):
        return pltpu.make_async_remote_copy(
            src_ref=src, dst_ref=dst, send_sem=ssem, recv_sem=rsem,
            device_id={"tok": target}, device_id_type=pl.DeviceIdType.MESH,
        )

    small = [
        pltpu.make_async_copy(src, dst, w_sem.at[3 + k])
        for k, (src, dst) in enumerate(
            ((ids_hbm, ids_ref), (rw_hbm, rw_ref), (tok_hbm, tok_ref), (og_hbm, raw.at[hid]))
        )
    ]
    for c in small:
        c.start()

    bar = pltpu.get_barrier_semaphore()
    for dz, dc in PARTNERS:
        pl.semaphore_signal(
            bar, inc=1, device_id={"tok": 2 * m4(z + dz) + lax.rem(core + dc, 2)},
            device_id_type=pl.DeviceIdType.MESH)
    for k in range(1, 4):
        for target in (4 * m4(cx + k) + cy, 4 * cx + m4(cy + k)):
            pl.semaphore_signal(
                bar, inc=1, device_id={"hid": target}, device_id_type=pl.DeviceIdType.MESH)

    w_copies = [
        pltpu.make_async_copy(wg_hbm, wg, w_sem.at[0]),
        pltpu.make_async_copy(wu_hbm, wu, w_sem.at[1]),
        pltpu.make_async_copy(wd_hbm, wd, w_sem.at[2]),
    ]
    for c in w_copies:
        c.start()

    for c in small:
        c.wait()

    n_tok = tok_ref.shape[0]
    ids = ids_ref[...]
    rw = rw_ref[...].astype(F32)
    expert = lax.broadcasted_iota(I32, (NT, n_tok), 0)
    first = ids[0:1, :] == expert
    second = ids[1:2, :] == expert
    named = jnp.where(first, 1.0, 0.0) + jnp.where(second, 1.0, 0.0)
    weight = jnp.where(first, rw[0:1, :], 0.0) + jnp.where(second, rw[1:2, :], 0.0)
    earlier = (
        lax.broadcasted_iota(I32, (n_tok, n_tok), 0) < lax.broadcasted_iota(I32, (n_tok, n_tok), 1)
    )
    place = dot(named.astype(BF), jnp.where(earlier, 1.0, 0.0).astype(BF))
    code = jnp.where(named > 0.5, place, -1.0).astype(I32)
    slot = lax.broadcasted_iota(I32, (cap, n_tok), 0)
    lane = lax.broadcasted_iota(I32, (cap, n_tok), 1)
    diag = slot == lane
    for e in range(NT):
        one = jnp.where(slot == code[e : e + 1, :], 1.0, 0.0)
        sel[e] = one
        col = jnp.sum(one * weight[e : e + 1, :], axis=1, keepdims=True)
        row = jnp.sum(jnp.where(diag, col, 0.0), axis=0, keepdims=True)
        psend[e] = jnp.broadcast_to(row, (8, n_tok))
    picks[...] = sel[...].reshape(rows, n_tok).astype(BF)
    pack[...] = dot(picks[...], tok_ref[...]).astype(BF).reshape(NT, cap, fb)
    xg[0, hid, core] = pack[t]
    precv[core] = psend[t]

    pl.semaphore_wait(bar, len(PARTNERS) + 6)

    def partner(m, back):
        dz, dc = PARTNERS[m]
        return 2 * m4(z - dz if back else z + dz) + lax.rem(core + dc, 2)

    def z_send(a, m):
        to = partner(m, False)
        place = 2 * PLACE[-PARTNERS[m][0] % 4] + core
        group = (m + 3) // 4
        if a == 2:
            return to_tok(psend.at[to], precv.at[place], zs.at[1], zr.at[2, 0], to)
        src = pack.at[to] if a == 0 else pk.at[hid, to]
        return to_tok(src, xg.at[a, hid, place], zs.at[3 * a], zr.at[a, group], to)

    def z_recv(a, group):
        first, count = ((0, 1), (2, 4), (6, 2))[group]
        ref = xg.at[a, hid, pl.ds(1 - core if group == 0 else first, count)]
        return to_tok(ref, ref, zs.at[0], zr.at[a, group], partner(0, True))

    def p_recv():
        ref = precv.at[pl.ds(0, 7)]
        return to_tok(ref, ref, zs.at[1], zr.at[2, 0], partner(0, True))

    prim = (cx, cy)
    seco = (cy, cx)

    def blk(a, p, s):
        return 4 * p + s if a == 0 else 4 * s + p

    half = NT // 2

    def part(st, block, h=None):
        array, first, count = STREAMS[st][:3]
        if h is not None:
            count //= 2
            first += h * count
        base = raw.at[block] if array == 2 else xg.at[array, block]
        return base.at[pl.ds(first, count)]

    def gather_copy(st, block, h, sem, target):
        ref = part(st, block, h)
        rsem = gr.at[st, sem] if sem < 11 else gf.at[st, sem - 11]
        return to_hid(ref, ref, gs.at[STREAMS[st][0]], rsem, target)

    def frame(st):
        g = STREAMS[st][3]
        return g, prim[g], seco[g]

    def p_own(st, d, recv=False):
        g, p, s = frame(st)
        b = blk(g, m4(p - SIGN[d]) if recv else p, s)
        return gather_copy(st, b, None, d, blk(g, m4(p + SIGN[d]), s))

    def p_fwd(st, d):
        g, p, s = frame(st)
        return gather_copy(st, blk(g, m4(p - SIGN[d]), s), d, 2, blk(g, m4(p + SIGN[d]), s))

    def s_own(st, o, d, recv=False):
        g, p, s = frame(st)
        b = blk(g, m4(p + o), m4(s - SIGN[d]) if recv else s)
        return gather_copy(st, b, None, 3 + 2 * o + d, blk(g, p, m4(s + SIGN[d])))

    def s_fwd(st, o, d):
        g, p, s = frame(st)
        return gather_copy(st, blk(g, m4(p + o), m4(s - SIGN[d])), d, 11 + o, blk(g, p, m4(s + SIGN[d])))

    def gather_begin(st):
        for d in range(2):
            p_own(st, d).start()
            s_own(st, 0, d).start()

    def gather_1(st):
        for d in range(2):
            p_own(st, d, True).wait_recv()
            p_fwd(st, d).start()
            for d2 in range(2):
                s_own(st, (4 - SIGN[d]) % 4, d2).start()
        for d in range(2):
            s_own(st, 0, d, True).wait_recv()
            s_fwd(st, 0, d).start()

    def gather_5(st):
        g, p, s = frame(st)
        gather_copy(st, blk(g, m4(p + 2), s), None, 2, blk(g, m4(p + 1), s)).wait_recv()
        for d in range(2):
            s_own(st, 2, d).start()

    def gather_pass(st, *offsets):
        for o in offsets:
            for d in range(2):
                s_own(st, o, d, True).wait_recv()
                s_fwd(st, o, d).start()

    def gather_end(st, *offsets):
        g, p, s = frame(st)
        for o in offsets:
            gather_copy(st, blk(g, m4(p + o), m4(s + 2)), None, 11 + o, blk(g, p, m4(s + 1))).wait_recv()

    o_of = (0, 3, 1, 0, 0, 3, 3, 1, 1, 2, 0, 2, 3, 2, 1, 2)
    q_of = (0, 0, 0, 3, 1, 3, 1, 3, 1, 0, 2, 3, 2, 1, 2, 2)

    def raw_block(n):
        return blk(1, m4(cy + pick(n, o_of)), m4(cx + pick(n, q_of)))

    def raw_pack(n):
        h = raw_block(n)
        pk[h] = dot(picks[...], raw[h]).astype(BF).reshape(NT, cap, fb)
        xg[1, h, core] = pk[h, t]
        for m in range(5):
            to = partner(m, False)
            place = 2 * PLACE[-PARTNERS[m][0] % 4] + core
            to_tok(pk.at[h, to], xg.at[1, h, place], zs.at[2], zg.at[n], to).start()

    def raw_packs(*places):
        loop(0, len(places), lambda i: raw_pack(pick(i, places)))

    gather_begin(RAW)
    for m in range(5):
        z_send(0, m).start()
    raw_pack(0)
    for a in range(2):
        for m in (5, 6):
            z_send(a, m).start()
    for m in range(7):
        z_send(2, m).start()
    z_recv(0, 0).wait_recv()
    gather_begin(X_OWN)
    acc_g[...] = jnp.zeros_like(acc_g)
    acc_u[...] = jnp.zeros_like(acc_u)
    acc_r[...] = jnp.zeros_like(acc_r)
    selt[...] = sel[...].reshape(rows, n_tok).T
    gather_1(RAW)
    raw_packs(1, 2, 3, 4)
    gather_1(X_OWN)
    gather_5(RAW)
    raw_packs(9)
    gather_5(X_OWN)
    gather_pass(RAW, 3, 1)
    raw_packs(5, 6, 7, 8)
    gather_pass(X_OWN, 3, 1)
    gather_pass(RAW, 2)
    z_recv(0, 1).wait_recv()
    gather_begin(X_NEXT)
    z_recv(0, 2).wait_recv()
    gather_begin(X_FAR)
    z_recv(1, 2).wait_recv()
    gather_begin(G_FAR)
    raw_packs(11, 13)
    gather_pass(X_OWN, 2)
    gather_end(RAW, 0, 3, 1, 2)
    raw_packs(10, 12, 14, 15)
    for st in (X_NEXT, X_FAR, G_FAR):
        gather_1(st)
    for c in w_copies:
        c.wait()
    gather_end(X_OWN, 0, 3, 1, 2)

    def gather_step(j):
        @pl.when(j == 2)
        def _():
            for st in (X_NEXT, X_FAR, G_FAR):
                gather_5(st)
            for st in (X_NEXT, X_FAR, G_FAR):
                gather_pass(st, 3, 1)

        @pl.when(j == 4)
        def _():
            for st in (X_NEXT, X_FAR, G_FAR):
                gather_pass(st, 2)

        for n, near, far in ((4, (), (0,)), (5, (0,), (3,)), (6, (3,), (1,)), (7, (1, 2), (2,))):
            @pl.when(j == n)
            def _():
                gather_end(X_NEXT, *near)
                gather_end(G_FAR, *near)
                gather_end(X_FAR, *far)

        hx, hg = [], []
        for k in (2 * j, 2 * j + 1):
            hx.append(blk(0, m4(cx + pick(k, o_of)), m4(cy + pick(k, q_of))))
            hg.append(raw_block(k))

        for k in range(2):
            five = xg.at[1, hg[k], pl.ds(1, 5)]
            to_tok(five, five, zs.at[2], zg.at[2 * j + k], partner(0, True)).wait_recv()
        pair(hx, hg)

    def pair(hx, hg):
        x = jnp.concatenate([xg[0, h].reshape(rows, fb) for h in hx], axis=1)
        acc_g[...] += dot(x, jnp.concatenate([wg[h] for h in hx], axis=0))
        acc_u[...] += dot(x, jnp.concatenate([wu[h] for h in hx], axis=0))
        acc_r[...] += dot_nt(
            jnp.concatenate([xg[1, h].reshape(rows, fb) for h in hg], axis=1),
            jnp.concatenate([wd[:, pl.ds(pl.multiple_of(h * fb, fb), fb)] for h in hg], axis=1))
        for h in hx:
            xt[h] = xg[0, h].reshape(rows, fb).T
            for w in (wg, wu):
                for k in range(hu // fb):
                    w[h, :, k * fb : (k + 1) * fb] = w[h, :, k * fb : (k + 1) * fb].T

    p_recv().wait_recv()
    loop(0, NH // 2, gather_step)

    def deltas(b):
        at = pl.ds(pl.multiple_of(b * cap, cap), cap)
        g = acc_g[at, :]
        u = acc_u[at, :]
        r = acc_r[at, :]
        p = jnp.sum(jnp.where(diag, precv[b, 0:1, :], 0.0), axis=1, keepdims=True)
        s = 1.0 / (1.0 + jnp.exp(-g))
        act = g * s
        au = act * u
        hp[at, :] = (au * p).astype(BF)
        q = jnp.sum(au.astype(BF).astype(F32) * r, axis=1, keepdims=True)
        qs[pl.ds(b, 1), :] = jnp.sum(jnp.where(diag, q, 0.0), axis=0, keepdims=True)
        rp = r * p
        dd[at, 0:hu] = (rp * u * s * (1.0 + g * (1.0 - s))).astype(BF)
        dd[at, hu : 2 * hu] = (rp * act).astype(BF)

    loop(0, NT, deltas)

    hrows = rows // 2

    def along(a, d):
        p, s = prim[a], seco[a]
        return blk(a, m4(p + SIGN[d]), s)

    def across(a, d):
        p, s = prim[a], seco[a]
        return blk(a, p, m4(s + SIGN[d]))

    def rl1(a, d, i):
        return to_hid(rl1s.at[a, d, i], rl1r.at[a, d, i], r1s.at[0], r1r.at[a, d, i], along(a, d))

    def fn1(a, d, q):
        return to_hid(fn1s.at[a, d, q], fn1r.at[a, q, d], r1s.at[1], f1r.at[a, q], along(a, d))

    def rl2(a, d):
        return to_hid(rl2s.at[a, d], rl2r.at[a, d], r1s.at[2], r2r.at[a, d], across(a, d))

    def fn2(a, d):
        return to_hid(fn2s.at[a, d], fn2r.at[a, d], r1s.at[3], f2r.at[a], across(a, d))

    def q_x(k):
        return to_hid(qs, q1.at[cx], qss.at[0], qsr.at[0], 4 * m4(cx + k) + cy)

    def q_y(k):
        return to_hid(qt, q2.at[cy], qss.at[1], qsr.at[1], 4 * cx + m4(cy + k))

    x_of = (2, 2, 3, 2, 1, 2, 0, 1, 3, 3, 1, 1, 3, 0, 0, 0)
    y_of = (2, 3, 2, 1, 2, 0, 2, 3, 3, 1, 1, 0, 0, 1, 3, 0)

    def e_step(n):
        where = []
        for k in range(2):
            h = 4 * m4(cx + pick(2 * n + k, x_of)) + m4(cy + pick(2 * n + k, y_of))
            turned = jnp.concatenate(
                [w[h, :, i * fb : (i + 1) * fb] for w in (wg, wu) for i in range(hu // fb)], axis=0)
            where.append(h)
            e32[h] = dot(dd[...], turned).reshape(2, hrows, fb)
        for k, todo in enumerate(RELAYS):
            @pl.when(n == k // 2)
            def _():
                for a, d, i in todo:
                    rl1s[a, d, i] = e32[where[k % 2], a].astype(BF)
                    rl1(a, d, i).start()

    q1[cx] = qs[...]
    for k in range(1, 4):
        q_x(k).start()
    loop(0, NH // 2, e_step)

    relayed = {2: (0, 0), 1: (0, 1), 3: (1, 0), 0: (1, 1)}

    def first_step(q):
        way, i = relayed[q]
        for d in (1 - way, way):
            for a in range(2):
                e = e32[blk(a, m4(prim[a] + SIGN[d]), m4(seco[a] + q)), a]
                if d == way:
                    rl1(a, d, i).wait_recv()
                    e = e + rl1r[a, d, i].astype(F32)
                fn1s[a, d, q] = e.astype(BF)
                fn1(a, d, q).start()

    def total_of(a, q):
        to_hid(fn1r.at[a, q], fn1r.at[a, q], r1s.at[1], f1r.at[a, q], along(a, 0)).wait_recv()
        return (e32[blk(a, prim[a], m4(seco[a] + q)), a]
                + fn1r[a, q, 0].astype(F32) + fn1r[a, q, 1].astype(F32))

    hpt[...] = hp[...].T

    def weight_step(c):
        at = pl.ds(pl.multiple_of(2 * c * fb, 2 * fb), 2 * fb)
        x = xt[pl.ds(2 * c, 2)].reshape(2 * fb, rows)
        gate_ref[at, :] = dot(x, dd[:, 0:hu]).astype(BF)
        up_ref[at, :] = dot(x, dd[:, hu : 2 * hu]).astype(BF)
        for i in range(2):
            h = 2 * c + i
            down_ref[:, pl.ds(pl.multiple_of(h * fb, fb), fb)] = dot(
                hpt[...], xg[1, h].reshape(rows, fb)).astype(BF)

    first_step(2)
    first_step(3)
    to_hid(q1.at[pl.ds(0, 3)], q1.at[pl.ds(0, 3)], qss.at[0], qsr.at[0], along(0, 0)).wait_recv()
    qt[...] = q1[0] + q1[1] + q1[2] + q1[3]
    q2[cy] = qt[...]
    for k in range(1, 4):
        q_y(k).start()
    loop(0, 2, weight_step)
    first_step(1)
    loop(2, 3, weight_step)
    quarter = hrows // 2
    for a in range(2):
        s = total_of(a, 2)
        for d in range(2):
            rl2s[a, d] = s[d * quarter : (d + 1) * quarter].astype(BF)
            rl2(a, d).start()
    first_step(0)
    loop(3, 6, weight_step)
    to_hid(q2.at[pl.ds(0, 3)], q2.at[pl.ds(0, 3)], qss.at[1], qsr.at[1], across(0, 0)).wait_recv()
    qw = q2[0] + q2[1] + q2[2] + q2[3]
    qsum = qb.at[NT]
    qsum[...] = qw
    qb[t] = qw

    def c_send(m):
        to = partner(m, False)
        return to_tok(qb.at[NT], qb.at[t], bs.at[1], br.at[1], to)

    for m in range(7):
        c_send(m).start()

    for d, q in ((1, 3), (0, 1)):
        for a in range(2):
            s = total_of(a, q)
            rl2(a, d).wait_recv()
            r = rl2r[a, d].astype(F32)
            at = slice(d * quarter, (d + 1) * quarter)
            other = slice((1 - d) * quarter, (2 - d) * quarter)
            fn2s[a, d, d] = (s[at] + r).astype(BF)
            fn2s[a, d, 1 - d] = s[other].astype(BF)
            fn2(a, d).start()
    loop(6, 8, weight_step)

    def b_send(m):
        to = partner(m, False)
        dz, dc = PARTNERS[m]
        return to_tok(shr.at[2 * PLACE[dz] + lax.rem(core + dc, 2)], rb.at[t], bs.at[0], br.at[0], to)

    for a in (1, 0):
        s = total_of(a, 0)
        to_hid(fn2r.at[a], fn2r.at[a], r1s.at[3], f2r.at[a], across(a, 0)).wait_recv()
        for d in range(2):
            s = s + fn2r[a, d].astype(F32).reshape(hrows, fb)
        shr[a * half : (a + 1) * half] = s.astype(BF).reshape(half, cap, fb)
        for m, (dz, dc) in enumerate(PARTNERS):
            if PLACE[dz] // 2 == a:
                b_send(m).start()
    rb[t] = shr[core]

    def back_wait(ref, k):
        ref = ref.at[pl.ds(0, len(PARTNERS))]
        return to_tok(ref, ref, bs.at[k], br.at[k], partner(0, True))

    back_wait(qb, 1).wait_recv()
    block = lax.broadcasted_iota(I32, (8, n_tok), 0)
    zero = jnp.zeros((1, n_tok), F32)
    route = [zero, zero]
    for e in range(NT):
        row = jnp.sum(jnp.where(block == 2 * pick(m4(z - e // 2), PLACE) + core, qb[e], 0.0), axis=0, keepdims=True)
        col = jnp.sum(jnp.where(diag, row, 0.0), axis=1, keepdims=True)
        val = jnp.sum(sel[e] * col, axis=0, keepdims=True)
        for k in range(2):
            route[k] = route[k] + jnp.where(ids[k : k + 1, :] == e, val, 0.0)
    rg_ref[...] = jnp.concatenate(route, axis=0).astype(BF)

    back_wait(rb, 0).wait_recv()
    ig_ref[...] = dot(selt[...].astype(BF), rb[...].reshape(rows, fb)).astype(BF)

    n_z = len(PARTNERS)
    near = partner(0, False)
    beside = along(0, 0)
    ends = [
        to_tok(pack.at[pl.ds(0, n_z)], pack.at[pl.ds(0, n_z)], zs.at[0], zr.at[0, 0], near),
        to_tok(xg.at[0, pl.ds(0, 10)], xg.at[0, pl.ds(0, 10)], zs.at[2], zr.at[0, 0], near),
        to_tok(pk.at[0, pl.ds(0, 2)], pk.at[0, pl.ds(0, 2)], zs.at[3], zr.at[0, 0], near),
        to_tok(psend.at[pl.ds(0, n_z)], psend.at[pl.ds(0, n_z)], zs.at[1], zr.at[0, 0], near),
        to_hid(xg.at[0, pl.ds(0, NH - 1)], xg.at[0, pl.ds(0, NH - 1)], gs.at[0], gf.at[0, 0], beside),
        to_hid(xg.at[1, pl.ds(0, NH - 1), pl.ds(6, 2)], xg.at[1, pl.ds(0, NH - 1), pl.ds(6, 2)],
               gs.at[1], gf.at[0, 0], beside),
        to_hid(raw.at[pl.ds(0, NH - 1)], raw.at[pl.ds(0, NH - 1)], gs.at[2], gf.at[0, 0], beside),
        to_hid(rl1s, rl1r, r1s.at[0], gf.at[0, 0], beside),
        to_hid(fn1s, fn1s, r1s.at[1], gf.at[0, 0], beside),
        to_hid(rl2s, rl2r, r1s.at[2], gf.at[0, 0], beside),
        to_hid(fn2s, fn2r, r1s.at[3], gf.at[0, 0], beside),
        to_hid(q1.at[pl.ds(0, 3)], q1.at[pl.ds(0, 3)], qss.at[0], gf.at[0, 0], beside),
        to_hid(q2.at[pl.ds(0, 3)], q2.at[pl.ds(0, 3)], qss.at[1], gf.at[0, 0], beside),
        back_wait(shr, 0),
        back_wait(qb, 1),
    ]
    for c in ends:
        c.wait_send()


def copy_out(*refs):
    n = (len(refs) - 1) // 2
    sem = refs[2 * n]
    copies = [pltpu.make_async_copy(refs[k], refs[n + k], sem.at[k]) for k in range(n)]
    for c in copies:
        c.start()
    for c in copies:
        c.wait()


def per_device(tokens, out_grad, routing_ids, route_weights, gate_matrix, up_matrix, down_matrix):
    n_tok, fb = tokens.shape
    cap = 3 * n_tok // NT
    rows = NT * cap
    hu = gate_matrix.shape[2]
    width = gate_matrix.shape[1]
    hr = rows // 2
    vmem = pltpu.VMEM
    dma = pltpu.SemaphoreType.DMA
    hbm_spec = pl.BlockSpec(memory_space=pltpu.HBM)
    vm_spec = pl.BlockSpec(memory_space=pltpu.VMEM)
    shapes = (
        jax.ShapeDtypeStruct((n_tok, fb), BF),
        jax.ShapeDtypeStruct((2, n_tok), BF),
        jax.ShapeDtypeStruct((width, hu), BF),
        jax.ShapeDtypeStruct((width, hu), BF),
        jax.ShapeDtypeStruct((hu, width), BF),
    )
    held = pl.pallas_call(
        exchange,
        name="exchange",
        out_shape=tuple(vmem(s.shape, s.dtype) for s in shapes),
        in_specs=[hbm_spec] * 7,
        out_specs=(vm_spec,) * 5,
        scratch_shapes=[
            vmem((2, n_tok), I32), vmem((2, n_tok), BF), vmem((n_tok, fb), BF), vmem((NH, n_tok, fb), BF),
            vmem((NH, fb, hu), BF), vmem((NH, fb, hu), BF), vmem((hu, width), BF),
            vmem((NT, cap, n_tok), F32), vmem((rows, n_tok), BF), vmem((n_tok, rows), F32),
            vmem((NT, cap, fb), BF), vmem((NH, NT, cap, fb), BF), vmem((NT, 8, n_tok), F32), vmem((NT, 8, n_tok), F32),
            vmem((2, NH, NT, cap, fb), BF), vmem((NH, fb, rows), BF),
            vmem((rows, hu), F32), vmem((rows, hu), F32), vmem((rows, hu), F32),
            vmem((rows, 2 * hu), BF), vmem((rows, hu), BF), vmem((hu, rows), BF),
            vmem((8, n_tok), F32), vmem((4, 8, n_tok), F32), vmem((4, 8, n_tok), F32),
            vmem((8, n_tok), F32), vmem((NT + 1, 8, n_tok), F32),
            vmem((NH, 2, hr, fb), F32),
            vmem((2, 2, 2, hr, fb), BF), vmem((2, 2, 2, hr, fb), BF),
            vmem((2, 2, 4, hr, fb), BF), vmem((2, 4, 2, hr, fb), BF),
            vmem((2, 2, hr // 2, fb), BF), vmem((2, 2, hr // 2, fb), BF),
            vmem((2, 2, 2, hr // 2, fb), BF), vmem((2, 2, 2, hr // 2, fb), BF),
            vmem((NT, cap, fb), BF), vmem((NT, cap, fb), BF),
            dma((7,)),
            dma((4,)), dma((3, 3)), dma((NH,)),
            dma((3,)), dma((5, 11)), dma((5, 4)),
            dma((4,)), dma((2, 2, 2)), dma((2, 4)), dma((2, 2)), dma((2,)),
            dma((2,)), dma((2,)), dma((2,)), dma((2,)),
        ],
        compiler_params=pltpu.CompilerParams(
            collective_id=0, has_side_effects=True, vmem_limit_bytes=50 * 1024 * 1024
        ),
    )(*[
        pltpu.with_memory_space_constraint(a, pltpu.HBM)
        for a in (
            routing_ids.T, route_weights.T, tokens, out_grad,
            gate_matrix.reshape(NH, fb, hu), up_matrix.reshape(NH, fb, hu), down_matrix[0],
        )
    ])
    ig, rg, gate_out, up_out, down_out = pl.pallas_call(
        copy_out,
        name="copy_out",
        out_shape=shapes,
        in_specs=[vm_spec] * 5,
        out_specs=(hbm_spec,) * 5,
        scratch_shapes=[dma((5,))],
        compiler_params=pltpu.CompilerParams(vmem_limit_bytes=1024 * 1024),
    )(*[pltpu.with_memory_space_constraint(a, pltpu.VMEM) for a in held])
    return (ig, rg.T, gate_out[None], up_out[None], down_out[None])


def solution(mesh):
    in_specs = (
        P("tok", "hid"),
        P("tok", "hid"),
        P("tok", None),
        P("tok", None),
        P("tok", None, "hid"),
        P("tok", None, "hid"),
        P("tok", "hid", None),
    )
    out_specs = (
        P("tok", "hid"),
        P("tok", None),
        P("tok", None, "hid"),
        P("tok", None, "hid"),
        P("tok", "hid", None),
    )
    return jax.shard_map(
        per_device, mesh=mesh, in_specs=in_specs, out_specs=out_specs, check_vma=False
    )
```

```python
import jax
import jax.numpy as jnp
from jax import lax
from jax.experimental import pallas as pl
from jax.experimental.pallas import tpu as pltpu
from jax.sharding import PartitionSpec as P

BF = jnp.bfloat16
F32 = jnp.float32
I32 = jnp.int32
NT = 8
NH = 16
SIGN = (1, -1)
PARTNERS = ((0, 1), (1, 0), (1, 1), (3, 0), (3, 1), (2, 0), (2, 1))
PLACE = (0, 1, 3, 2)
STREAMS = ((0, 0, 2, 0), (0, 2, 4, 0), (0, 6, 2, 1), (1, 6, 2, 1), (2, 0, 128, 1))
X_OWN, X_NEXT, X_FAR, G_FAR, RAW = range(5)
RELAYS = (
    ((0, 0, 0), (1, 0, 0)), ((0, 1, 0),), ((1, 1, 0),), ((0, 0, 1),), ((1, 0, 1),), ((0, 1, 1),), ((1, 1, 1),),
)


def dot(a, b):
    return lax.dot_general(a, b, (((1,), (0,)), ((), ())), preferred_element_type=F32)


def dot_nt(a, b):
    return lax.dot_general(a, b, (((1,), (1,)), ((), ())), preferred_element_type=F32)


def m4(v):
    return lax.rem(v + 8, 4)


def pick(index, values):
    out = values[-1]
    for k in range(len(values) - 2, -1, -1):
        out = jnp.where(index == k, values[k], out)
    return out


def loop(lo, hi, body):
    def step(i, carry):
        body(i)
        return carry

    lax.fori_loop(lo, hi, step, 0)


def exchange(
    ids_hbm, rw_hbm, tok_hbm, og_hbm, wg_hbm, wu_hbm, wd_hbm,
    ig_ref, rg_ref, gate_ref, up_ref, down_ref,
    ids_ref, rw_ref, tok_ref, raw, wg, wu, wd, sel, picks, selt, pack, pk, psend, precv, xg, xt, acc_g, acc_u, acc_r,
    dd, hp, hpt, qs, q1, q2, qt, qb,
    e32, rl1s, rl1r, fn1s, fn1r, rl2s, rl2r, fn2s, fn2r, shr, rb,
    w_sem, zs, zr, zg, gs, gr, gf, r1s, r1r, f1r, r2r, f2r, qss, qsr, bs, br,
):
    t = lax.axis_index("tok")
    hid = lax.axis_index("hid")
    z = lax.div(t, 2)
    core = lax.rem(t, 2)
    cx = lax.div(hid, 4)
    cy = lax.rem(hid, 4)
    cap = sel.shape[1]
    rows = NT * cap
    fb = xg.shape[-1]
    hu = wg.shape[-1]

    def to_hid(src, dst, ssem, rsem, target):
        return pltpu.make_async_remote_copy(
            src_ref=src, dst_ref=dst, send_sem=ssem, recv_sem=rsem,
            device_id={"hid": target}, device_id_type=pl.DeviceIdType.MESH,
        )

    def to_tok(src, dst, ssem, rsem, target):
        return pltpu.make_async_remote_copy(
            src_ref=src, dst_ref=dst, send_sem=ssem, recv_sem=rsem,
            device_id={"tok": target}, device_id_type=pl.DeviceIdType.MESH,
        )

    small = [
        pltpu.make_async_copy(src, dst, w_sem.at[3 + k])
        for k, (src, dst) in enumerate(
            ((ids_hbm, ids_ref), (rw_hbm, rw_ref), (tok_hbm, tok_ref), (og_hbm, raw.at[hid]))
        )
    ]
    for c in small:
        c.start()

    bar = pltpu.get_barrier_semaphore()
    for dz, dc in PARTNERS:
        pl.semaphore_signal(
            bar, inc=1, device_id={"tok": 2 * m4(z + dz) + lax.rem(core + dc, 2)},
            device_id_type=pl.DeviceIdType.MESH)
    for k in range(1, 4):
        for target in (4 * m4(cx + k) + cy, 4 * cx + m4(cy + k)):
            pl.semaphore_signal(
                bar, inc=1, device_id={"hid": target}, device_id_type=pl.DeviceIdType.MESH)

    w_copies = [
        pltpu.make_async_copy(wg_hbm, wg, w_sem.at[0]),
        pltpu.make_async_copy(wu_hbm, wu, w_sem.at[1]),
        pltpu.make_async_copy(wd_hbm, wd, w_sem.at[2]),
    ]
    for c in w_copies:
        c.start()

    for c in small:
        c.wait()

    n_tok = tok_ref.shape[0]
    ids = ids_ref[...]
    rw = rw_ref[...].astype(F32)
    expert = lax.broadcasted_iota(I32, (NT, n_tok), 0)
    first = ids[0:1, :] == expert
    second = ids[1:2, :] == expert
    named = jnp.where(first, 1.0, 0.0) + jnp.where(second, 1.0, 0.0)
    weight = jnp.where(first, rw[0:1, :], 0.0) + jnp.where(second, rw[1:2, :], 0.0)
    earlier = (
        lax.broadcasted_iota(I32, (n_tok, n_tok), 0) < lax.broadcasted_iota(I32, (n_tok, n_tok), 1)
    )
    place = dot(named.astype(BF), jnp.where(earlier, 1.0, 0.0).astype(BF))
    code = jnp.where(named > 0.5, place, -1.0).astype(I32)
    slot = lax.broadcasted_iota(I32, (cap, n_tok), 0)
    lane = lax.broadcasted_iota(I32, (cap, n_tok), 1)
    diag = slot == lane
    for e in range(NT):
        one = jnp.where(slot == code[e : e + 1, :], 1.0, 0.0)
        sel[e] = one
        col = jnp.sum(one * weight[e : e + 1, :], axis=1, keepdims=True)
        row = jnp.sum(jnp.where(diag, col, 0.0), axis=0, keepdims=True)
        psend[e] = jnp.broadcast_to(row, (8, n_tok))
    picks[...] = sel[...].reshape(rows, n_tok).astype(BF)
    pack[...] = dot(picks[...], tok_ref[...]).astype(BF).reshape(NT, cap, fb)
    xg[0, hid, core] = pack[t]
    precv[core] = psend[t]

    pl.semaphore_wait(bar, len(PARTNERS) + 6)

    def partner(m, back):
        dz, dc = PARTNERS[m]
        return 2 * m4(z - dz if back else z + dz) + lax.rem(core + dc, 2)

    def z_send(a, m):
        to = partner(m, False)
        place = 2 * PLACE[-PARTNERS[m][0] % 4] + core
        group = (m + 3) // 4
        if a == 2:
            return to_tok(psend.at[to], precv.at[place], zs.at[1], zr.at[2, 0], to)
        src = pack.at[to] if a == 0 else pk.at[hid, to]
        return to_tok(src, xg.at[a, hid, place], zs.at[3 * a], zr.at[a, group], to)

    def z_recv(a, group):
        first, count = ((0, 1), (2, 4), (6, 2))[group]
        ref = xg.at[a, hid, pl.ds(1 - core if group == 0 else first, count)]
        return to_tok(ref, ref, zs.at[0], zr.at[a, group], partner(0, True))

    def p_recv():
        ref = precv.at[pl.ds(0, 7)]
        return to_tok(ref, ref, zs.at[1], zr.at[2, 0], partner(0, True))

    prim = (cx, cy)
    seco = (cy, cx)

    def blk(a, p, s):
        return 4 * p + s if a == 0 else 4 * s + p

    half = NT // 2

    def part(st, block, h=None):
        array, first, count = STREAMS[st][:3]
        if h is not None:
            count //= 2
            first += h * count
        base = raw.at[block] if array == 2 else xg.at[array, block]
        return base.at[pl.ds(first, count)]

    def gather_copy(st, block, h, sem, target):
        ref = part(st, block, h)
        rsem = gr.at[st, sem] if sem < 11 else gf.at[st, sem - 11]
        return to_hid(ref, ref, gs.at[STREAMS[st][0]], rsem, target)

    def frame(st):
        g = STREAMS[st][3]
        return g, prim[g], seco[g]

    def p_own(st, d, recv=False):
        g, p, s = frame(st)
        b = blk(g, m4(p - SIGN[d]) if recv else p, s)
        return gather_copy(st, b, None, d, blk(g, m4(p + SIGN[d]), s))

    def p_fwd(st, d):
        g, p, s = frame(st)
        return gather_copy(st, blk(g, m4(p - SIGN[d]), s), d, 2, blk(g, m4(p + SIGN[d]), s))

    def s_own(st, o, d, recv=False):
        g, p, s = frame(st)
        b = blk(g, m4(p + o), m4(s - SIGN[d]) if recv else s)
        return gather_copy(st, b, None, 3 + 2 * o + d, blk(g, p, m4(s + SIGN[d])))

    def s_fwd(st, o, d):
        g, p, s = frame(st)
        return gather_copy(st, blk(g, m4(p + o), m4(s - SIGN[d])), d, 11 + o, blk(g, p, m4(s + SIGN[d])))

    def gather_begin(*sts):
        for st in sts:
            for d in range(2):
                p_own(st, d).start()
        for st in sts:
            for d in range(2):
                s_own(st, 0, d).start()

    def gather_p(*sts):
        for st in sts:
            for d in range(2):
                p_own(st, d, True).wait_recv()
                p_fwd(st, d).start()
        for st in sts:
            for d in range(2):
                for d2 in range(2):
                    s_own(st, (4 - SIGN[d]) % 4, d2).start()

    def gather_s(*sts):
        for st in sts:
            for d in range(2):
                s_own(st, 0, d, True).wait_recv()
                s_fwd(st, 0, d).start()

    def gather_1(st):
        gather_p(st)
        gather_s(st)

    def gather_5(st):
        g, p, s = frame(st)
        gather_copy(st, blk(g, m4(p + 2), s), None, 2, blk(g, m4(p + 1), s)).wait_recv()
        for d in range(2):
            s_own(st, 2, d).start()

    def gather_pass(st, *offsets):
        for o in offsets:
            for d in range(2):
                s_own(st, o, d, True).wait_recv()
                s_fwd(st, o, d).start()

    def gather_end(st, *offsets):
        g, p, s = frame(st)
        for o in offsets:
            gather_copy(st, blk(g, m4(p + o), m4(s + 2)), None, 11 + o, blk(g, p, m4(s + 1))).wait_recv()

    o_of = (0, 3, 1, 0, 0, 3, 3, 1, 1, 2, 0, 2, 3, 2, 1, 2)
    q_of = (0, 0, 0, 3, 1, 3, 1, 3, 1, 0, 2, 3, 2, 1, 2, 2)

    def raw_block(n):
        return blk(1, m4(cy + pick(n, o_of)), m4(cx + pick(n, q_of)))

    def raw_pack(n):
        h = raw_block(n)
        pk[h] = dot(picks[...], raw[h]).astype(BF).reshape(NT, cap, fb)
        xg[1, h, core] = pk[h, t]
        for m in range(5):
            to = partner(m, False)
            place = 2 * PLACE[-PARTNERS[m][0] % 4] + core
            to_tok(pk.at[h, to], xg.at[1, h, place], zs.at[2], zg.at[lax.div(n, 2)], to).start()

    def raw_packs(*places):
        loop(0, len(places), lambda i: raw_pack(pick(i, places)))

    gather_begin(RAW)
    for m in range(5):
        z_send(0, m).start()
    raw_pack(0)
    for a in range(2):
        for m in (5, 6):
            z_send(a, m).start()
    for m in range(7):
        z_send(2, m).start()
    z_recv(0, 0).wait_recv()
    gather_begin(X_OWN)
    acc_g[...] = jnp.zeros_like(acc_g)
    acc_u[...] = jnp.zeros_like(acc_u)
    acc_r[...] = jnp.zeros_like(acc_r)
    selt[...] = sel[...].reshape(rows, n_tok).T
    gather_1(RAW)
    raw_packs(1, 2, 3, 4)
    gather_1(X_OWN)
    gather_5(RAW)
    raw_packs(9)
    gather_5(X_OWN)
    gather_pass(RAW, 3, 1)
    raw_packs(5, 6, 7, 8)
    gather_pass(X_OWN, 3, 1)
    gather_pass(RAW, 2)
    z_recv(0, 1).wait_recv()
    z_recv(0, 2).wait_recv()
    z_recv(1, 2).wait_recv()
    gather_begin(X_FAR, G_FAR, X_NEXT)
    raw_packs(11, 13)
    gather_pass(X_OWN, 2)
    gather_p(X_FAR, X_NEXT, G_FAR)
    gather_end(RAW, 0, 3, 1, 2)
    raw_packs(10, 12, 14, 15)
    gather_s(X_FAR, X_NEXT, G_FAR)
    for c in w_copies:
        c.wait()
    gather_end(X_OWN, 0, 3, 1, 2)

    def gather_step(j):
        @pl.when(j == 1)
        def _():
            for st in (X_FAR, X_NEXT, G_FAR):
                gather_5(st)

        @pl.when(j == 2)
        def _():
            for st in (X_NEXT, X_FAR, G_FAR):
                gather_pass(st, 3, 1)

        @pl.when(j == 4)
        def _():
            for st in (X_NEXT, X_FAR, G_FAR):
                gather_pass(st, 2)

        for n, near, far in ((4, (), (0,)), (5, (0,), (3,)), (6, (3,), (1,)), (7, (1, 2), (2,))):
            @pl.when(j == n)
            def _():
                gather_end(X_NEXT, *near)
                gather_end(G_FAR, *near)
                gather_end(X_FAR, *far)

        hx, hg = [], []
        for k in (2 * j, 2 * j + 1):
            hx.append(blk(0, m4(cx + pick(k, o_of)), m4(cy + pick(k, q_of))))
            hg.append(raw_block(k))

        ten = xg.at[1, pl.ds(0, 2), pl.ds(0, 5)]
        to_tok(ten, ten, zs.at[2], zg.at[j], partner(0, True)).wait_recv()
        pair(hx, hg)

    def pair(hx, hg):
        x = jnp.concatenate([xg[0, h].reshape(rows, fb) for h in hx], axis=1)
        acc_g[...] += dot(x, jnp.concatenate([wg[h] for h in hx], axis=0))
        acc_u[...] += dot(x, jnp.concatenate([wu[h] for h in hx], axis=0))
        acc_r[...] += dot_nt(
            jnp.concatenate([xg[1, h].reshape(rows, fb) for h in hg], axis=1),
            jnp.concatenate([wd[:, pl.ds(pl.multiple_of(h * fb, fb), fb)] for h in hg], axis=1))
        for h in hx:
            xt[h] = xg[0, h].reshape(rows, fb).T
            for w in (wg, wu):
                for k in range(hu // fb):
                    w[h, :, k * fb : (k + 1) * fb] = w[h, :, k * fb : (k + 1) * fb].T

    p_recv().wait_recv()
    loop(0, NH // 2, gather_step)

    def deltas(b):
        at = pl.ds(pl.multiple_of(b * cap, cap), cap)
        g = acc_g[at, :]
        u = acc_u[at, :]
        r = acc_r[at, :]
        p = jnp.sum(jnp.where(diag, precv[b, 0:1, :], 0.0), axis=1, keepdims=True)
        s = 1.0 / (1.0 + jnp.exp(-g))
        act = g * s
        rp = r * p
        dd[at, 0:hu] = (rp * u * s * (1.0 + g * (1.0 - s))).astype(BF)
        dd[at, hu : 2 * hu] = (rp * act).astype(BF)

    def hiddens(b):
        at = pl.ds(pl.multiple_of(b * cap, cap), cap)
        g = acc_g[at, :]
        p = jnp.sum(jnp.where(diag, precv[b, 0:1, :], 0.0), axis=1, keepdims=True)
        au = g * (1.0 / (1.0 + jnp.exp(-g))) * acc_u[at, :]
        hp[at, :] = (au * p).astype(BF)
        q = jnp.sum(au.astype(BF).astype(F32) * acc_r[at, :], axis=1, keepdims=True)
        qs[pl.ds(b, 1), :] = jnp.sum(jnp.where(diag, q, 0.0), axis=0, keepdims=True)

    loop(0, NT, deltas)

    hrows = rows // 2

    def along(a, d):
        p, s = prim[a], seco[a]
        return blk(a, m4(p + SIGN[d]), s)

    def across(a, d):
        p, s = prim[a], seco[a]
        return blk(a, p, m4(s + SIGN[d]))

    def rl1(a, d, i):
        return to_hid(rl1s.at[a, d, i], rl1r.at[d, i, a], r1s.at[0], r1r.at[d, i], along(a, d))

    def fn1(a, d, q):
        return to_hid(fn1s.at[a, d, q], fn1r.at[a, q, d], r1s.at[1], f1r.at[a, q], along(a, d))

    def rl2(a, d):
        return to_hid(rl2s.at[a, d], rl2r.at[a, d], r1s.at[2], r2r.at[a, d], across(a, d))

    def fn2(a, d):
        return to_hid(fn2s.at[a, d], fn2r.at[a, d], r1s.at[3], f2r.at[a], across(a, d))

    def q_x(k):
        return to_hid(qs, q1.at[cx], qss.at[0], qsr.at[0], 4 * m4(cx + k) + cy)

    def q_y(k):
        return to_hid(qt, q2.at[cy], qss.at[1], qsr.at[1], 4 * cx + m4(cy + k))

    x_of = (2, 2, 3, 2, 1, 2, 0, 1, 3, 3, 1, 1, 3, 0, 0, 0)
    y_of = (2, 3, 2, 1, 2, 0, 2, 3, 3, 1, 1, 0, 0, 1, 3, 0)

    def e_step(n):
        where = []
        for k in range(2):
            h = 4 * m4(cx + pick(2 * n + k, x_of)) + m4(cy + pick(2 * n + k, y_of))
            turned = jnp.concatenate(
                [w[h, :, i * fb : (i + 1) * fb] for w in (wg, wu) for i in range(hu // fb)], axis=0)
            where.append(h)
            e32[h] = dot(dd[...], turned).reshape(2, hrows, fb)
        for k, todo in enumerate(RELAYS):
            @pl.when(n == k // 2)
            def _():
                for a, d, i in todo:
                    rl1s[a, d, i] = e32[where[k % 2], a].astype(BF)
                    rl1(a, d, i).start()

    relayed = {2: (0, 0), 1: (0, 1), 3: (1, 0), 0: (1, 1)}

    def first_send(q, d):
        way, i = relayed[q]
        if d == way:
            to_hid(rl1r.at[d, i], rl1r.at[d, i], r1s.at[0], r1r.at[d, i], along(0, d)).wait_recv()
        for a in range(2):
            e = e32[blk(a, m4(prim[a] + SIGN[d]), m4(seco[a] + q)), a]
            if d == way:
                e = e + rl1r[d, i, a].astype(F32)
            fn1s[a, d, q] = e.astype(BF)
            fn1(a, d, q).start()

    def first_step(q):
        way = relayed[q][0]
        first_send(q, 1 - way)
        first_send(q, way)

    def total_of(a, q):
        to_hid(fn1r.at[a, q], fn1r.at[a, q], r1s.at[1], f1r.at[a, q], along(a, 0)).wait_recv()
        return (e32[blk(a, prim[a], m4(seco[a] + q)), a]
                + fn1r[a, q, 0].astype(F32) + fn1r[a, q, 1].astype(F32))

    def weight_step(c):
        at = pl.ds(pl.multiple_of(2 * c * fb, 2 * fb), 2 * fb)
        x = xt[pl.ds(2 * c, 2)].reshape(2 * fb, rows)
        gate_ref[at, :] = dot(x, dd[:, 0:hu]).astype(BF)
        up_ref[at, :] = dot(x, dd[:, hu : 2 * hu]).astype(BF)
        for i in range(2):
            h = 2 * c + i
            down_ref[:, pl.ds(pl.multiple_of(h * fb, fb), fb)] = dot(
                hpt[...], xg[1, h].reshape(rows, fb)).astype(BF)

    loop(0, 4, e_step)
    first_send(2, 1)
    loop(4, NH // 2, e_step)
    first_send(3, 0)
    first_send(2, 0)
    first_send(3, 1)
    loop(0, NT, hiddens)
    q1[cx] = qs[...]
    for k in range(1, 4):
        q_x(k).start()
    first_step(1)
    hpt[...] = hp[...].T
    loop(0, 2, weight_step)
    quarter = hrows // 2
    for a in range(2):
        s = total_of(a, 2)
        for d in range(2):
            rl2s[a, d] = s[d * quarter : (d + 1) * quarter].astype(BF)
            rl2(a, d).start()
    first_step(0)
    loop(2, 3, weight_step)
    to_hid(q1.at[pl.ds(0, 3)], q1.at[pl.ds(0, 3)], qss.at[0], qsr.at[0], along(0, 0)).wait_recv()
    qt[...] = q1[0] + q1[1] + q1[2] + q1[3]
    q2[cy] = qt[...]
    for k in range(1, 4):
        q_y(k).start()
    loop(3, 4, weight_step)
    for d, q in ((1, 3), (0, 1)):
        for a in range(2):
            s = total_of(a, q)
            rl2(a, d).wait_recv()
            r = rl2r[a, d].astype(F32)
            at = slice(d * quarter, (d + 1) * quarter)
            other = slice((1 - d) * quarter, (2 - d) * quarter)
            fn2s[a, d, d] = (s[at] + r).astype(BF)
            fn2s[a, d, 1 - d] = s[other].astype(BF)
            fn2(a, d).start()
    loop(4, 5, weight_step)
    to_hid(q2.at[pl.ds(0, 3)], q2.at[pl.ds(0, 3)], qss.at[1], qsr.at[1], across(0, 0)).wait_recv()
    qw = q2[0] + q2[1] + q2[2] + q2[3]
    qsum = qb.at[NT]
    qsum[...] = qw
    qb[t] = qw

    def c_send(m):
        to = partner(m, False)
        return to_tok(qb.at[NT], qb.at[t], bs.at[1], br.at[1], to)

    for m in range(7):
        c_send(m).start()


    def b_send(m):
        to = partner(m, False)
        dz, dc = PARTNERS[m]
        return to_tok(shr.at[2 * PLACE[dz] + lax.rem(core + dc, 2)], rb.at[t], bs.at[0], br.at[0], to)

    for a in (1, 0):
        s = total_of(a, 0)
        to_hid(fn2r.at[a], fn2r.at[a], r1s.at[3], f2r.at[a], across(a, 0)).wait_recv()
        for d in range(2):
            s = s + fn2r[a, d].astype(F32).reshape(hrows, fb)
        shr[a * half : (a + 1) * half] = s.astype(BF).reshape(half, cap, fb)
        for m in (5, 6, 0, 1, 2, 3, 4):
            if PLACE[PARTNERS[m][0]] // 2 == a:
                b_send(m).start()
    rb[t] = shr[core]
    loop(5, 8, weight_step)

    def back_wait(ref, k):
        ref = ref.at[pl.ds(0, len(PARTNERS))]
        return to_tok(ref, ref, bs.at[k], br.at[k], partner(0, True))

    back_wait(qb, 1).wait_recv()
    block = lax.broadcasted_iota(I32, (8, n_tok), 0)
    zero = jnp.zeros((1, n_tok), F32)
    route = [zero, zero]
    for e in range(NT):
        row = jnp.sum(jnp.where(block == 2 * pick(m4(z - e // 2), PLACE) + core, qb[e], 0.0), axis=0, keepdims=True)
        col = jnp.sum(jnp.where(diag, row, 0.0), axis=1, keepdims=True)
        val = jnp.sum(sel[e] * col, axis=0, keepdims=True)
        for k in range(2):
            route[k] = route[k] + jnp.where(ids[k : k + 1, :] == e, val, 0.0)
    rg_ref[...] = jnp.concatenate(route, axis=0).astype(BF)

    back_wait(rb, 0).wait_recv()
    ig_ref[...] = dot(selt[...].astype(BF), rb[...].reshape(rows, fb)).astype(BF)

    n_z = len(PARTNERS)
    near = partner(0, False)
    beside = along(0, 0)
    ends = [
        to_tok(pack.at[pl.ds(0, n_z)], pack.at[pl.ds(0, n_z)], zs.at[0], zr.at[0, 0], near),
        to_tok(xg.at[0, pl.ds(0, 10)], xg.at[0, pl.ds(0, 10)], zs.at[2], zr.at[0, 0], near),
        to_tok(pk.at[0, pl.ds(0, 2)], pk.at[0, pl.ds(0, 2)], zs.at[3], zr.at[0, 0], near),
        to_tok(psend.at[pl.ds(0, n_z)], psend.at[pl.ds(0, n_z)], zs.at[1], zr.at[0, 0], near),
        to_hid(xg.at[0, pl.ds(0, NH - 1)], xg.at[0, pl.ds(0, NH - 1)], gs.at[0], gf.at[0, 0], beside),
        to_hid(xg.at[1, pl.ds(0, NH - 1), pl.ds(6, 2)], xg.at[1, pl.ds(0, NH - 1), pl.ds(6, 2)],
               gs.at[1], gf.at[0, 0], beside),
        to_hid(raw.at[pl.ds(0, NH - 1)], raw.at[pl.ds(0, NH - 1)], gs.at[2], gf.at[0, 0], beside),
        to_hid(rl1s, rl1r, r1s.at[0], gf.at[0, 0], beside),
        to_hid(fn1s, fn1s, r1s.at[1], gf.at[0, 0], beside),
        to_hid(rl2s, rl2r, r1s.at[2], gf.at[0, 0], beside),
        to_hid(fn2s, fn2r, r1s.at[3], gf.at[0, 0], beside),
        to_hid(q1.at[pl.ds(0, 3)], q1.at[pl.ds(0, 3)], qss.at[0], gf.at[0, 0], beside),
        to_hid(q2.at[pl.ds(0, 3)], q2.at[pl.ds(0, 3)], qss.at[1], gf.at[0, 0], beside),
        back_wait(shr, 0),
        back_wait(qb, 1),
    ]
    for c in ends:
        c.wait_send()


def copy_out(*refs):
    n = (len(refs) - 1) // 2
    sem = refs[2 * n]
    copies = [pltpu.make_async_copy(refs[k], refs[n + k], sem.at[k]) for k in range(n)]
    for c in copies:
        c.start()
    for c in copies:
        c.wait()


def per_device(tokens, out_grad, routing_ids, route_weights, gate_matrix, up_matrix, down_matrix):
    n_tok, fb = tokens.shape
    cap = 3 * n_tok // NT
    rows = NT * cap
    hu = gate_matrix.shape[2]
    width = gate_matrix.shape[1]
    hr = rows // 2
    vmem = pltpu.VMEM
    dma = pltpu.SemaphoreType.DMA
    hbm_spec = pl.BlockSpec(memory_space=pltpu.HBM)
    vm_spec = pl.BlockSpec(memory_space=pltpu.VMEM)
    shapes = (
        jax.ShapeDtypeStruct((n_tok, fb), BF),
        jax.ShapeDtypeStruct((2, n_tok), BF),
        jax.ShapeDtypeStruct((width, hu), BF),
        jax.ShapeDtypeStruct((width, hu), BF),
        jax.ShapeDtypeStruct((hu, width), BF),
    )
    held = pl.pallas_call(
        exchange,
        name="exchange",
        out_shape=tuple(vmem(s.shape, s.dtype) for s in shapes),
        in_specs=[hbm_spec] * 7,
        out_specs=(vm_spec,) * 5,
        scratch_shapes=[
            vmem((2, n_tok), I32), vmem((2, n_tok), BF), vmem((n_tok, fb), BF), vmem((NH, n_tok, fb), BF),
            vmem((NH, fb, hu), BF), vmem((NH, fb, hu), BF), vmem((hu, width), BF),
            vmem((NT, cap, n_tok), F32), vmem((rows, n_tok), BF), vmem((n_tok, rows), F32),
            vmem((NT, cap, fb), BF), vmem((NH, NT, cap, fb), BF), vmem((NT, 8, n_tok), F32), vmem((NT, 8, n_tok), F32),
            vmem((2, NH, NT, cap, fb), BF), vmem((NH, fb, rows), BF),
            vmem((rows, hu), F32), vmem((rows, hu), F32), vmem((rows, hu), F32),
            vmem((rows, 2 * hu), BF), vmem((rows, hu), BF), vmem((hu, rows), BF),
            vmem((8, n_tok), F32), vmem((4, 8, n_tok), F32), vmem((4, 8, n_tok), F32),
            vmem((8, n_tok), F32), vmem((NT + 1, 8, n_tok), F32),
            vmem((NH, 2, hr, fb), F32),
            vmem((2, 2, 2, hr, fb), BF), vmem((2, 2, 2, hr, fb), BF),
            vmem((2, 2, 4, hr, fb), BF), vmem((2, 4, 2, hr, fb), BF),
            vmem((2, 2, hr // 2, fb), BF), vmem((2, 2, hr // 2, fb), BF),
            vmem((2, 2, 2, hr // 2, fb), BF), vmem((2, 2, 2, hr // 2, fb), BF),
            vmem((NT, cap, fb), BF), vmem((NT, cap, fb), BF),
            dma((7,)),
            dma((4,)), dma((3, 3)), dma((NH // 2,)),
            dma((3,)), dma((5, 11)), dma((5, 4)),
            dma((4,)), dma((2, 2)), dma((2, 4)), dma((2, 2)), dma((2,)),
            dma((2,)), dma((2,)), dma((2,)), dma((2,)),
        ],
        compiler_params=pltpu.CompilerParams(
            collective_id=0, has_side_effects=True, vmem_limit_bytes=50 * 1024 * 1024
        ),
    )(*[
        pltpu.with_memory_space_constraint(a, pltpu.HBM)
        for a in (
            routing_ids.T, route_weights.T, tokens, out_grad,
            gate_matrix.reshape(NH, fb, hu), up_matrix.reshape(NH, fb, hu), down_matrix[0],
        )
    ])
    ig, rg, gate_out, up_out, down_out = pl.pallas_call(
        copy_out,
        name="copy_out",
        out_shape=shapes,
        in_specs=[vm_spec] * 5,
        out_specs=(hbm_spec,) * 5,
        scratch_shapes=[dma((5,))],
        compiler_params=pltpu.CompilerParams(vmem_limit_bytes=1024 * 1024),
    )(*[pltpu.with_memory_space_constraint(a, pltpu.VMEM) for a in held])
    return (ig, rg.T, gate_out[None], up_out[None], down_out[None])


def solution(mesh):
    in_specs = (
        P("tok", "hid"),
        P("tok", "hid"),
        P("tok", None),
        P("tok", None),
        P("tok", None, "hid"),
        P("tok", None, "hid"),
        P("tok", "hid", None),
    )
    out_specs = (
        P("tok", "hid"),
        P("tok", None),
        P("tok", None, "hid"),
        P("tok", None, "hid"),
        P("tok", "hid", None),
    )
    return jax.shard_map(
        per_device, mesh=mesh, in_specs=in_specs, out_specs=out_specs, check_vma=False
    )
```

```python
import jax
import jax.numpy as jnp
from jax import lax
from jax.experimental import pallas as pl
from jax.experimental.pallas import tpu as pltpu
from jax.sharding import PartitionSpec as P

BF = jnp.bfloat16
F32 = jnp.float32
I32 = jnp.int32
NT = 8
NH = 16
SIGN = (1, -1)
PARTNERS = ((0, 1), (1, 0), (1, 1), (3, 0), (3, 1), (2, 0), (2, 1))
PLACE = (0, 1, 3, 2)
STREAMS = ((0, 0, 2, 0), (0, 2, 4, 0), (0, 6, 2, 1), (1, 6, 2, 1), (2, 0, 128, 1))
X_OWN, X_NEXT, X_FAR, G_FAR, RAW = range(5)
RELAYS = (
    ((0, 0, 0), (1, 0, 0)), ((0, 1, 0),), ((1, 1, 0),), ((0, 0, 1),), ((1, 0, 1),), ((0, 1, 1),), ((1, 1, 1),),
)


def dot(a, b):
    return lax.dot_general(a, b, (((1,), (0,)), ((), ())), preferred_element_type=F32)


def dot_nt(a, b):
    return lax.dot_general(a, b, (((1,), (1,)), ((), ())), preferred_element_type=F32)


def m4(v):
    return lax.rem(v + 8, 4)


def pick(index, values):
    out = values[-1]
    for k in range(len(values) - 2, -1, -1):
        out = jnp.where(index == k, values[k], out)
    return out


def loop(lo, hi, body):
    def step(i, carry):
        body(i)
        return carry

    lax.fori_loop(lo, hi, step, 0)


def exchange(
    ids_hbm, rw_hbm, tok_hbm, og_hbm, wg_hbm, wu_hbm, wd_hbm,
    ig_ref, rg_ref, gate_ref, up_ref, down_ref,
    ids_ref, rw_ref, tok_ref, raw, wg, wu, wd, sel, picks, selt, pack, pk, psend, precv, xg, xt, acc_g, acc_u, acc_r,
    dd, hp, hpt, qs, q1, q2, qt, qb,
    e32, rl1s, rl1r, fn1s, fn1r, rl2s, rl2r, fn2s, fn2r, shr, rb,
    w_sem, zs, zr, zg, gs, gr, gf, r1s, r1r, f1r, r2r, f2r, qss, qsr, bs, br,
):
    t = lax.axis_index("tok")
    hid = lax.axis_index("hid")
    z = lax.div(t, 2)
    core = lax.rem(t, 2)
    cx = lax.div(hid, 4)
    cy = lax.rem(hid, 4)
    cap = sel.shape[1]
    rows = NT * cap
    fb = xg.shape[-1]
    hu = wg.shape[-1]

    def to_hid(src, dst, ssem, rsem, target):
        return pltpu.make_async_remote_copy(
            src_ref=src, dst_ref=dst, send_sem=ssem, recv_sem=rsem,
            device_id={"hid": target}, device_id_type=pl.DeviceIdType.MESH,
        )

    def to_tok(src, dst, ssem, rsem, target):
        return pltpu.make_async_remote_copy(
            src_ref=src, dst_ref=dst, send_sem=ssem, recv_sem=rsem,
            device_id={"tok": target}, device_id_type=pl.DeviceIdType.MESH,
        )

    small = [
        pltpu.make_async_copy(src, dst, w_sem.at[3 + k])
        for k, (src, dst) in enumerate(
            ((ids_hbm, ids_ref), (rw_hbm, rw_ref), (tok_hbm, tok_ref), (og_hbm, raw.at[hid]))
        )
    ]
    for c in small:
        c.start()

    bar = pltpu.get_barrier_semaphore()
    for dz, dc in PARTNERS:
        pl.semaphore_signal(
            bar, inc=1, device_id={"tok": 2 * m4(z + dz) + lax.rem(core + dc, 2)},
            device_id_type=pl.DeviceIdType.MESH)
    for k in range(1, 4):
        for target in (4 * m4(cx + k) + cy, 4 * cx + m4(cy + k)):
            pl.semaphore_signal(
                bar, inc=1, device_id={"hid": target}, device_id_type=pl.DeviceIdType.MESH)

    w_copies = [
        pltpu.make_async_copy(wg_hbm, wg, w_sem.at[0]),
        pltpu.make_async_copy(wu_hbm, wu, w_sem.at[1]),
        pltpu.make_async_copy(wd_hbm, wd, w_sem.at[2]),
    ]
    for c in w_copies:
        c.start()

    for c in small:
        c.wait()

    n_tok = tok_ref.shape[0]
    ids = ids_ref[...]
    rw = rw_ref[...].astype(F32)
    expert = lax.broadcasted_iota(I32, (NT, n_tok), 0)
    first = ids[0:1, :] == expert
    second = ids[1:2, :] == expert
    named = jnp.where(first, 1.0, 0.0) + jnp.where(second, 1.0, 0.0)
    weight = jnp.where(first, rw[0:1, :], 0.0) + jnp.where(second, rw[1:2, :], 0.0)
    earlier = (
        lax.broadcasted_iota(I32, (n_tok, n_tok), 0) < lax.broadcasted_iota(I32, (n_tok, n_tok), 1)
    )
    place = dot(named.astype(BF), jnp.where(earlier, 1.0, 0.0).astype(BF))
    code = jnp.where(named > 0.5, place, -1.0).astype(I32)
    slot = lax.broadcasted_iota(I32, (cap, n_tok), 0)
    lane = lax.broadcasted_iota(I32, (cap, n_tok), 1)
    diag = slot == lane
    for e in range(NT):
        one = jnp.where(slot == code[e : e + 1, :], 1.0, 0.0)
        sel[e] = one
        col = jnp.sum(one * weight[e : e + 1, :], axis=1, keepdims=True)
        row = jnp.sum(jnp.where(diag, col, 0.0), axis=0, keepdims=True)
        psend[e] = jnp.broadcast_to(row, (8, n_tok))
    picks[...] = sel[...].reshape(rows, n_tok).astype(BF)
    pack[...] = dot(picks[...], tok_ref[...]).astype(BF).reshape(NT, cap, fb)
    xg[0, hid, core] = pack[t]
    precv[core] = psend[t]

    pl.semaphore_wait(bar, len(PARTNERS) + 6)

    def partner(m, back):
        dz, dc = PARTNERS[m]
        return 2 * m4(z - dz if back else z + dz) + lax.rem(core + dc, 2)

    def z_send(a, m):
        to = partner(m, False)
        place = 2 * PLACE[-PARTNERS[m][0] % 4] + core
        group = (m + 3) // 4
        if a == 2:
            return to_tok(psend.at[to], precv.at[place], zs.at[1], zr.at[2, 0], to)
        src = pack.at[to] if a == 0 else pk.at[hid, to]
        return to_tok(src, xg.at[a, hid, place], zs.at[3 * a], zr.at[a, group], to)

    def z_recv(a, group):
        first, count = ((0, 1), (2, 4), (6, 2))[group]
        ref = xg.at[a, hid, pl.ds(1 - core if group == 0 else first, count)]
        return to_tok(ref, ref, zs.at[0], zr.at[a, group], partner(0, True))

    def p_recv():
        ref = precv.at[pl.ds(0, 7)]
        return to_tok(ref, ref, zs.at[1], zr.at[2, 0], partner(0, True))

    prim = (cx, cy)
    seco = (cy, cx)

    def blk(a, p, s):
        return 4 * p + s if a == 0 else 4 * s + p

    half = NT // 2

    def part(st, block, h=None):
        array, first, count = STREAMS[st][:3]
        if h is not None:
            count //= 2
            first += h * count
        base = raw.at[block] if array == 2 else xg.at[array, block]
        return base.at[pl.ds(first, count)]

    def gather_copy(st, block, h, sem, target):
        ref = part(st, block, h)
        rsem = gr.at[st, sem] if sem < 11 else gf.at[st, sem - 11]
        return to_hid(ref, ref, gs.at[STREAMS[st][0]], rsem, target)

    def frame(st):
        g = STREAMS[st][3]
        return g, prim[g], seco[g]

    def p_own(st, d, recv=False):
        g, p, s = frame(st)
        b = blk(g, m4(p - SIGN[d]) if recv else p, s)
        return gather_copy(st, b, None, d, blk(g, m4(p + SIGN[d]), s))

    def p_fwd(st, d):
        g, p, s = frame(st)
        return gather_copy(st, blk(g, m4(p - SIGN[d]), s), d, 2, blk(g, m4(p + SIGN[d]), s))

    def s_own(st, o, d, recv=False):
        g, p, s = frame(st)
        b = blk(g, m4(p + o), m4(s - SIGN[d]) if recv else s)
        return gather_copy(st, b, None, 3 + 2 * o + d, blk(g, p, m4(s + SIGN[d])))

    def s_fwd(st, o, d):
        g, p, s = frame(st)
        return gather_copy(st, blk(g, m4(p + o), m4(s - SIGN[d])), d, 11 + o, blk(g, p, m4(s + SIGN[d])))

    def gather_begin(*sts):
        for st in sts:
            for d in range(2):
                p_own(st, d).start()
        for st in sts:
            for d in range(2):
                s_own(st, 0, d).start()

    def gather_p(*sts):
        for st in sts:
            for d in range(2):
                p_own(st, d, True).wait_recv()
                p_fwd(st, d).start()
        for st in sts:
            for d in range(2):
                for d2 in range(2):
                    s_own(st, (4 - SIGN[d]) % 4, d2).start()

    def gather_s(*sts):
        for st in sts:
            for d in range(2):
                s_own(st, 0, d, True).wait_recv()
                s_fwd(st, 0, d).start()

    def gather_1(st):
        gather_p(st)
        gather_s(st)

    def gather_5(st):
        g, p, s = frame(st)
        gather_copy(st, blk(g, m4(p + 2), s), None, 2, blk(g, m4(p + 1), s)).wait_recv()
        for d in range(2):
            s_own(st, 2, d).start()

    def gather_pass(st, *offsets):
        for o in offsets:
            for d in range(2):
                s_own(st, o, d, True).wait_recv()
                s_fwd(st, o, d).start()

    def gather_end(st, *offsets):
        g, p, s = frame(st)
        for o in offsets:
            gather_copy(st, blk(g, m4(p + o), m4(s + 2)), None, 11 + o, blk(g, p, m4(s + 1))).wait_recv()

    o_of = (0, 3, 1, 0, 0, 3, 3, 1, 1, 2, 0, 2, 3, 2, 1, 2)
    q_of = (0, 0, 0, 3, 1, 3, 1, 3, 1, 0, 2, 3, 2, 1, 2, 2)

    def raw_block(n):
        return blk(1, m4(cy + pick(n, o_of)), m4(cx + pick(n, q_of)))

    def raw_pack(n):
        h = raw_block(n)
        pk[h] = dot(picks[...], raw[h]).astype(BF).reshape(NT, cap, fb)
        xg[1, h, core] = pk[h, t]
        for m in range(5):
            to = partner(m, False)
            place = 2 * PLACE[-PARTNERS[m][0] % 4] + core
            to_tok(pk.at[h, to], xg.at[1, h, place], zs.at[2], zg.at[lax.div(n, 2)], to).start()

    def raw_packs(*places):
        loop(0, len(places), lambda i: raw_pack(pick(i, places)))

    gather_begin(RAW)
    for m in range(5):
        z_send(0, m).start()
    raw_pack(0)
    for a in range(2):
        for m in (5, 6):
            z_send(a, m).start()
    for m in range(7):
        z_send(2, m).start()
    z_recv(0, 0).wait_recv()
    gather_begin(X_OWN)
    acc_g[...] = jnp.zeros_like(acc_g)
    acc_u[...] = jnp.zeros_like(acc_u)
    acc_r[...] = jnp.zeros_like(acc_r)
    selt[...] = sel[...].reshape(rows, n_tok).T
    gather_1(RAW)
    raw_packs(1, 2, 3, 4)
    gather_1(X_OWN)
    gather_5(RAW)
    raw_packs(9)
    gather_5(X_OWN)
    gather_pass(RAW, 3, 1)
    raw_packs(5, 6, 7, 8)
    gather_pass(X_OWN, 3, 1)
    gather_pass(RAW, 2)
    z_recv(0, 1).wait_recv()
    z_recv(0, 2).wait_recv()
    z_recv(1, 2).wait_recv()
    gather_begin(X_FAR, G_FAR, X_NEXT)
    raw_packs(11, 13)
    gather_pass(X_OWN, 2)
    gather_p(X_FAR, X_NEXT, G_FAR)
    gather_end(RAW, 0, 3, 1, 2)
    raw_packs(10, 12, 14, 15)
    gather_s(X_FAR, X_NEXT, G_FAR)
    for c in w_copies:
        c.wait()
    gather_end(X_OWN, 0, 3, 1, 2)

    def gather_step(j):
        @pl.when(j == 1)
        def _():
            for st in (X_FAR, X_NEXT, G_FAR):
                gather_5(st)

        @pl.when(j == 2)
        def _():
            for st in (X_NEXT, X_FAR, G_FAR):
                gather_pass(st, 3, 1)

        @pl.when(j == 4)
        def _():
            for st in (X_NEXT, X_FAR, G_FAR):
                gather_pass(st, 2)

        for n, near, far in ((4, (), (0,)), (5, (0,), (3,)), (6, (3,), (1,)), (7, (1, 2), (2,))):
            @pl.when(j == n)
            def _():
                gather_end(X_NEXT, *near)
                gather_end(G_FAR, *near)
                gather_end(X_FAR, *far)

        hx, hg = [], []
        for k in (2 * j, 2 * j + 1):
            hx.append(blk(0, m4(cx + pick(k, o_of)), m4(cy + pick(k, q_of))))
            hg.append(raw_block(k))

        ten = xg.at[1, pl.ds(0, 2), pl.ds(0, 5)]
        to_tok(ten, ten, zs.at[2], zg.at[j], partner(0, True)).wait_recv()
        pair(hx, hg)

    def pair(hx, hg):
        x = jnp.concatenate([xg[0, h].reshape(rows, fb) for h in hx], axis=1)
        acc_g[...] += dot(x, jnp.concatenate([wg[h] for h in hx], axis=0))
        acc_u[...] += dot(x, jnp.concatenate([wu[h] for h in hx], axis=0))
        acc_r[...] += dot_nt(
            jnp.concatenate([xg[1, h].reshape(rows, fb) for h in hg], axis=1),
            jnp.concatenate([wd[:, pl.ds(pl.multiple_of(h * fb, fb), fb)] for h in hg], axis=1))
        for h in hx:
            xt[h] = xg[0, h].reshape(rows, fb).T
            for w in (wg, wu):
                for k in range(hu // fb):
                    w[h, :, k * fb : (k + 1) * fb] = w[h, :, k * fb : (k + 1) * fb].T

    p_recv().wait_recv()
    loop(0, NH // 2, gather_step)

    def deltas(b):
        at = pl.ds(pl.multiple_of(b * cap, cap), cap)
        g = acc_g[at, :]
        u = acc_u[at, :]
        r = acc_r[at, :]
        p = jnp.sum(jnp.where(diag, precv[b, 0:1, :], 0.0), axis=1, keepdims=True)
        s = 1.0 / (1.0 + jnp.exp(-g))
        act = g * s
        rp = r * p
        dd[at, 0:hu] = (rp * u * s * (1.0 + g * (1.0 - s))).astype(BF)
        dd[at, hu : 2 * hu] = (rp * act).astype(BF)

    def hiddens(b):
        at = pl.ds(pl.multiple_of(b * cap, cap), cap)
        g = acc_g[at, :]
        p = jnp.sum(jnp.where(diag, precv[b, 0:1, :], 0.0), axis=1, keepdims=True)
        au = g * (1.0 / (1.0 + jnp.exp(-g))) * acc_u[at, :]
        hp[at, :] = (au * p).astype(BF)
        q = jnp.sum(au.astype(BF).astype(F32) * acc_r[at, :], axis=1, keepdims=True)
        qs[pl.ds(b, 1), :] = jnp.sum(jnp.where(diag, q, 0.0), axis=0, keepdims=True)

    loop(0, NT, deltas)

    hrows = rows // 2

    def along(a, d):
        p, s = prim[a], seco[a]
        return blk(a, m4(p + SIGN[d]), s)

    def across(a, d):
        p, s = prim[a], seco[a]
        return blk(a, p, m4(s + SIGN[d]))

    def rl1(a, d, i):
        return to_hid(rl1s.at[a, d, i], rl1r.at[d, i, a], r1s.at[0], r1r.at[d, i], along(a, d))

    def fn1(a, d, q):
        return to_hid(fn1s.at[a, d, q], fn1r.at[a, q, d], r1s.at[1], f1r.at[a, q], along(a, d))

    def rl2(a, d):
        return to_hid(rl2s.at[a, d], rl2r.at[a, d], r1s.at[2], r2r.at[a, d], across(a, d))

    def fn2(a, d, k):
        return to_hid(fn2s.at[a, d, k], fn2r.at[a, d, k], r1s.at[3], f2r.at[a], across(a, d))

    def q_x(k):
        return to_hid(qs, q1.at[cx], qss.at[0], qsr.at[0], 4 * m4(cx + k) + cy)

    def q_y(k):
        return to_hid(qt, q2.at[cy], qss.at[1], qsr.at[1], 4 * cx + m4(cy + k))

    x_of = (2, 2, 3, 2, 1, 2, 0, 1, 3, 3, 1, 1, 3, 0, 0, 0)
    y_of = (2, 3, 2, 1, 2, 0, 2, 3, 3, 1, 1, 0, 0, 1, 3, 0)

    def e_step(n):
        where = []
        for k in range(2):
            h = 4 * m4(cx + pick(2 * n + k, x_of)) + m4(cy + pick(2 * n + k, y_of))
            turned = jnp.concatenate(
                [w[h, :, i * fb : (i + 1) * fb] for w in (wg, wu) for i in range(hu // fb)], axis=0)
            where.append(h)
            e32[h] = dot(dd[...], turned).reshape(2, hrows, fb)
        for k, todo in enumerate(RELAYS):
            @pl.when(n == k // 2)
            def _():
                for a, d, i in todo:
                    rl1s[a, d, i] = e32[where[k % 2], a].astype(BF)
                    rl1(a, d, i).start()

    relayed = {2: (0, 0), 1: (0, 1), 3: (1, 0), 0: (1, 1)}

    def first_send(q, d):
        way, i = relayed[q]
        if d == way:
            to_hid(rl1r.at[d, i], rl1r.at[d, i], r1s.at[0], r1r.at[d, i], along(0, d)).wait_recv()
        for a in range(2):
            e = e32[blk(a, m4(prim[a] + SIGN[d]), m4(seco[a] + q)), a]
            if d == way:
                e = e + rl1r[d, i, a].astype(F32)
            fn1s[a, d, q] = e.astype(BF)
            fn1(a, d, q).start()

    def first_step(q):
        way = relayed[q][0]
        first_send(q, 1 - way)
        first_send(q, way)

    def total_of(a, q):
        to_hid(fn1r.at[a, q], fn1r.at[a, q], r1s.at[1], f1r.at[a, q], along(a, 0)).wait_recv()
        return (e32[blk(a, prim[a], m4(seco[a] + q)), a]
                + fn1r[a, q, 0].astype(F32) + fn1r[a, q, 1].astype(F32))

    def weight_step(c):
        at = pl.ds(pl.multiple_of(2 * c * fb, 2 * fb), 2 * fb)
        x = xt[pl.ds(2 * c, 2)].reshape(2 * fb, rows)
        gate_ref[at, :] = dot(x, dd[:, 0:hu]).astype(BF)
        up_ref[at, :] = dot(x, dd[:, hu : 2 * hu]).astype(BF)
        for i in range(2):
            h = 2 * c + i
            down_ref[:, pl.ds(pl.multiple_of(h * fb, fb), fb)] = dot(
                hpt[...], xg[1, h].reshape(rows, fb)).astype(BF)

    loop(0, 4, e_step)
    first_send(2, 1)
    loop(4, NH // 2, e_step)
    first_send(3, 0)
    first_send(2, 0)
    first_send(3, 1)
    loop(0, NT, hiddens)
    q1[cx] = qs[...]
    for k in range(1, 4):
        q_x(k).start()
    first_step(1)
    hpt[...] = hp[...].T
    loop(0, 2, weight_step)
    quarter = hrows // 2
    for a in range(2):
        s = total_of(a, 2)
        for d in range(2):
            rl2s[a, d] = s[d * quarter : (d + 1) * quarter].astype(BF)
            rl2(a, d).start()
    first_step(0)
    loop(2, 3, weight_step)
    to_hid(q1.at[pl.ds(0, 3)], q1.at[pl.ds(0, 3)], qss.at[0], qsr.at[0], along(0, 0)).wait_recv()
    qt[...] = q1[0] + q1[1] + q1[2] + q1[3]
    q2[cy] = qt[...]
    for k in range(1, 4):
        q_y(k).start()
    loop(3, 4, weight_step)
    for d, q in ((1, 3), (0, 1)):
        for a in range(2):
            s = total_of(a, q)
            fn2s[a, d, 1 - d] = s[(1 - d) * quarter : (2 - d) * quarter].astype(BF)
            fn2(a, d, 1 - d).start()
    for d, q in ((1, 3), (0, 1)):
        for a in range(2):
            at = slice(d * quarter, (d + 1) * quarter)
            s = e32[blk(a, prim[a], m4(seco[a] + q)), a, at]
            s = s + fn1r[a, q, 0, at].astype(F32) + fn1r[a, q, 1, at].astype(F32)
            rl2(a, d).wait_recv()
            fn2s[a, d, d] = (s + rl2r[a, d].astype(F32)).astype(BF)
            fn2(a, d, d).start()
    loop(4, 5, weight_step)
    to_hid(q2.at[pl.ds(0, 3)], q2.at[pl.ds(0, 3)], qss.at[1], qsr.at[1], across(0, 0)).wait_recv()
    qw = q2[0] + q2[1] + q2[2] + q2[3]
    qsum = qb.at[NT]
    qsum[...] = qw
    qb[t] = qw

    def c_send(m):
        to = partner(m, False)
        return to_tok(qb.at[NT], qb.at[t], bs.at[1], br.at[1], to)

    for m in range(7):
        c_send(m).start()


    def b_send(m):
        to = partner(m, False)
        dz, dc = PARTNERS[m]
        return to_tok(shr.at[2 * PLACE[dz] + lax.rem(core + dc, 2)], rb.at[t], bs.at[0], br.at[0], to)

    for a in (1, 0):
        s = total_of(a, 0)
        to_hid(fn2r.at[a], fn2r.at[a], r1s.at[3], f2r.at[a], across(a, 0)).wait_recv()
        for d in range(2):
            s = s + fn2r[a, d].astype(F32).reshape(hrows, fb)
        shr[a * half : (a + 1) * half] = s.astype(BF).reshape(half, cap, fb)
        for m in (5, 6, 0, 1, 2, 3, 4):
            if PLACE[PARTNERS[m][0]] // 2 == a:
                b_send(m).start()
    rb[t] = shr[core]
    loop(5, 8, weight_step)

    def back_wait(ref, k):
        ref = ref.at[pl.ds(0, len(PARTNERS))]
        return to_tok(ref, ref, bs.at[k], br.at[k], partner(0, True))

    back_wait(qb, 1).wait_recv()
    block = lax.broadcasted_iota(I32, (8, n_tok), 0)
    zero = jnp.zeros((1, n_tok), F32)
    route = [zero, zero]
    for e in range(NT):
        row = jnp.sum(jnp.where(block == 2 * pick(m4(z - e // 2), PLACE) + core, qb[e], 0.0), axis=0, keepdims=True)
        col = jnp.sum(jnp.where(diag, row, 0.0), axis=1, keepdims=True)
        val = jnp.sum(sel[e] * col, axis=0, keepdims=True)
        for k in range(2):
            route[k] = route[k] + jnp.where(ids[k : k + 1, :] == e, val, 0.0)
    rg_ref[...] = jnp.concatenate(route, axis=0).astype(BF)

    back_wait(rb, 0).wait_recv()
    ig_ref[...] = dot(selt[...].astype(BF), rb[...].reshape(rows, fb)).astype(BF)

    n_z = len(PARTNERS)
    near = partner(0, False)
    beside = along(0, 0)
    ends = [
        to_tok(pack.at[pl.ds(0, n_z)], pack.at[pl.ds(0, n_z)], zs.at[0], zr.at[0, 0], near),
        to_tok(xg.at[0, pl.ds(0, 10)], xg.at[0, pl.ds(0, 10)], zs.at[2], zr.at[0, 0], near),
        to_tok(pk.at[0, pl.ds(0, 2)], pk.at[0, pl.ds(0, 2)], zs.at[3], zr.at[0, 0], near),
        to_tok(psend.at[pl.ds(0, n_z)], psend.at[pl.ds(0, n_z)], zs.at[1], zr.at[0, 0], near),
        to_hid(xg.at[0, pl.ds(0, NH - 1)], xg.at[0, pl.ds(0, NH - 1)], gs.at[0], gf.at[0, 0], beside),
        to_hid(xg.at[1, pl.ds(0, NH - 1), pl.ds(6, 2)], xg.at[1, pl.ds(0, NH - 1), pl.ds(6, 2)],
               gs.at[1], gf.at[0, 0], beside),
        to_hid(raw.at[pl.ds(0, NH - 1)], raw.at[pl.ds(0, NH - 1)], gs.at[2], gf.at[0, 0], beside),
        to_hid(rl1s, rl1r, r1s.at[0], gf.at[0, 0], beside),
        to_hid(fn1s, fn1s, r1s.at[1], gf.at[0, 0], beside),
        to_hid(rl2s, rl2r, r1s.at[2], gf.at[0, 0], beside),
        to_hid(fn2s, fn2r, r1s.at[3], gf.at[0, 0], beside),
        to_hid(q1.at[pl.ds(0, 3)], q1.at[pl.ds(0, 3)], qss.at[0], gf.at[0, 0], beside),
        to_hid(q2.at[pl.ds(0, 3)], q2.at[pl.ds(0, 3)], qss.at[1], gf.at[0, 0], beside),
        back_wait(shr, 0),
        back_wait(qb, 1),
    ]
    for c in ends:
        c.wait_send()


def copy_out(*refs):
    n = (len(refs) - 1) // 2
    sem = refs[2 * n]
    copies = [pltpu.make_async_copy(refs[k], refs[n + k], sem.at[k]) for k in range(n)]
    for c in copies:
        c.start()
    for c in copies:
        c.wait()


def per_device(tokens, out_grad, routing_ids, route_weights, gate_matrix, up_matrix, down_matrix):
    n_tok, fb = tokens.shape
    cap = 3 * n_tok // NT
    rows = NT * cap
    hu = gate_matrix.shape[2]
    width = gate_matrix.shape[1]
    hr = rows // 2
    vmem = pltpu.VMEM
    dma = pltpu.SemaphoreType.DMA
    hbm_spec = pl.BlockSpec(memory_space=pltpu.HBM)
    vm_spec = pl.BlockSpec(memory_space=pltpu.VMEM)
    shapes = (
        jax.ShapeDtypeStruct((n_tok, fb), BF),
        jax.ShapeDtypeStruct((2, n_tok), BF),
        jax.ShapeDtypeStruct((width, hu), BF),
        jax.ShapeDtypeStruct((width, hu), BF),
        jax.ShapeDtypeStruct((hu, width), BF),
    )
    held = pl.pallas_call(
        exchange,
        name="exchange",
        out_shape=tuple(vmem(s.shape, s.dtype) for s in shapes),
        in_specs=[hbm_spec] * 7,
        out_specs=(vm_spec,) * 5,
        scratch_shapes=[
            vmem((2, n_tok), I32), vmem((2, n_tok), BF), vmem((n_tok, fb), BF), vmem((NH, n_tok, fb), BF),
            vmem((NH, fb, hu), BF), vmem((NH, fb, hu), BF), vmem((hu, width), BF),
            vmem((NT, cap, n_tok), F32), vmem((rows, n_tok), BF), vmem((n_tok, rows), F32),
            vmem((NT, cap, fb), BF), vmem((NH, NT, cap, fb), BF), vmem((NT, 8, n_tok), F32), vmem((NT, 8, n_tok), F32),
            vmem((2, NH, NT, cap, fb), BF), vmem((NH, fb, rows), BF),
            vmem((rows, hu), F32), vmem((rows, hu), F32), vmem((rows, hu), F32),
            vmem((rows, 2 * hu), BF), vmem((rows, hu), BF), vmem((hu, rows), BF),
            vmem((8, n_tok), F32), vmem((4, 8, n_tok), F32), vmem((4, 8, n_tok), F32),
            vmem((8, n_tok), F32), vmem((NT + 1, 8, n_tok), F32),
            vmem((NH, 2, hr, fb), F32),
            vmem((2, 2, 2, hr, fb), BF), vmem((2, 2, 2, hr, fb), BF),
            vmem((2, 2, 4, hr, fb), BF), vmem((2, 4, 2, hr, fb), BF),
            vmem((2, 2, hr // 2, fb), BF), vmem((2, 2, hr // 2, fb), BF),
            vmem((2, 2, 2, hr // 2, fb), BF), vmem((2, 2, 2, hr // 2, fb), BF),
            vmem((NT, cap, fb), BF), vmem((NT, cap, fb), BF),
            dma((7,)),
            dma((4,)), dma((3, 3)), dma((NH // 2,)),
            dma((3,)), dma((5, 11)), dma((5, 4)),
            dma((4,)), dma((2, 2)), dma((2, 4)), dma((2, 2)), dma((2,)),
            dma((2,)), dma((2,)), dma((2,)), dma((2,)),
        ],
        compiler_params=pltpu.CompilerParams(
            collective_id=0, has_side_effects=True, vmem_limit_bytes=50 * 1024 * 1024
        ),
    )(*[
        pltpu.with_memory_space_constraint(a, pltpu.HBM)
        for a in (
            routing_ids.T, route_weights.T, tokens, out_grad,
            gate_matrix.reshape(NH, fb, hu), up_matrix.reshape(NH, fb, hu), down_matrix[0],
        )
    ])
    ig, rg, gate_out, up_out, down_out = pl.pallas_call(
        copy_out,
        name="copy_out",
        out_shape=shapes,
        in_specs=[vm_spec] * 5,
        out_specs=(hbm_spec,) * 5,
        scratch_shapes=[dma((5,))],
        compiler_params=pltpu.CompilerParams(vmem_limit_bytes=1024 * 1024),
    )(*[pltpu.with_memory_space_constraint(a, pltpu.VMEM) for a in held])
    return (ig, rg.T, gate_out[None], up_out[None], down_out[None])


def solution(mesh):
    in_specs = (
        P("tok", "hid"),
        P("tok", "hid"),
        P("tok", None),
        P("tok", None),
        P("tok", None, "hid"),
        P("tok", None, "hid"),
        P("tok", "hid", None),
    )
    out_specs = (
        P("tok", "hid"),
        P("tok", None),
        P("tok", None, "hid"),
        P("tok", None, "hid"),
        P("tok", "hid", None),
    )
    return jax.shard_map(
        per_device, mesh=mesh, in_specs=in_specs, out_specs=out_specs, check_vma=False
    )
```
